128 devices in a mesh: tm: 8 (over x, y_hi), tile: 16 (over z, y_lo, core).
Axes of the slice: x: 4, y: 4 (y_hi: 2, y_lo: 2; y = y_hi * 2 + y_lo), z: 4, core: 2. Of those that a mesh axis runs over, the one named last changes fastest.
Arguments:
- first_input: bfloat16 [16, 32, 64, 384], P('tm', None, 'tile'), may hold values from -6 to 6
- second_input: bfloat16 [16, 32, 64, 384], P('tm', None, 'tile'), may hold values from -6 to 6
- output_grad: bfloat16 [16, 32, 64, 384], P('tm', None, 'tile'), may hold values from -6 to 6
- first_gain: float32 [384], replicated, may hold values from 0.1 to 1.9
- first_shift: float32 [384], replicated, may hold values from -1 to 1
- first_kernel: bfloat16 [27, 384, 384], replicated, may hold values from -1 to 1
- second_gain: float32 [384], replicated, may hold values from 0.1 to 1.9
- second_shift: float32 [384], replicated, may hold values from -1 to 1
- second_kernel: bfloat16 [27, 384, 384], replicated, may hold values from -1 to 1
- latent_kernel: bfloat16 [27, 16, 384], replicated, may hold values from -0.0625 to 0.0625
Outputs:
- latent_grad: float32 [64, 8192], P(None, ('tm', 'tile'))
The draws below stay inside these ranges and needn't reach their ends.
All inputs are finite; a program needn't handle non-finite values.
Results may differ from the reference program's by a relative error of at most 0.0044.
Values may be sent and summed in bfloat16 or wider, within the bound.
No kernel may reach another device: no remote copies, remote signals or barrier semaphores. Data moves between devices by JAX's collectives and lax.ppermute only.
A program may use at most 64 MiB of HBM per device.

```python
import jax
import jax.numpy as jnp
from jax import lax

C = 384
L = 16
GROUPS = 32
H = 32
TT = 16
W = 64


def shared_parts(key):
    base_key = jax.random.fold_in(key, 7001)
    level_key, field_key, group_key = jax.random.split(base_key, 3)
    levels = jax.random.uniform(level_key, (W // 2,), jnp.float32, -1.0, 3.0)
    profile = jnp.repeat(levels, 2)
    raw_field = jax.random.normal(field_key, (H + 2, W + 2), jnp.float32)
    smooth = jnp.zeros((H, W), jnp.float32)
    for row_shift in range(3):
        for col_shift in range(3):
            smooth = smooth + raw_field[row_shift:row_shift + H, col_shift:col_shift + W]
    smooth = smooth / 3.0
    group_sign = jax.random.normal(group_key, (GROUPS,), jnp.float32)
    group_weight = jnp.repeat(group_sign, C // GROUPS)
    return (profile, smooth, group_weight)


def stored_draw(key, marker, profile_scale, field_scale):
    profile, smooth, group_weight = shared_parts(key)
    own_key = jax.random.fold_in(key, marker)
    noise_key, slope_key = jax.random.split(own_key, 2)
    noise_part = jax.random.normal(noise_key, (TT, H, W, C), jnp.float32)
    slopes = jax.random.normal(slope_key, (2, C), jnp.float32)
    along_profile = profile_scale * group_weight + 0.25 * slopes[0]
    along_field = field_scale * group_weight + 0.25 * slopes[1]
    result = 0.8 * noise_part + along_profile * profile[None, None, :, None] + along_field * smooth[None, :, :, None]
    return jnp.clip(result, -6.0, 6.0).astype(jnp.bfloat16)


def kernel_draw(key, marker):
    own_key = jax.random.fold_in(key, marker)
    entries = jnp.clip(jax.random.normal(own_key, (27, C, C), jnp.float32), -6.0, 6.0)
    entries = entries * (27.0 * C) ** (-0.5)
    entries = entries.at[22].add(0.5 * jnp.eye(C, dtype=jnp.float32))
    return entries.astype(jnp.bfloat16)


def draw_first_input(key, part):
    return stored_draw(key, 11, 0.5, 0.6)


def draw_second_input(key, part):
    return stored_draw(key, 12, 0.5, 0.6)


def draw_output_grad(key, part):
    return stored_draw(key, 13, 0.6, 0.6)


def draw_first_kernel(key, part):
    return kernel_draw(key, 21)


def draw_second_kernel(key, part):
    return kernel_draw(key, 22)


def noise(key, dims, spread, bound, kind=jnp.bfloat16):
    array = jax.random.normal(key, dims, jnp.float32) * spread
    return jnp.minimum(jnp.maximum(array, -bound), bound).astype(kind)


def setup_inputs(seed: int = 0) -> dict:
    arg_keys = jax.random.split(jax.random.key(seed), 11)
    first_input = draw_first_input(jax.random.fold_in(arg_keys[10], 71), 0)
    second_input = draw_second_input(jax.random.fold_in(arg_keys[10], 71), 0)
    output_grad = draw_output_grad(jax.random.fold_in(arg_keys[10], 71), 0)
    first_gain = jnp.clip(1.0 + 0.18 * jax.random.normal(arg_keys[3], (C,), jnp.float32), 0.1, 1.9)
    first_shift = jnp.clip(jax.random.uniform(arg_keys[4], (C,), jnp.float32, -1.0, 1.0), -1.0, 1.0)
    first_kernel = draw_first_kernel(jax.random.fold_in(arg_keys[10], 71), 0)
    second_gain = jnp.clip(1.0 + 0.18 * jax.random.normal(arg_keys[6], (C,), jnp.float32), 0.1, 1.9)
    second_shift = jnp.clip(jax.random.uniform(arg_keys[7], (C,), jnp.float32, -1.0, 1.0), -1.0, 1.0)
    second_kernel = draw_second_kernel(jax.random.fold_in(arg_keys[10], 71), 0)
    latent_kernel = noise(arg_keys[9], (27, L, C), (27 * C) ** -0.5, 0.0625)
    return dict(first_input=first_input, second_input=second_input, output_grad=output_grad, first_gain=first_gain, first_shift=first_shift, first_kernel=first_kernel, second_gain=second_gain, second_shift=second_shift, second_kernel=second_kernel, latent_kernel=latent_kernel)


epsilon = 1e-05

def apply_taps(padded, kernel):
    taps = kernel.reshape(3, 3, 3, kernel.shape[1], kernel.shape[2])[::-1, ::-1, ::-1]
    result = lax.conv_general_dilated(padded[None], taps, (1, 1, 1), 'VALID', dimension_numbers=('NDHWC', 'DHWOI', 'NDHWC'), preferred_element_type=jnp.float32)
    return result[0]

def backward_section(stored, grad, kernel, gain, shift):
    frame_count, row_count, col_count, channel_count = stored.shape
    values = stored.astype(jnp.float32).reshape(frame_count, row_count, col_count, GROUPS, -1)
    cell_count = row_count * col_count * values.shape[-1]
    average = lax.optimization_barrier(jnp.sum(values, axis=(1, 2, 4))) / cell_count
    variance = lax.optimization_barrier(jnp.sum(values * values, axis=(1, 2, 4))) / cell_count - average * average
    inv_std = lax.rsqrt(variance + epsilon)[:, None, None, :, None]
    normed = (values - average[:, None, None, :, None]) * inv_std
    group_gain = gain.reshape(GROUPS, -1)
    preact = normed * group_gain + shift.reshape(GROUPS, -1)
    padded = jnp.pad(grad, ((0, 2), (1, 1), (1, 1), (0, 0)))
    upstream = apply_taps(padded, kernel).reshape(values.shape)
    sigmoid_z = jax.nn.sigmoid(preact)
    through = upstream * sigmoid_z * (1.0 + preact * (1.0 - sigmoid_z)) * group_gain
    mean_grad = lax.optimization_barrier(jnp.sum(through, axis=(1, 2, 4))) / cell_count
    mean_cross = lax.optimization_barrier(jnp.sum(through * normed, axis=(1, 2, 4))) / cell_count
    result = grad.astype(jnp.float32).reshape(values.shape) + inv_std * (through - mean_grad[:, None, None, :, None] - normed * mean_cross[:, None, None, :, None])
    return result.reshape(frame_count, row_count, col_count, channel_count).astype(jnp.bfloat16)

def reference(first_input, second_input, output_grad, first_gain, first_shift, first_kernel, second_gain, second_shift, second_kernel, latent_kernel):
    second_grad = backward_section(second_input, output_grad, second_kernel, second_gain, second_shift)
    first_grad = backward_section(first_input, second_grad, first_kernel, first_gain, first_shift)
    frame_count, row_count, col_count, channel_count = first_grad.shape
    padded = jnp.pad(first_grad, ((0, 2), (1, 1), (1, 1), (0, 0)))
    pixel_grad = apply_taps(padded, latent_kernel)
    latent_count = pixel_grad.shape[-1]
    tiled = pixel_grad.reshape(frame_count, row_count // 2, 2, col_count // 2, 2, latent_count)
    tiled = jnp.transpose(tiled, (5, 2, 4, 0, 1, 3))
    return tiled.reshape(4 * latent_count, -1)
```

```python
import functools

import jax
import jax.numpy as jnp
import numpy as np
from jax import lax
from jax.experimental import pallas as pl
from jax.experimental.pallas import tpu as pltpu
from jax.sharding import Mesh
from jax.sharding import PartitionSpec as P

GROUPS = 32
TILE = ("tile_0", "tile_1", "tile_2")
TM_TILE = ("tm",) + TILE
EPSILON = 1e-05
MIB = 1 << 20


def vmem(count):
    return [pl.BlockSpec(memory_space=pltpu.VMEM)] * count


def nt_dot(left, right, **kw):
    return lax.dot_general(
        left, right, (((1,), (1,)), ((), ())), preferred_element_type=jnp.float32, **kw
    )


def exact_dot(left, right):
    return jnp.dot(
        left, right, precision=lax.Precision.HIGHEST, preferred_element_type=jnp.float32
    )


def group_sum(rows):
    channels = rows.shape[-1]
    per = channels // GROUPS
    row = lax.broadcasted_iota(jnp.int32, (channels, channels), 0) // per
    col = lax.broadcasted_iota(jnp.int32, (channels, channels), 1) // per
    return exact_dot(rows, (row == col).astype(jnp.float32))


def spread(ref, rows):
    ref[...] = jnp.broadcast_to(rows[None], ref.shape)


def moments_kernel(second_ref, first_ref, out_ref):
    rows = []
    for ref in (second_ref, first_ref):
        frames = ref.shape[0]
        values = [ref[f].astype(jnp.float32).reshape(-1, ref.shape[-1]) for f in range(frames)]
        rows += [jnp.sum(v, axis=0, keepdims=True) for v in values]
        rows += [jnp.sum(v * v, axis=0, keepdims=True) for v in values]
    spread(out_ref, jnp.concatenate(rows, axis=0))


def moments(second, first, peers):
    frames, _, _, channels = second.shape
    return pl.pallas_call(
        moments_kernel,
        out_shape=jax.ShapeDtypeStruct((peers, 4 * frames, channels), jnp.float32),
        in_specs=vmem(2),
        out_specs=pl.BlockSpec(memory_space=pltpu.VMEM),
        compiler_params=pltpu.CompilerParams(vmem_limit_bytes=8 * MIB),
        name="moments",
    )(second, first)


def conv_kernel(
    cells,
    base,
    par_ref,
    own_ref,
    next_ref,
    ra_ref,
    rb_ref,
    ran_ref,
    rbn_ref,
    x_ref,
    mom_ref,
    gain_ref,
    shift_ref,
    w_hbm,
    q_ref,
    sums_ref,
    stats_ref,
    ext,
    acc,
    wbuf,
    sems,
):
    frames, cols, rows, channels = own_ref.shape
    taps = 3
    copies = [
        pltpu.make_async_copy(
            w_hbm.at[pl.ds(taps * k, taps)], wbuf.at[pl.ds(taps * k, taps)], sems.at[k]
        )
        for k in range(9)
    ]
    for copy in copies:
        copy.start()
    even = par_ref[0] == 0
    ext[0:frames, 1 : cols + 1] = own_ref[...]
    ext[frames : 2 * frames, 1 : cols + 1] = next_ref[...]
    for at, a_ref, b_ref in ((0, ra_ref, rb_ref), (frames, ran_ref, rbn_ref)):
        a, b = a_ref[...], b_ref[...]
        ext[at : at + frames, 0] = jnp.where(even, b, a)
        ext[at : at + frames, cols + 1] = jnp.where(even, a, b)
    count = frames * cols * rows
    for a in range(3):
        left = jnp.concatenate(
            [
                ext[2 - a : 2 - a + frames, 2 - c : 2 - c + cols].reshape(count, channels)
                for c in range(3)
            ],
            axis=1,
        )
        for b in range(3):
            k = 3 * a + b
            copies[k].wait()
            right = jnp.concatenate([wbuf[3 * k + c] for c in range(3)], axis=1)
            part = nt_dot(left, right)
            acc[b] = part if a == 0 else acc[b] + part
    row = lax.broadcasted_iota(jnp.int32, (count, 1), 0) % rows
    up = jnp.where(row < rows - 1, pltpu.roll(acc[0], count - 1, 0), 0.0)
    down = jnp.where(row > 0, pltpu.roll(acc[2], 1, 0), 0.0)
    upstream = acc[1] + up + down

    totals = group_sum(jnp.sum(mom_ref[...], axis=0)) * (1.0 / cells)
    gain, shift = gain_ref[...], shift_ref[...]
    sums, crosses, means, scales = [], [], [], []
    half = count // frames
    for f in range(frames):
        mean = totals[base + f : base + f + 1]
        var = totals[base + frames + f : base + frames + f + 1] - mean * mean
        scale = lax.rsqrt(var + EPSILON)
        normed = (x_ref[f].astype(jnp.float32).reshape(half, channels) - mean) * scale
        pre = normed * gain + shift
        sig = jax.nn.sigmoid(pre)
        q = upstream[f * half : (f + 1) * half] * sig * (1.0 + pre * (1.0 - sig)) * gain
        q_ref[f] = q.reshape(cols, rows, channels)
        sums.append(jnp.sum(q, axis=0, keepdims=True))
        crosses.append(jnp.sum(q * normed, axis=0, keepdims=True))
        means.append(mean)
        scales.append(scale)
    spread(sums_ref, jnp.concatenate(sums + crosses, axis=0))
    stats_ref[...] = jnp.concatenate(means + scales, axis=0)


def conv_section(par, grad, halo, stored, mom, gain, shift, kernel, cells, base, peers):
    frames, cols, rows, channels = grad.shape
    nxt, ra, rb, ran, rbn = halo
    hbm = pl.BlockSpec(memory_space=pl.ANY)
    return pl.pallas_call(
        functools.partial(conv_kernel, cells, base),
        out_shape=(
            jax.ShapeDtypeStruct(grad.shape, jnp.float32),
            jax.ShapeDtypeStruct((peers, 2 * frames, channels), jnp.float32),
            jax.ShapeDtypeStruct((2 * frames, channels), jnp.float32),
        ),
        in_specs=[pl.BlockSpec(memory_space=pltpu.SMEM)] + vmem(10) + [hbm],
        out_specs=tuple(vmem(3)),
        scratch_shapes=[
            pltpu.VMEM((2 * frames, cols + 2, rows, channels), jnp.bfloat16),
            pltpu.VMEM((3, frames * cols * rows, channels), jnp.float32),
            pltpu.VMEM(kernel.shape, jnp.bfloat16),
            pltpu.SemaphoreType.DMA((9,)),
        ],
        compiler_params=pltpu.CompilerParams(vmem_limit_bytes=32 * MIB),
        name="conv",
    )(par, grad, nxt, ra, rb, ran, rbn, stored, mom, gain, shift, kernel)


def block_grad(cells, grad_ref, q_ref, x_ref, stats_ref, sums_ref):
    frames, cols, rows, channels = grad_ref.shape
    totals = group_sum(jnp.sum(sums_ref[...], axis=0)) * (1.0 / cells)
    result = []
    for f in range(frames):
        mean = stats_ref[f : f + 1]
        scale = stats_ref[frames + f : frames + f + 1]
        flat = (cols * rows, channels)
        normed = (x_ref[f].astype(jnp.float32).reshape(flat) - mean) * scale
        value = grad_ref[f].astype(jnp.float32).reshape(flat) + scale * (
            q_ref[f].reshape(flat)
            - totals[f : f + 1]
            - normed * totals[frames + f : frames + f + 1]
        )
        result.append(value.astype(jnp.bfloat16))
    return result


def dx_kernel(cells, par_ref, grad_ref, q_ref, x_ref, stats_ref, sums_ref, dx_ref, sa_ref, sb_ref):
    frames, cols, rows, channels = grad_ref.shape
    even = par_ref[0] == 0
    for f, value in enumerate(block_grad(cells, grad_ref, q_ref, x_ref, stats_ref, sums_ref)):
        value = value.reshape(cols, rows, channels)
        dx_ref[f] = value
        sa_ref[f] = jnp.where(even, value[cols - 1], value[0])
        sb_ref[f] = jnp.where(even, value[0], value[cols - 1])


def dx_section(par, grad, q, stored, stats, sums, cells):
    frames, cols, rows, channels = grad.shape
    edge = jax.ShapeDtypeStruct((frames, rows, channels), jnp.bfloat16)
    return pl.pallas_call(
        functools.partial(dx_kernel, cells),
        out_shape=(jax.ShapeDtypeStruct(grad.shape, jnp.bfloat16), edge, edge),
        in_specs=[pl.BlockSpec(memory_space=pltpu.SMEM)] + vmem(5),
        out_specs=tuple(vmem(3)),
        compiler_params=pltpu.CompilerParams(vmem_limit_bytes=8 * MIB),
        name="dx",
    )(par, grad, q, stored, stats, sums)


def latent_kernel_body(cells, grad_ref, q_ref, x_ref, stats_ref, sums_ref, k_ref, own_ref, prev_ref, wide):
    frames, cols, rows, channels = grad_ref.shape
    lat = k_ref.shape[1]
    lanes = wide.shape[1]
    grad = jnp.concatenate(
        block_grad(cells, grad_ref, q_ref, x_ref, stats_ref, sums_ref), axis=0
    )
    count = frames * cols * rows
    wide[...] = jnp.zeros_like(wide)
    for k in range(9):
        wide[k, 0 : 3 * lat] = k_ref[3 * k : 3 * k + 3].reshape(3 * lat, channels)
    row = lax.broadcasted_iota(jnp.int32, (count, 1), 0) % rows
    placed = {}
    for a in range(3):
        z = [nt_dot(grad, wide[3 * a + b]) for b in range(3)]
        up = jnp.where(row < rows - 1, pltpu.roll(z[0], count - 1, 0), 0.0)
        down = jnp.where(row > 0, pltpu.roll(z[2], 1, 0), 0.0)
        total = (z[1] + up + down).reshape(frames, cols, rows, lanes)
        for f in range(frames):
            out = total[f, 0]
            for w in range(1, cols):
                out = out + pltpu.roll(total[f, w], lat * w, 1)
            at = f + a - 2
            placed[at] = placed[at] + out if at in placed else out
    for f in range(frames):
        own_ref[f] = placed[f]
        prev_ref[f] = placed[f - 2]


def latent_section(grad, q, stored, stats, sums, kernel, cells):
    frames, cols, rows, channels = grad.shape
    lanes = 128
    out = jax.ShapeDtypeStruct((frames, rows, lanes), jnp.float32)
    return pl.pallas_call(
        functools.partial(latent_kernel_body, cells),
        out_shape=(out, out),
        in_specs=vmem(6),
        out_specs=tuple(vmem(2)),
        scratch_shapes=[pltpu.VMEM((9, lanes, channels), jnp.bfloat16)],
        compiler_params=pltpu.CompilerParams(vmem_limit_bytes=16 * MIB),
        name="latent",
    )(grad, q, stored, stats, sums, kernel)


def assemble_kernel(lat, cols, width, got_ref, e_ref, perm_ref, out_ref):
    peers, quad, lanes = got_ref.shape
    parts = {}
    for r in range(quad):
        hh, p = r // 2, r % 2
        spots = lax.dot_general(
            got_ref[:, r, :],
            e_ref[hh],
            (((0,), (0,)), ((), ())),
            precision=lax.Precision.HIGHEST,
            preferred_element_type=jnp.float32,
        )
        for col in range(cols + 2):
            q = (col + 1) % 2
            piece = spots[lat * col : lat * (col + 1), 128 * col : 128 * (col + 1)]
            parts[p, q] = parts[p, q] + piece if (p, q) in parts else piece
    stacked = jnp.concatenate([parts[p, q] for p in range(2) for q in range(2)], axis=0)
    out_ref[...] = exact_dot(perm_ref[...], stacked)[:, : out_ref.shape[1]]


def assemble(got, lat, cols):
    peers, quad, lanes = got.shape
    width = peers * cols // 2
    tokens = quad // 2 * width
    place = np.zeros((quad // 2, peers, (cols + 2) * 128), np.float32)
    for hh in range(quad // 2):
        for s in range(peers):
            for col in range(cols + 2):
                x = s * cols + col - 1
                if 0 <= x < peers * cols:
                    place[hh, s, 128 * col + hh * width + x // 2] = 1.0
    perm = np.zeros((4 * lat, 4 * lat), np.float32)
    for pq in range(4):
        for one in range(lat):
            perm[one * 4 + pq, pq * lat + one] = 1.0
    return pl.pallas_call(
        functools.partial(assemble_kernel, lat, cols, width),
        out_shape=jax.ShapeDtypeStruct((4 * lat, tokens), jnp.float32),
        in_specs=vmem(3),
        out_specs=pl.BlockSpec(memory_space=pltpu.VMEM),
        compiler_params=pltpu.CompilerParams(vmem_limit_bytes=8 * MIB),
        name="assemble",
    )(got, jnp.asarray(place), jnp.asarray(perm))


def pick(even, one, other):
    return jnp.where(even, one, other)


def exchange(value, send_a, send_b, even):
    tms = lax.axis_size("tm")
    tiles = lax.axis_size(TILE)
    cols = value.shape[1]
    back = [(t + 1, t) for t in range(tms - 1)]
    swap = [(0, 1), (1, 0)]
    hops = []
    for k in range(1, tiles - 1, 2):
        hops += [(k, k + 1), (k + 1, k)]
    diagonal = [((t + 1) * tiles + s, t * tiles + d) for t in range(tms - 1) for s, d in hops]
    nxt = lax.ppermute(value, "tm", back)
    rb = lax.ppermute(send_b, TILE, hops)
    rbn = lax.ppermute(send_b, TM_TILE, diagonal)
    ra = lax.ppermute(send_a, "tile_2", swap)
    ran = lax.ppermute(pick(even, nxt[:, cols - 1], nxt[:, 0]), "tile_2", swap)
    return nxt, ra, rb, ran, rbn


def everyone(rows):
    return lax.all_to_all(rows, TILE, 0, 0)


def shards(
    first_input,
    second_input,
    output_grad,
    first_gain,
    first_shift,
    first_kernel,
    second_gain,
    second_shift,
    second_kernel,
    latent_kernel,
):
    frames, rows, cols, channels = first_input.shape
    peers = lax.axis_size(TILE)
    cells = rows * cols * peers * (channels // GROUPS)
    core = lax.axis_index("tile_2")
    even = core == 0
    par = core.astype(jnp.int32).reshape(1)
    turn = lambda x: jnp.transpose(x, (0, 2, 1, 3))
    row = lambda x: x.reshape(1, channels)

    grad = turn(output_grad)
    halo = exchange(
        grad,
        pick(even, grad[:, cols - 1], grad[:, 0]),
        pick(even, grad[:, 0], grad[:, cols - 1]),
        even,
    )
    second, first = turn(second_input), turn(first_input)
    mom = everyone(moments(second, first, peers))
    q, sums, stats = conv_section(
        par, grad, halo, second, mom, row(second_gain), row(second_shift), second_kernel,
        cells, 0, peers,
    )
    grad, send_a, send_b = dx_section(par, grad, q, second, stats, everyone(sums), cells)
    halo = exchange(grad, send_a, send_b, even)
    q, sums, stats = conv_section(
        par, grad, halo, first, mom, row(first_gain), row(first_shift), first_kernel,
        cells, 2 * frames, peers,
    )
    own, prev = latent_section(grad, q, first, stats, everyone(sums), latent_kernel, cells)
    tms = lax.axis_size("tm")
    own = own + lax.ppermute(prev, "tm", [(t + 1, t) for t in range(tms - 1)])
    got = everyone(own.reshape(peers, frames * rows // peers, own.shape[-1]))
    return assemble(got, latent_kernel.shape[1], cols)


def solution(mesh):
    torus = Mesh(
        mesh.devices.reshape(mesh.shape["tm"], 4, 2, 2), ("tm", "tile_0", "tile_1", "tile_2")
    )
    block = P("tm", None, TILE, None)
    placed = (block, block, block) + (P(),) * 7
    return jax.shard_map(
        shards, mesh=torus, in_specs=placed, out_specs=P(None, TM_TILE), check_vma=False
    )
```

```python
import functools

import jax
import jax.numpy as jnp
import numpy as np
from jax import lax
from jax.experimental import pallas as pl
from jax.experimental.pallas import tpu as pltpu
from jax.experimental.layout import Layout, with_layout_constraint
from jax.sharding import Mesh
from jax.sharding import PartitionSpec as P

GROUPS = 32
TILE = ("tile_0", "tile_1", "tile_2")
TM_TILE = ("tm",) + TILE
EPSILON = 1e-05
MIB = 1 << 20


def vmem(count):
    return [pl.BlockSpec(memory_space=pltpu.VMEM)] * count


def nt_dot(left, right, **kw):
    return lax.dot_general(
        left, right, (((1,), (1,)), ((), ())), preferred_element_type=jnp.float32, **kw
    )


def thirds(value):
    high = value.astype(jnp.bfloat16)
    rest = value - high.astype(jnp.float32)
    middle = rest.astype(jnp.bfloat16)
    return high, middle, (rest - middle.astype(jnp.float32)).astype(jnp.bfloat16)


def group_sum(rows):
    count, channels = rows.shape
    per = channels // GROUPS
    row = lax.broadcasted_iota(jnp.int32, (channels, channels), 0) // per
    col = lax.broadcasted_iota(jnp.int32, (channels, channels), 1) // per
    same = jnp.where(row == col, 1.0, 0.0).astype(jnp.bfloat16)
    if count < 8:
        rows = jnp.concatenate([rows, jnp.zeros((8 - count, channels), jnp.float32)], axis=0)
    split = jnp.concatenate([part.astype(jnp.float32) for part in thirds(rows)], axis=0)
    sums = jnp.dot(split.astype(jnp.bfloat16), same, preferred_element_type=jnp.float32)
    return sums[0:count] + sums[8 : 8 + count] + sums[16 : 16 + count]


def spread(ref, rows):
    ref[...] = jnp.broadcast_to(rows[None], ref.shape)


def moments_kernel(second_ref, first_ref, out_ref):
    rows = []
    for ref in (second_ref, first_ref):
        frames = ref.shape[0]
        values = [ref[f].astype(jnp.float32) for f in range(frames)]
        rows += [jnp.sum(v, axis=(0, 1)).reshape(1, -1) for v in values]
        rows += [jnp.sum(v * v, axis=(0, 1)).reshape(1, -1) for v in values]
    spread(out_ref, jnp.concatenate(rows, axis=0))


def moments(second, first, peers):
    frames, _, _, channels = second.shape
    return pl.pallas_call(
        moments_kernel,
        out_shape=jax.ShapeDtypeStruct((peers, 4 * frames, channels), jnp.float32),
        in_specs=vmem(2),
        out_specs=pl.BlockSpec(memory_space=pltpu.VMEM),
        compiler_params=pltpu.CompilerParams(vmem_limit_bytes=8 * MIB),
        name="moments",
    )(second, first)


def conv_kernel(
    cells,
    base,
    par_ref,
    own_ref,
    next_ref,
    ra_ref,
    rb_ref,
    ran_ref,
    rbn_ref,
    x_ref,
    mom_ref,
    gain_ref,
    shift_ref,
    w_hbm,
    q_ref,
    sums_ref,
    stats_ref,
    ext,
    acc,
    wbuf,
    sems,
):
    frames, cols, rows, channels = own_ref.shape
    taps = 3
    copies = [
        pltpu.make_async_copy(
            w_hbm.at[pl.ds(taps * k, taps)], wbuf.at[pl.ds(taps * k, taps)], sems.at[k]
        )
        for k in range(9)
    ]
    for copy in copies:
        copy.start()
    even, side, later = par_ref[0] == 0, par_ref[1] == 1, par_ref[2] == 1
    zero = jnp.bfloat16(0)
    ext[0:frames, 1 : cols + 1] = own_ref[...]
    ext[frames : 2 * frames, 1 : cols + 1] = jnp.where(later, next_ref[...], zero)
    for at, a_ref, b_ref in ((0, ra_ref, rb_ref), (frames, ran_ref, rbn_ref)):
        a, b = a_ref[...], jnp.where(side, b_ref[...], zero)
        if at:
            a, b = jnp.where(later, a, zero), jnp.where(later, b, zero)
        ext[at : at + frames, 0] = jnp.where(even, b, a)
        ext[at : at + frames, cols + 1] = jnp.where(even, a, b)
    count = frames * cols * rows
    for a in range(3):
        left = jnp.concatenate(
            [
                ext[2 - a : 2 - a + frames, 2 - c : 2 - c + cols].reshape(count, channels)
                for c in range(3)
            ],
            axis=1,
        )
        for b in range(3):
            k = 3 * a + b
            copies[k].wait()
            right = jnp.concatenate([wbuf[3 * k + c] for c in range(3)], axis=1)
            part = nt_dot(left, right)
            acc[b] = part if a == 0 else acc[b] + part
    row = lax.broadcasted_iota(jnp.int32, (count, 1), 0) % rows
    up = jnp.where(row < rows - 1, pltpu.roll(acc[0], count - 1, 0), 0.0)
    down = jnp.where(row > 0, pltpu.roll(acc[2], 1, 0), 0.0)
    upstream = acc[1] + up + down

    totals = group_sum(jnp.sum(mom_ref[...], axis=0)) * (1.0 / cells)
    gain, shift = gain_ref[...].reshape(1, channels), shift_ref[...].reshape(1, channels)
    sums, crosses, means, scales = [], [], [], []
    half = count // frames
    for f in range(frames):
        mean = totals[base + f : base + f + 1]
        var = totals[base + frames + f : base + frames + f + 1] - mean * mean
        scale = lax.rsqrt(var + EPSILON)
        normed = (x_ref[f].astype(jnp.float32).reshape(half, channels) - mean) * scale
        pre = normed * gain + shift
        sig = jax.nn.sigmoid(pre)
        q = upstream[f * half : (f + 1) * half] * sig * (1.0 + pre * (1.0 - sig)) * gain
        q_ref[f] = q.reshape(cols, rows, channels)
        sums.append(jnp.sum(q, axis=0, keepdims=True))
        crosses.append(jnp.sum(q * normed, axis=0, keepdims=True))
        means.append(mean)
        scales.append(scale)
    spread(sums_ref, jnp.concatenate(sums + crosses, axis=0))
    stats_ref[...] = jnp.concatenate(means + scales, axis=0)


def conv_section(par, grad, halo, stored, mom, gain, shift, kernel, cells, base, peers):
    frames, cols, rows, channels = grad.shape
    nxt, ra, rb, ran, rbn = halo
    hbm = pl.BlockSpec(memory_space=pltpu.HBM)
    return pl.pallas_call(
        functools.partial(conv_kernel, cells, base),
        out_shape=(
            jax.ShapeDtypeStruct(grad.shape, jnp.float32),
            jax.ShapeDtypeStruct((peers, 2 * frames, channels), jnp.float32),
            jax.ShapeDtypeStruct((2 * frames, channels), jnp.float32),
        ),
        in_specs=[pl.BlockSpec(memory_space=pltpu.SMEM)] + vmem(10) + [hbm],
        out_specs=tuple(vmem(3)),
        scratch_shapes=[
            pltpu.VMEM((2 * frames, cols + 2, rows, channels), jnp.bfloat16),
            pltpu.VMEM((3, frames * cols * rows, channels), jnp.float32),
            pltpu.VMEM(kernel.shape, jnp.bfloat16),
            pltpu.SemaphoreType.DMA((9,)),
        ],
        compiler_params=pltpu.CompilerParams(vmem_limit_bytes=32 * MIB),
        name="conv",
    )(par, grad, nxt, ra, rb, ran, rbn, stored, mom, gain, shift, kernel)


def block_grad(cells, grad_ref, q_ref, x_ref, stats_ref, sums_ref):
    frames, cols, rows, channels = grad_ref.shape
    totals = group_sum(jnp.sum(sums_ref[...], axis=0)) * (1.0 / cells)
    result = []
    for f in range(frames):
        mean = stats_ref[f : f + 1]
        scale = stats_ref[frames + f : frames + f + 1]
        flat = (cols * rows, channels)
        normed = (x_ref[f].astype(jnp.float32).reshape(flat) - mean) * scale
        value = grad_ref[f].astype(jnp.float32).reshape(flat) + scale * (
            q_ref[f].reshape(flat)
            - totals[f : f + 1]
            - normed * totals[frames + f : frames + f + 1]
        )
        result.append(value.astype(jnp.bfloat16))
    return result


def dx_kernel(cells, par_ref, grad_ref, q_ref, x_ref, stats_ref, sums_ref, dx_ref, sa_ref, sb_ref):
    frames, cols, rows, channels = grad_ref.shape
    even = par_ref[0] == 0
    for f, value in enumerate(block_grad(cells, grad_ref, q_ref, x_ref, stats_ref, sums_ref)):
        value = value.reshape(cols, rows, channels)
        dx_ref[f] = value
        sa_ref[f] = jnp.where(even, value[cols - 1], value[0])
        sb_ref[f] = jnp.where(even, value[0], value[cols - 1])


def dx_section(par, grad, q, stored, stats, sums, cells):
    frames, cols, rows, channels = grad.shape
    edge = jax.ShapeDtypeStruct((frames, rows, channels), jnp.bfloat16)
    return pl.pallas_call(
        functools.partial(dx_kernel, cells),
        out_shape=(jax.ShapeDtypeStruct(grad.shape, jnp.bfloat16), edge, edge),
        in_specs=[pl.BlockSpec(memory_space=pltpu.SMEM)] + vmem(5),
        out_specs=tuple(vmem(3)),
        compiler_params=pltpu.CompilerParams(vmem_limit_bytes=8 * MIB),
        name="dx",
    )(par, grad, q, stored, stats, sums)


def latent_kernel_body(cells, grad_ref, q_ref, x_ref, stats_ref, sums_ref, k_ref, own_ref, prev_ref, wide):
    frames, cols, rows, channels = grad_ref.shape
    lat = k_ref.shape[1]
    lanes = wide.shape[1]
    grad = jnp.concatenate(
        block_grad(cells, grad_ref, q_ref, x_ref, stats_ref, sums_ref), axis=0
    )
    count = frames * cols * rows
    wide[...] = jnp.zeros_like(wide)
    for k in range(9):
        wide[k, 0 : 3 * lat] = k_ref[3 * k : 3 * k + 3].reshape(3 * lat, channels)
    row = lax.broadcasted_iota(jnp.int32, (count, 1), 0) % rows
    placed = {}
    for a in range(3):
        z = [nt_dot(grad, wide[3 * a + b]) for b in range(3)]
        up = jnp.where(row < rows - 1, pltpu.roll(z[0], count - 1, 0), 0.0)
        down = jnp.where(row > 0, pltpu.roll(z[2], 1, 0), 0.0)
        total = (z[1] + up + down).reshape(frames, cols, rows, lanes)
        for f in range(frames):
            out = total[f, 0]
            for w in range(1, cols):
                out = out + pltpu.roll(total[f, w], lat * w, 1)
            at = f + a - 2
            placed[at] = placed[at] + out if at in placed else out
    for f in range(frames):
        own_ref[f] = placed[f]
        prev_ref[f] = placed[f - 2]


def latent_section(grad, q, stored, stats, sums, kernel, cells):
    frames, cols, rows, channels = grad.shape
    lanes = 128
    out = jax.ShapeDtypeStruct((frames, rows, lanes), jnp.float32)
    return pl.pallas_call(
        functools.partial(latent_kernel_body, cells),
        out_shape=(out, out),
        in_specs=vmem(6),
        out_specs=tuple(vmem(2)),
        scratch_shapes=[pltpu.VMEM((9, lanes, channels), jnp.bfloat16)],
        compiler_params=pltpu.CompilerParams(vmem_limit_bytes=16 * MIB),
        name="latent",
    )(grad, q, stored, stats, sums, kernel)


def assemble_kernel(lat, cols, got_ref, e_ref, perm_ref, out_ref):
    peers, quad, lanes = got_ref.shape
    parts = {}
    for p in range(2):
        rows = jnp.concatenate([got_ref[:, p, :], got_ref[:, 2 + p, :]], axis=0)
        spots = lax.dot_general(
            jnp.concatenate(thirds(rows), axis=0),
            e_ref[...],
            (((0,), (0,)), ((), ())),
            preferred_element_type=jnp.float32,
        )
        for col in range(cols + 2):
            q = (col + 1) % 2
            piece = spots[lat * col : lat * (col + 1), 128 * col : 128 * (col + 1)]
            parts[p, q] = parts[p, q] + piece if (p, q) in parts else piece
    stacked = jnp.concatenate([parts[p, q] for p in range(2) for q in range(2)], axis=0)
    final = jnp.dot(
        perm_ref[...],
        jnp.concatenate(thirds(stacked), axis=0),
        preferred_element_type=jnp.float32,
    )
    out_ref[...] = final[:, : out_ref.shape[1]]


def assemble(got, lat, cols):
    peers, quad, lanes = got.shape
    width = peers * cols // 2
    tokens = quad // 2 * width
    place = np.zeros((quad // 2, peers, (cols + 2) * 128), np.float32)
    for hh in range(quad // 2):
        for s in range(peers):
            for col in range(cols + 2):
                x = s * cols + col - 1
                if 0 <= x < peers * cols:
                    place[hh, s, 128 * col + hh * width + x // 2] = 1.0
    place = np.tile(place.reshape(-1, place.shape[-1]), (3, 1))
    perm = np.zeros((4 * lat, 4 * lat), np.float32)
    for pq in range(4):
        for one in range(lat):
            perm[one * 4 + pq, pq * lat + one] = 1.0
    perm = np.tile(perm, (1, 3))
    return pl.pallas_call(
        functools.partial(assemble_kernel, lat, cols),
        out_shape=jax.ShapeDtypeStruct((4 * lat, tokens), jnp.float32),
        in_specs=vmem(3),
        out_specs=pl.BlockSpec(memory_space=pltpu.VMEM),
        compiler_params=pltpu.CompilerParams(vmem_limit_bytes=8 * MIB),
        name="assemble",
    )(got, jnp.asarray(place, jnp.bfloat16), jnp.asarray(perm, jnp.bfloat16))


def pick(even, one, other):
    return jnp.where(even, one, other)


def exchange(value, send_a, send_b, even):
    tms = lax.axis_size("tm")
    tiles = lax.axis_size(TILE)
    cols = value.shape[1]
    back = ring(tms)
    swap = [(0, 1), (1, 0)]
    hops = []
    for k in range(1, tiles, 2):
        hops += [(k, (k + 1) % tiles), ((k + 1) % tiles, k)]
    diagonal = [(t * tiles + s, u * tiles + d) for t, u in back for s, d in hops]
    nxt = lax.ppermute(value, "tm", back)
    rb = lax.ppermute(send_b, TILE, hops)
    rbn = lax.ppermute(send_b, TM_TILE, diagonal)
    ra = lax.ppermute(send_a, "tile_2", swap)
    ran = lax.ppermute(pick(even, nxt[:, cols - 1], nxt[:, 0]), "tile_2", swap)
    return nxt, ra, rb, ran, rbn


def ring(count):
    return [(t, (t - 1) % count) for t in range(count)]


def everyone(rows):
    return lax.all_to_all(rows, TILE, 0, 0)


def shards(
    first_input,
    second_input,
    output_grad,
    first_gain,
    first_shift,
    first_kernel,
    second_gain,
    second_shift,
    second_kernel,
    latent_kernel,
):
    frames, rows, cols, channels = first_input.shape
    peers = lax.axis_size(TILE)
    cells = rows * cols * peers * (channels // GROUPS)
    core = lax.axis_index("tile_2")
    even = core == 0
    tile, when = lax.axis_index(TILE), lax.axis_index("tm")
    later = when < lax.axis_size("tm") - 1
    side = jnp.where(even, tile > 0, tile < peers - 1)
    par = jnp.stack([core.astype(jnp.int32), side.astype(jnp.int32), later.astype(jnp.int32)])
    turn = lambda x: with_layout_constraint(
        jnp.transpose(x, (0, 2, 1, 3)), Layout(major_to_minor=(0, 1, 2, 3))
    )

    grad = turn(output_grad)
    halo = exchange(
        grad,
        pick(even, grad[:, cols - 1], grad[:, 0]),
        pick(even, grad[:, 0], grad[:, cols - 1]),
        even,
    )
    mom = everyone(moments(second_input, first_input, peers))
    second, first = turn(second_input), turn(first_input)
    q, sums, stats = conv_section(
        par, grad, halo, second, mom, second_gain, second_shift, second_kernel,
        cells, 0, peers,
    )
    grad, send_a, send_b = dx_section(par, grad, q, second, stats, everyone(sums), cells)
    halo = exchange(grad, send_a, send_b, even)
    q, sums, stats = conv_section(
        par, grad, halo, first, mom, first_gain, first_shift, first_kernel,
        cells, 2 * frames, peers,
    )
    own, prev = latent_section(grad, q, first, stats, everyone(sums), latent_kernel, cells)
    tms = lax.axis_size("tm")
    own = own + jnp.where(later, lax.ppermute(prev, "tm", ring(tms)), 0.0)
    got = everyone(own.reshape(peers, frames * rows // peers, own.shape[-1]))
    return assemble(got, latent_kernel.shape[1], cols)


def solution(mesh):
    torus = Mesh(
        mesh.devices.reshape(mesh.shape["tm"], 4, 2, 2), ("tm", "tile_0", "tile_1", "tile_2")
    )
    block = P("tm", None, TILE, None)
    placed = (block, block, block) + (P(),) * 7
    return jax.shard_map(
        shards, mesh=torus, in_specs=placed, out_specs=P(None, TM_TILE), check_vma=False
    )
```

```python
import functools

import jax
import jax.numpy as jnp
import numpy as np
from jax import lax
from jax.experimental import pallas as pl
from jax.experimental.pallas import tpu as pltpu
from jax.experimental.layout import Layout, with_layout_constraint
from jax.sharding import Mesh
from jax.sharding import PartitionSpec as P

GROUPS = 32
TILE = ("tile_0", "tile_1", "tile_2")
TM_TILE = ("tm",) + TILE
EPSILON = 1e-05
MIB = 1 << 20


def vmem(count):
    return [pl.BlockSpec(memory_space=pltpu.VMEM)] * count


def in_hbm(value):
    return pltpu.with_memory_space_constraint(value, pltpu.HBM)


def nt_dot(left, right, **kw):
    return lax.dot_general(
        left, right, (((1,), (1,)), ((), ())), preferred_element_type=jnp.float32, **kw
    )


def thirds(value):
    high = value.astype(jnp.bfloat16)
    rest = value - high.astype(jnp.float32)
    middle = rest.astype(jnp.bfloat16)
    return high, middle, (rest - middle.astype(jnp.float32)).astype(jnp.bfloat16)


def group_sum(rows):
    count, channels = rows.shape
    per = channels // GROUPS
    row = lax.broadcasted_iota(jnp.int32, (channels, channels), 0) // per
    col = lax.broadcasted_iota(jnp.int32, (channels, channels), 1) // per
    same = jnp.where(row == col, 1.0, 0.0).astype(jnp.bfloat16)
    if count < 8:
        rows = jnp.concatenate([rows, jnp.zeros((8 - count, channels), jnp.float32)], axis=0)
    split = jnp.concatenate([part.astype(jnp.float32) for part in thirds(rows)], axis=0)
    sums = jnp.dot(split.astype(jnp.bfloat16), same, preferred_element_type=jnp.float32)
    return sums[0:count] + sums[8 : 8 + count] + sums[16 : 16 + count]


def spread(ref, rows):
    ref[...] = jnp.broadcast_to(rows[None], ref.shape)


def moments_kernel(second_hbm, first_hbm, out_ref, second_ref, first_ref, sems):
    pairs = ((second_hbm, second_ref), (first_hbm, first_ref))
    copies = [pltpu.make_async_copy(*pair, sems.at[k]) for k, pair in enumerate(pairs)]
    for copy in copies:
        copy.start()
    rows = []
    for copy, (_, ref) in zip(copies, pairs):
        copy.wait()
        frames = ref.shape[0]
        values = [ref[f].astype(jnp.float32) for f in range(frames)]
        rows += [jnp.sum(v, axis=(0, 1)).reshape(1, -1) for v in values]
        rows += [jnp.sum(v * v, axis=(0, 1)).reshape(1, -1) for v in values]
    spread(out_ref, jnp.concatenate(rows, axis=0))


def moments(second, first, peers):
    frames, _, _, channels = second.shape
    return pl.pallas_call(
        moments_kernel,
        out_shape=jax.ShapeDtypeStruct((peers, 4 * frames, channels), jnp.float32),
        in_specs=[pl.BlockSpec(memory_space=pltpu.HBM)] * 2,
        out_specs=pl.BlockSpec(memory_space=pltpu.VMEM),
        scratch_shapes=[
            pltpu.VMEM(second.shape, jnp.bfloat16),
            pltpu.VMEM(first.shape, jnp.bfloat16),
            pltpu.SemaphoreType.DMA((2,)),
        ],
        compiler_params=pltpu.CompilerParams(vmem_limit_bytes=8 * MIB),
        name="moments",
    )(in_hbm(second), in_hbm(first))


def conv_kernel(
    cells,
    base,
    par_ref,
    own_ref,
    next_ref,
    ra_ref,
    rb_ref,
    ran_ref,
    rbn_ref,
    x_ref,
    mom_ref,
    gain_hbm,
    shift_hbm,
    w_hbm,
    q_ref,
    sums_ref,
    stats_ref,
    ext,
    acc,
    wbuf,
    gain_ref,
    shift_ref,
    sems,
):
    frames, cols, rows, channels = own_ref.shape
    copies = {
        a: pltpu.make_async_copy(
            w_hbm.at[pl.ds(9 * a, 9)], wbuf.at[pl.ds(9 * a, 9)], sems.at[a]
        )
        for a in (2, 1, 0)
    }
    for copy in copies.values():
        copy.start()
    affine = [
        pltpu.make_async_copy(src, dst, sems.at[3 + k])
        for k, (src, dst) in enumerate(((gain_hbm, gain_ref), (shift_hbm, shift_ref)))
    ]
    for copy in affine:
        copy.start()
    even, side, later = par_ref[0] == 0, par_ref[1] == 1, par_ref[2] == 1
    zero = jnp.bfloat16(0)
    ext[0:frames, 1 : cols + 1] = own_ref[...]
    ext[frames : 2 * frames, 1 : cols + 1] = jnp.where(later, next_ref[...], zero)
    for at, a_ref, b_ref in ((0, ra_ref, rb_ref), (frames, ran_ref, rbn_ref)):
        a, b = a_ref[...], jnp.where(side, b_ref[...], zero)
        if at:
            a, b = jnp.where(later, a, zero), jnp.where(later, b, zero)
        ext[at : at + frames, 0] = jnp.where(even, b, a)
        ext[at : at + frames, cols + 1] = jnp.where(even, a, b)
    count = frames * cols * rows
    for a in (2, 1, 0):
        left = jnp.concatenate(
            [
                ext[2 - a : 2 - a + frames, 2 - c : 2 - c + cols].reshape(count, channels)
                for c in range(3)
            ],
            axis=1,
        )
        copies[a].wait()
        right = jnp.concatenate(
            [
                jnp.concatenate([wbuf[9 * a + 3 * b + c] for c in range(3)], axis=1)
                for b in range(3)
            ],
            axis=0,
        )
        part = nt_dot(left, right)
        acc[...] = part if a == 2 else acc[...] + part
    row = lax.broadcasted_iota(jnp.int32, (count, 1), 0) % rows
    up = jnp.where(row < rows - 1, pltpu.roll(acc[:, :channels], count - 1, 0), 0.0)
    down = jnp.where(row > 0, pltpu.roll(acc[:, 2 * channels :], 1, 0), 0.0)
    upstream = acc[:, channels : 2 * channels] + up + down

    totals = group_sum(jnp.sum(mom_ref[...], axis=0)) * (1.0 / cells)
    for copy in affine:
        copy.wait()
    gain, shift = gain_ref[...].reshape(1, channels), shift_ref[...].reshape(1, channels)
    sums, crosses, means, scales = [], [], [], []
    half = count // frames
    for f in range(frames):
        mean = totals[base + f : base + f + 1]
        var = totals[base + frames + f : base + frames + f + 1] - mean * mean
        scale = lax.rsqrt(var + EPSILON)
        normed = (x_ref[f].astype(jnp.float32).reshape(half, channels) - mean) * scale
        pre = normed * gain + shift
        sig = jax.nn.sigmoid(pre)
        q = upstream[f * half : (f + 1) * half] * sig * (1.0 + pre * (1.0 - sig)) * gain
        q_ref[f] = q.reshape(cols, rows, channels)
        sums.append(jnp.sum(q, axis=0, keepdims=True))
        crosses.append(jnp.sum(q * normed, axis=0, keepdims=True))
        means.append(mean)
        scales.append(scale)
    spread(sums_ref, jnp.concatenate(sums + crosses, axis=0))
    stats_ref[...] = jnp.concatenate(means + scales, axis=0)


def conv_section(par, grad, halo, stored, mom, gain, shift, kernel, cells, base, peers):
    frames, cols, rows, channels = grad.shape
    nxt, ra, rb, ran, rbn = halo
    hbm = pl.BlockSpec(memory_space=pltpu.HBM)
    return pl.pallas_call(
        functools.partial(conv_kernel, cells, base),
        out_shape=(
            jax.ShapeDtypeStruct(grad.shape, jnp.float32),
            jax.ShapeDtypeStruct((peers, 2 * frames, channels), jnp.float32),
            jax.ShapeDtypeStruct((2 * frames, channels), jnp.float32),
        ),
        in_specs=[pl.BlockSpec(memory_space=pltpu.SMEM)] + vmem(8) + [hbm] * 3,
        out_specs=tuple(vmem(3)),
        scratch_shapes=[
            pltpu.VMEM((2 * frames, cols + 2, rows, channels), jnp.bfloat16),
            pltpu.VMEM((frames * cols * rows, 3 * channels), jnp.float32),
            pltpu.VMEM(kernel.shape, jnp.bfloat16),
            pltpu.VMEM(gain.shape, jnp.float32),
            pltpu.VMEM(shift.shape, jnp.float32),
            pltpu.SemaphoreType.DMA((5,)),
        ],
        compiler_params=pltpu.CompilerParams(vmem_limit_bytes=32 * MIB),
        name="conv",
    )(par, grad, nxt, ra, rb, ran, rbn, stored, mom, *map(in_hbm, (gain, shift, kernel)))


def block_grad(cells, grad_ref, q_ref, x_ref, stats_ref, sums_ref):
    frames, cols, rows, channels = grad_ref.shape
    totals = group_sum(jnp.sum(sums_ref[...], axis=0)) * (1.0 / cells)
    result = []
    for f in range(frames):
        mean = stats_ref[f : f + 1]
        scale = stats_ref[frames + f : frames + f + 1]
        flat = (cols * rows, channels)
        normed = (x_ref[f].astype(jnp.float32).reshape(flat) - mean) * scale
        value = grad_ref[f].astype(jnp.float32).reshape(flat) + scale * (
            q_ref[f].reshape(flat)
            - totals[f : f + 1]
            - normed * totals[frames + f : frames + f + 1]
        )
        result.append(value.astype(jnp.bfloat16))
    return result


def dx_kernel(cells, par_ref, grad_ref, q_ref, x_ref, stats_ref, sums_ref, dx_ref, sa_ref, sb_ref):
    frames, cols, rows, channels = grad_ref.shape
    even = par_ref[0] == 0
    for f, value in enumerate(block_grad(cells, grad_ref, q_ref, x_ref, stats_ref, sums_ref)):
        value = value.reshape(cols, rows, channels)
        dx_ref[f] = value
        sa_ref[f] = jnp.where(even, value[cols - 1], value[0])
        sb_ref[f] = jnp.where(even, value[0], value[cols - 1])


def dx_section(par, grad, q, stored, stats, sums, cells):
    frames, cols, rows, channels = grad.shape
    edge = jax.ShapeDtypeStruct((frames, rows, channels), jnp.bfloat16)
    return pl.pallas_call(
        functools.partial(dx_kernel, cells),
        out_shape=(jax.ShapeDtypeStruct(grad.shape, jnp.bfloat16), edge, edge),
        in_specs=[pl.BlockSpec(memory_space=pltpu.SMEM)] + vmem(5),
        out_specs=tuple(vmem(3)),
        compiler_params=pltpu.CompilerParams(vmem_limit_bytes=8 * MIB),
        name="dx",
    )(par, grad, q, stored, stats, sums)


def latent_kernel_body(cells, grad_ref, q_ref, x_ref, stats_ref, sums_ref, k_ref, own_ref, prev_ref, wide):
    frames, cols, rows, channels = grad_ref.shape
    lat = k_ref.shape[1]
    lanes = wide.shape[1]
    grad = jnp.concatenate(
        block_grad(cells, grad_ref, q_ref, x_ref, stats_ref, sums_ref), axis=0
    )
    count = frames * cols * rows
    wide[...] = jnp.zeros_like(wide)
    for k in range(9):
        wide[k, 0 : 3 * lat] = k_ref[3 * k : 3 * k + 3].reshape(3 * lat, channels)
    row = lax.broadcasted_iota(jnp.int32, (count, 1), 0) % rows
    placed = {}
    for a in range(3):
        z = [nt_dot(grad, wide[3 * a + b]) for b in range(3)]
        up = jnp.where(row < rows - 1, pltpu.roll(z[0], count - 1, 0), 0.0)
        down = jnp.where(row > 0, pltpu.roll(z[2], 1, 0), 0.0)
        total = (z[1] + up + down).reshape(frames, cols, rows, lanes)
        for f in range(frames):
            out = total[f, 0]
            for w in range(1, cols):
                out = out + pltpu.roll(total[f, w], lat * w, 1)
            at = f + a - 2
            placed[at] = placed[at] + out if at in placed else out
    for f in range(frames):
        own_ref[f] = placed[f]
        prev_ref[f] = placed[f - 2]


def latent_section(grad, q, stored, stats, sums, kernel, cells):
    frames, cols, rows, channels = grad.shape
    lanes = 128
    out = jax.ShapeDtypeStruct((frames, rows, lanes), jnp.float32)
    return pl.pallas_call(
        functools.partial(latent_kernel_body, cells),
        out_shape=(out, out),
        in_specs=vmem(6),
        out_specs=tuple(vmem(2)),
        scratch_shapes=[pltpu.VMEM((9, lanes, channels), jnp.bfloat16)],
        compiler_params=pltpu.CompilerParams(vmem_limit_bytes=16 * MIB),
        name="latent",
    )(grad, q, stored, stats, sums, kernel)


def assemble_kernel(lat, cols, got_ref, e_ref, perm_ref, out_ref):
    peers, quad, lanes = got_ref.shape
    parts = {}
    for p in range(2):
        rows = jnp.concatenate([got_ref[:, p, :], got_ref[:, 2 + p, :]], axis=0)
        spots = lax.dot_general(
            jnp.concatenate(thirds(rows), axis=0),
            e_ref[...],
            (((0,), (0,)), ((), ())),
            preferred_element_type=jnp.float32,
        )
        for col in range(cols + 2):
            q = (col + 1) % 2
            piece = spots[lat * col : lat * (col + 1), 128 * col : 128 * (col + 1)]
            parts[p, q] = parts[p, q] + piece if (p, q) in parts else piece
    stacked = jnp.concatenate([parts[p, q] for p in range(2) for q in range(2)], axis=0)
    final = jnp.dot(
        perm_ref[...],
        jnp.concatenate(thirds(stacked), axis=0),
        preferred_element_type=jnp.float32,
    )
    out_ref[...] = final[:, : out_ref.shape[1]]


def assemble(got, lat, cols):
    peers, quad, lanes = got.shape
    width = peers * cols // 2
    tokens = quad // 2 * width
    place = np.zeros((quad // 2, peers, (cols + 2) * 128), np.float32)
    for hh in range(quad // 2):
        for s in range(peers):
            for col in range(cols + 2):
                x = s * cols + col - 1
                if 0 <= x < peers * cols:
                    place[hh, s, 128 * col + hh * width + x // 2] = 1.0
    place = np.tile(place.reshape(-1, place.shape[-1]), (3, 1))
    perm = np.zeros((4 * lat, 4 * lat), np.float32)
    for pq in range(4):
        for one in range(lat):
            perm[one * 4 + pq, pq * lat + one] = 1.0
    perm = np.tile(perm, (1, 3))
    return pl.pallas_call(
        functools.partial(assemble_kernel, lat, cols),
        out_shape=jax.ShapeDtypeStruct((4 * lat, tokens), jnp.float32),
        in_specs=vmem(3),
        out_specs=pl.BlockSpec(memory_space=pltpu.VMEM),
        compiler_params=pltpu.CompilerParams(vmem_limit_bytes=8 * MIB),
        name="assemble",
    )(got, jnp.asarray(place, jnp.bfloat16), jnp.asarray(perm, jnp.bfloat16))


def pick(even, one, other):
    return jnp.where(even, one, other)


def exchange(value, send_a, send_b, even):
    tms = lax.axis_size("tm")
    tiles = lax.axis_size(TILE)
    cols = value.shape[1]
    back = ring(tms)
    swap = [(0, 1), (1, 0)]
    hops = []
    for k in range(1, tiles, 2):
        hops += [(k, (k + 1) % tiles), ((k + 1) % tiles, k)]
    diagonal = [(t * tiles + s, u * tiles + d) for t, u in back for s, d in hops]
    nxt = lax.ppermute(value, "tm", back)
    rb = lax.ppermute(send_b, TILE, hops)
    rbn = lax.ppermute(send_b, TM_TILE, diagonal)
    ra = lax.ppermute(send_a, "tile_2", swap)
    ran = lax.ppermute(pick(even, nxt[:, cols - 1], nxt[:, 0]), "tile_2", swap)
    return nxt, ra, rb, ran, rbn


def ring(count):
    return [(t, (t - 1) % count) for t in range(count)]


def everyone(rows):
    return lax.all_to_all(rows, TILE, 0, 0)


def shards(
    first_input,
    second_input,
    output_grad,
    first_gain,
    first_shift,
    first_kernel,
    second_gain,
    second_shift,
    second_kernel,
    latent_kernel,
):
    frames, rows, cols, channels = first_input.shape
    peers = lax.axis_size(TILE)
    cells = rows * cols * peers * (channels // GROUPS)
    core = lax.axis_index("tile_2")
    even = core == 0
    tile, when = lax.axis_index(TILE), lax.axis_index("tm")
    later = when < lax.axis_size("tm") - 1
    side = jnp.where(even, tile > 0, tile < peers - 1)
    par = jnp.stack([core.astype(jnp.int32), side.astype(jnp.int32), later.astype(jnp.int32)])
    turn = lambda x: with_layout_constraint(
        jnp.transpose(x, (0, 2, 1, 3)), Layout(major_to_minor=(0, 1, 2, 3))
    )

    grad = turn(output_grad)
    halo = exchange(
        grad,
        pick(even, grad[:, cols - 1], grad[:, 0]),
        pick(even, grad[:, 0], grad[:, cols - 1]),
        even,
    )
    mom = everyone(moments(second_input, first_input, peers))
    second, first = turn(second_input), turn(first_input)
    q, sums, stats = conv_section(
        par, grad, halo, second, mom, second_gain, second_shift, second_kernel,
        cells, 0, peers,
    )
    grad, send_a, send_b = dx_section(par, grad, q, second, stats, everyone(sums), cells)
    halo = exchange(grad, send_a, send_b, even)
    q, sums, stats = conv_section(
        par, grad, halo, first, mom, first_gain, first_shift, first_kernel,
        cells, 2 * frames, peers,
    )
    own, prev = latent_section(grad, q, first, stats, everyone(sums), latent_kernel, cells)
    tms = lax.axis_size("tm")
    own = own + jnp.where(later, lax.ppermute(prev, "tm", ring(tms)), 0.0)
    got = everyone(own.reshape(peers, frames * rows // peers, own.shape[-1]))
    return assemble(got, latent_kernel.shape[1], cols)


def solution(mesh):
    torus = Mesh(
        mesh.devices.reshape(mesh.shape["tm"], 4, 2, 2), ("tm", "tile_0", "tile_1", "tile_2")
    )
    block = P("tm", None, TILE, None)
    placed = (block, block, block) + (P(),) * 7
    return jax.shard_map(
        shards, mesh=torus, in_specs=placed, out_specs=P(None, TM_TILE), check_vma=False
    )
```

```python
import functools

import jax
import jax.numpy as jnp
import numpy as np
from jax import lax
from jax.experimental import pallas as pl
from jax.experimental.pallas import tpu as pltpu
from jax.experimental.layout import Layout, with_layout_constraint
from jax.sharding import Mesh
from jax.sharding import PartitionSpec as P

GROUPS = 32
TILE = ("tile_0", "tile_1", "tile_2")
TM_TILE = ("tm",) + TILE
EPSILON = 1e-05
MIB = 1 << 20


def vmem(count):
    return [pl.BlockSpec(memory_space=pltpu.VMEM)] * count


HBM = [pl.BlockSpec(memory_space=pltpu.HBM)]


def matmul_cost(count, kernel):
    return pl.CostEstimate(
        flops=2 * count * kernel.size, bytes_accessed=2 * kernel.size, transcendentals=0
    )


def in_hbm(value):
    return pltpu.with_memory_space_constraint(value, pltpu.HBM)


def nt_dot(left, right, **kw):
    return lax.dot_general(
        left, right, (((1,), (1,)), ((), ())), preferred_element_type=jnp.float32, **kw
    )


def thirds(value):
    high = value.astype(jnp.bfloat16)
    rest = value - high.astype(jnp.float32)
    middle = rest.astype(jnp.bfloat16)
    return high, middle, (rest - middle.astype(jnp.float32)).astype(jnp.bfloat16)


def group_sum(rows):
    count, channels = rows.shape
    per = channels // GROUPS
    row = lax.broadcasted_iota(jnp.int32, (channels, channels), 0) // per
    col = lax.broadcasted_iota(jnp.int32, (channels, channels), 1) // per
    same = jnp.where(row == col, 1.0, 0.0).astype(jnp.bfloat16)
    if count < 8:
        rows = jnp.concatenate([rows, jnp.zeros((8 - count, channels), jnp.float32)], axis=0)
    split = jnp.concatenate([part.astype(jnp.float32) for part in thirds(rows)], axis=0)
    sums = jnp.dot(split.astype(jnp.bfloat16), same, preferred_element_type=jnp.float32)
    return sums[0:count] + sums[8 : 8 + count] + sums[16 : 16 + count]


def spread(ref, rows):
    ref[...] = jnp.broadcast_to(rows[None], ref.shape)


def moments_kernel(second_hbm, first_hbm, out_ref, second_ref, first_ref, sems):
    pairs = ((second_hbm, second_ref), (first_hbm, first_ref))
    copies = [pltpu.make_async_copy(*pair, sems.at[k]) for k, pair in enumerate(pairs)]
    for copy in copies:
        copy.start()
    rows = []
    for copy, (_, ref) in zip(copies, pairs):
        copy.wait()
        frames = ref.shape[0]
        values = [ref[f].astype(jnp.float32) for f in range(frames)]
        rows += [jnp.sum(v, axis=(0, 1)).reshape(1, -1) for v in values]
        rows += [jnp.sum(v * v, axis=(0, 1)).reshape(1, -1) for v in values]
    spread(out_ref, jnp.concatenate(rows, axis=0))


def moments(second, first, peers):
    frames, _, _, channels = second.shape
    return pl.pallas_call(
        moments_kernel,
        out_shape=jax.ShapeDtypeStruct((peers, 4 * frames, channels), jnp.float32),
        in_specs=[pl.BlockSpec(memory_space=pltpu.HBM)] * 2,
        out_specs=pl.BlockSpec(memory_space=pltpu.VMEM),
        scratch_shapes=[
            pltpu.VMEM(second.shape, jnp.bfloat16),
            pltpu.VMEM(first.shape, jnp.bfloat16),
            pltpu.SemaphoreType.DMA((2,)),
        ],
        compiler_params=pltpu.CompilerParams(vmem_limit_bytes=8 * MIB),
        name="moments",
    )(in_hbm(second), in_hbm(first))


def fill(ext, at, block, a, b, even):
    frames, cols = block.shape[:2]
    ext[at : at + frames, 1 : cols + 1] = block
    ext[at : at + frames, 0] = jnp.where(even, b, a)
    ext[at : at + frames, cols + 1] = jnp.where(even, a, b)


def time_tap(ext, wbuf, a, slot, frames, cols):
    rows, channels = ext.shape[2:]
    left = jnp.concatenate(
        [
            ext[2 - a : 2 - a + frames, 2 - c : 2 - c + cols].reshape(-1, channels)
            for c in range(3)
        ],
        axis=1,
    )
    right = jnp.concatenate(
        [
            jnp.concatenate([wbuf[9 * slot + 3 * b + c] for c in range(3)], axis=1)
            for b in range(3)
        ],
        axis=0,
    )
    return nt_dot(left, right)


def row_taps(wide, rows):
    count, channels = wide.shape[0], wide.shape[1] // 3
    row = lax.broadcasted_iota(jnp.int32, (count, 1), 0) % rows
    up = jnp.where(row < rows - 1, pltpu.roll(wide[:, :channels], count - 1, 0), 0.0)
    down = jnp.where(row > 0, pltpu.roll(wide[:, 2 * channels :], 1, 0), 0.0)
    return wide[:, channels : 2 * channels] + up + down


def stream(w_hbm, wbuf, sems, taps):
    copies = {}
    for slot, a in enumerate(taps):
        copies[a] = pltpu.make_async_copy(
            w_hbm.at[pl.ds(9 * a, 9)], wbuf.at[pl.ds(9 * slot, 9)], sems.at[slot]
        )
        copies[a].start()
    return copies


def conv_kernel(
    par_ref, own_ref, next_ref, ra_ref, rb_ref, ran_ref, rbn_ref, w_hbm, u_ref, ext, acc, wbuf, sems
):
    frames, cols, rows, channels = own_ref.shape
    taps = (2, 1, 0)
    copies = stream(w_hbm, wbuf, sems, taps)
    even, side, later = par_ref[0] == 0, par_ref[1] == 1, par_ref[2] == 1
    zero = jnp.bfloat16(0)
    own = lambda v: jnp.where(side, v, zero)
    nxt = lambda v: jnp.where(later, v, zero)
    fill(ext, 0, own_ref[...], ra_ref[...], own(rb_ref[...]), even)
    fill(ext, frames, nxt(next_ref[...]), nxt(ran_ref[...]), nxt(own(rbn_ref[...])), even)
    for slot, a in enumerate(taps):
        copies[a].wait()
        part = time_tap(ext, wbuf, a, slot, frames, cols)
        acc[...] = part if slot == 0 else acc[...] + part
    u_ref[...] = row_taps(acc, rows)


def conv_section(par, grad, halo, kernel):
    frames, cols, rows, channels = grad.shape
    count = frames * cols * rows
    return pl.pallas_call(
        conv_kernel,
        out_shape=jax.ShapeDtypeStruct((count, channels), jnp.float32),
        in_specs=[pl.BlockSpec(memory_space=pltpu.SMEM)] + vmem(6) + HBM,
        out_specs=vmem(1)[0],
        scratch_shapes=[
            pltpu.VMEM((2 * frames, cols + 2, rows, channels), jnp.bfloat16),
            pltpu.VMEM((count, 3 * channels), jnp.float32),
            pltpu.VMEM(kernel.shape, jnp.bfloat16),
            pltpu.SemaphoreType.DMA((3,)),
        ],
        compiler_params=pltpu.CompilerParams(vmem_limit_bytes=16 * MIB),
        cost_estimate=matmul_cost(count, kernel),
        name="conv",
    )(par, grad, *halo, in_hbm(kernel))


def norm_stats(cells, base, frames, mom_ref):
    totals = group_sum(jnp.sum(mom_ref[...], axis=0)) * (1.0 / cells)
    means, scales = [], []
    for f in range(frames):
        mean = totals[base + f : base + f + 1]
        var = totals[base + frames + f : base + frames + f + 1] - mean * mean
        means.append(mean)
        scales.append(lax.rsqrt(var + EPSILON))
    return means, scales


def through(upstream, normed, gain, shift):
    pre = normed * gain + shift
    sig = jax.nn.sigmoid(pre)
    return upstream * sig * (1.0 + pre * (1.0 - sig)) * gain


def small_copies(pairs, sems, first):
    copies = [pltpu.make_async_copy(*pair, sems.at[first + k]) for k, pair in enumerate(pairs)]
    for copy in copies:
        copy.start()
    return copies


def norm_kernel(
    cells,
    base,
    par_ref,
    u_ref,
    grad_ref,
    x_ref,
    mom_ref,
    gain_hbm,
    shift_hbm,
    q_ref,
    sums_ref,
    stats_ref,
    pair_ref,
    sa_ref,
    sb_ref,
    gain_ref,
    shift_ref,
    sems,
):
    frames, cols, rows, channels = x_ref.shape
    affine = small_copies(((gain_hbm, gain_ref), (shift_hbm, shift_ref)), sems, 0)
    means, scales = norm_stats(cells, base, frames, mom_ref)
    for copy in affine:
        copy.wait()
    gain, shift = gain_ref[...].reshape(1, channels), shift_ref[...].reshape(1, channels)
    even = par_ref[0] == 0
    half = cols * rows
    sums, crosses = [], []
    for f in range(frames):
        normed = (x_ref[f].astype(jnp.float32).reshape(half, channels) - means[f]) * scales[f]
        q = through(u_ref[f * half : (f + 1) * half], normed, gain, shift)
        q_ref[f] = q.reshape(cols, rows, channels)
        sums.append(jnp.sum(q, axis=0, keepdims=True))
        crosses.append(jnp.sum(q * normed, axis=0, keepdims=True))
        early = grad_ref[f].astype(jnp.float32).reshape(half, channels) + scales[f] * q
        for k, value in enumerate((early, scales[f] * normed)):
            value = value.astype(jnp.bfloat16).reshape(cols, rows, channels)
            pair_ref[k, f] = value
            sa_ref[k, f] = jnp.where(even, value[cols - 1], value[0])
            sb_ref[k, f] = jnp.where(even, value[0], value[cols - 1])
    spread(sums_ref, jnp.concatenate(sums + crosses, axis=0))
    stats_ref[...] = jnp.concatenate(means + scales, axis=0)


def norm_section(par, upstream, grad, stored, mom, gain, shift, cells, base, peers):
    frames, cols, rows, channels = stored.shape
    edge = jax.ShapeDtypeStruct((2, frames, rows, channels), jnp.bfloat16)
    return pl.pallas_call(
        functools.partial(norm_kernel, cells, base),
        out_shape=(
            jax.ShapeDtypeStruct(stored.shape, jnp.float32),
            jax.ShapeDtypeStruct((peers, 2 * frames, channels), jnp.float32),
            jax.ShapeDtypeStruct((2 * frames, channels), jnp.float32),
            jax.ShapeDtypeStruct((2,) + stored.shape, jnp.bfloat16),
            edge,
            edge,
        ),
        in_specs=[pl.BlockSpec(memory_space=pltpu.SMEM)] + vmem(4) + HBM * 2,
        out_specs=tuple(vmem(6)),
        scratch_shapes=[
            pltpu.VMEM(gain.shape, jnp.float32),
            pltpu.VMEM(shift.shape, jnp.float32),
            pltpu.SemaphoreType.DMA((2,)),
        ],
        compiler_params=pltpu.CompilerParams(vmem_limit_bytes=8 * MIB),
        name="norm",
    )(par, upstream, grad, stored, mom, in_hbm(gain), in_hbm(shift))


def block_grad(cells, grad_ref, q_ref, x_ref, stats_ref, sums_ref):
    frames, cols, rows, channels = grad_ref.shape
    totals = group_sum(jnp.sum(sums_ref[...], axis=0)) * (1.0 / cells)
    result, firsts, crosses = [], [], []
    for f in range(frames):
        mean = stats_ref[f : f + 1]
        scale = stats_ref[frames + f : frames + f + 1]
        flat = (cols * rows, channels)
        normed = (x_ref[f].astype(jnp.float32).reshape(flat) - mean) * scale
        first, cross = totals[f : f + 1], totals[frames + f : frames + f + 1]
        value = grad_ref[f].astype(jnp.float32).reshape(flat) + scale * (
            q_ref[f].reshape(flat) - first - normed * cross
        )
        result.append(value.astype(jnp.bfloat16))
        firsts.append(scale * first)
        crosses.append(cross)
    return result, firsts + crosses


def dx_kernel(cells, grad_ref, q_ref, x_ref, stats_ref, sums_ref, dx_ref, means_ref):
    frames, cols, rows, channels = grad_ref.shape
    values, means = block_grad(cells, grad_ref, q_ref, x_ref, stats_ref, sums_ref)
    for f, value in enumerate(values):
        dx_ref[f] = value.reshape(cols, rows, channels)
    pad = [jnp.zeros((8 - 2 * frames, channels), jnp.float32)] if frames < 4 else []
    means_ref[...] = jnp.concatenate(means + pad, axis=0)


def dx_section(grad, q, stored, stats, sums, cells):
    frames, cols, rows, channels = grad.shape
    return pl.pallas_call(
        functools.partial(dx_kernel, cells),
        out_shape=(
            jax.ShapeDtypeStruct(grad.shape, jnp.bfloat16),
            jax.ShapeDtypeStruct((max(8, 2 * frames), channels), jnp.float32),
        ),
        in_specs=vmem(5),
        out_specs=tuple(vmem(2)),
        compiler_params=pltpu.CompilerParams(vmem_limit_bytes=8 * MIB),
        name="dx",
    )(grad, q, stored, stats, sums)


def settle(pair_ref, means_ref, f, frames):
    early, scaled = pair_ref[0, f].astype(jnp.float32), pair_ref[1, f].astype(jnp.float32)
    first, cross = means_ref[f : f + 1], means_ref[frames + f : frames + f + 1]
    return (early - first - scaled * cross).astype(jnp.bfloat16)


def settle_all(pair_ref, means_ref):
    frames = pair_ref.shape[1]
    return jnp.stack([settle(pair_ref, means_ref, f, frames) for f in range(frames)])


def near_kernel(par_ref, own_ref, ra_ref, rb_ref, means_ref, w_hbm, wide_ref, ext_ref, wbuf, sems):
    frames, cols, rows, channels = own_ref.shape
    copies = stream(w_hbm, wbuf, sems, (2,))
    even, side = par_ref[0] == 0, par_ref[1] == 1
    a = settle_all(ra_ref, means_ref)
    b = jnp.where(side, settle_all(rb_ref, means_ref), jnp.bfloat16(0))
    fill(ext_ref, 0, own_ref[...], a, b, even)
    copies[2].wait()
    wide_ref[...] = time_tap(ext_ref, wbuf, 2, 0, frames, cols)


def near_section(par, grad, ra, rb, means, kernel):
    frames, cols, rows, channels = grad.shape
    count = frames * cols * rows
    return pl.pallas_call(
        near_kernel,
        out_shape=(
            jax.ShapeDtypeStruct((count, 3 * channels), jnp.float32),
            jax.ShapeDtypeStruct((frames, cols + 2, rows, channels), jnp.bfloat16),
        ),
        in_specs=[pl.BlockSpec(memory_space=pltpu.SMEM)] + vmem(4) + HBM,
        out_specs=tuple(vmem(2)),
        scratch_shapes=[
            pltpu.VMEM((9,) + kernel.shape[1:], jnp.bfloat16),
            pltpu.SemaphoreType.DMA((1,)),
        ],
        compiler_params=pltpu.CompilerParams(vmem_limit_bytes=10 * MIB),
        cost_estimate=matmul_cost(count, kernel),
        name="near",
    )(par, grad, ra, rb, means, in_hbm(kernel))


def far_kernel(
    cells,
    base,
    par_ref,
    wide_ref,
    near_ref,
    next_ref,
    ran_ref,
    rbn_ref,
    means_ref,
    x_ref,
    mom_ref,
    gain_hbm,
    shift_hbm,
    w_hbm,
    q_ref,
    sums_ref,
    stats_ref,
    ext,
    acc,
    wbuf,
    gain_ref,
    shift_ref,
    sems,
):
    frames, cols, rows, channels = x_ref.shape
    copies = stream(w_hbm, wbuf, sems, (1, 0))
    affine = small_copies(((gain_hbm, gain_ref), (shift_hbm, shift_ref)), sems, 2)
    even, side, later = par_ref[0] == 0, par_ref[1] == 1, par_ref[2] == 1
    zero = jnp.bfloat16(0)
    nxt = lambda v: jnp.where(later, v, zero)
    ext[0:frames] = near_ref[...]
    b = jnp.where(side, settle_all(rbn_ref, means_ref), zero)
    fill(
        ext,
        frames,
        nxt(settle_all(next_ref, means_ref)),
        nxt(settle_all(ran_ref, means_ref)),
        nxt(b),
        even,
    )
    acc[...] = wide_ref[...]
    for slot, a in enumerate((1, 0)):
        copies[a].wait()
        acc[...] += time_tap(ext, wbuf, a, slot, frames, cols)
    upstream = row_taps(acc, rows)
    means, scales = norm_stats(cells, base, frames, mom_ref)
    for copy in affine:
        copy.wait()
    gain, shift = gain_ref[...].reshape(1, channels), shift_ref[...].reshape(1, channels)
    half = cols * rows
    sums, crosses = [], []
    for f in range(frames):
        normed = (x_ref[f].astype(jnp.float32).reshape(half, channels) - means[f]) * scales[f]
        q = through(upstream[f * half : (f + 1) * half], normed, gain, shift)
        q_ref[f] = q.reshape(cols, rows, channels)
        sums.append(jnp.sum(q, axis=0, keepdims=True))
        crosses.append(jnp.sum(q * normed, axis=0, keepdims=True))
    spread(sums_ref, jnp.concatenate(sums + crosses, axis=0))
    stats_ref[...] = jnp.concatenate(means + scales, axis=0)


def far_section(par, near, halo, means, stored, mom, gain, shift, kernel, cells, base, peers):
    frames, cols, rows, channels = stored.shape
    count = frames * cols * rows
    return pl.pallas_call(
        functools.partial(far_kernel, cells, base),
        out_shape=(
            jax.ShapeDtypeStruct(stored.shape, jnp.float32),
            jax.ShapeDtypeStruct((peers, 2 * frames, channels), jnp.float32),
            jax.ShapeDtypeStruct((2 * frames, channels), jnp.float32),
        ),
        in_specs=[pl.BlockSpec(memory_space=pltpu.SMEM)] + vmem(8) + HBM * 3,
        out_specs=tuple(vmem(3)),
        scratch_shapes=[
            pltpu.VMEM((2 * frames, cols + 2, rows, channels), jnp.bfloat16),
            pltpu.VMEM((count, 3 * channels), jnp.float32),
            pltpu.VMEM((18,) + kernel.shape[1:], jnp.bfloat16),
            pltpu.VMEM(gain.shape, jnp.float32),
            pltpu.VMEM(shift.shape, jnp.float32),
            pltpu.SemaphoreType.DMA((4,)),
        ],
        compiler_params=pltpu.CompilerParams(vmem_limit_bytes=16 * MIB),
        cost_estimate=matmul_cost(count, kernel),
        name="far",
    )(par, *near, *halo, means, stored, mom, *map(in_hbm, (gain, shift, kernel)))


def latent_kernel_body(cells, grad_ref, q_ref, x_ref, stats_ref, sums_ref, k_ref, own_ref, prev_ref, wide):
    frames, cols, rows, channels = grad_ref.shape
    lat = k_ref.shape[1]
    lanes = wide.shape[1]
    values, _ = block_grad(cells, grad_ref, q_ref, x_ref, stats_ref, sums_ref)
    grad = jnp.concatenate(values, axis=0)
    count = frames * cols * rows
    wide[...] = jnp.zeros_like(wide)
    for k in range(9):
        wide[k, 0 : 3 * lat] = k_ref[3 * k : 3 * k + 3].reshape(3 * lat, channels)
    row = lax.broadcasted_iota(jnp.int32, (count, 1), 0) % rows
    placed = {}
    for a in range(3):
        z = [nt_dot(grad, wide[3 * a + b]) for b in range(3)]
        up = jnp.where(row < rows - 1, pltpu.roll(z[0], count - 1, 0), 0.0)
        down = jnp.where(row > 0, pltpu.roll(z[2], 1, 0), 0.0)
        total = (z[1] + up + down).reshape(frames, cols, rows, lanes)
        for f in range(frames):
            out = total[f, 0]
            for w in range(1, cols):
                out = out + pltpu.roll(total[f, w], lat * w, 1)
            at = f + a - 2
            placed[at] = placed[at] + out if at in placed else out
    for f in range(frames):
        own_ref[f] = placed[f]
        prev_ref[f] = placed[f - 2]


def latent_section(grad, q, stored, stats, sums, kernel, cells):
    frames, cols, rows, channels = grad.shape
    lanes = 128
    out = jax.ShapeDtypeStruct((frames, rows, lanes), jnp.float32)
    return pl.pallas_call(
        functools.partial(latent_kernel_body, cells),
        out_shape=(out, out),
        in_specs=vmem(6),
        out_specs=tuple(vmem(2)),
        scratch_shapes=[pltpu.VMEM((9, lanes, channels), jnp.bfloat16)],
        compiler_params=pltpu.CompilerParams(vmem_limit_bytes=16 * MIB),
        name="latent",
    )(grad, q, stored, stats, sums, kernel)


def assemble_kernel(lat, cols, got_ref, e_ref, perm_ref, out_ref):
    peers, quad, lanes = got_ref.shape
    parts = {}
    for p in range(2):
        rows = jnp.concatenate([got_ref[:, p, :], got_ref[:, 2 + p, :]], axis=0)
        spots = lax.dot_general(
            jnp.concatenate(thirds(rows), axis=0),
            e_ref[...],
            (((0,), (0,)), ((), ())),
            preferred_element_type=jnp.float32,
        )
        for col in range(cols + 2):
            q = (col + 1) % 2
            piece = spots[lat * col : lat * (col + 1), 128 * col : 128 * (col + 1)]
            parts[p, q] = parts[p, q] + piece if (p, q) in parts else piece
    stacked = jnp.concatenate([parts[p, q] for p in range(2) for q in range(2)], axis=0)
    final = jnp.dot(
        perm_ref[...],
        jnp.concatenate(thirds(stacked), axis=0),
        preferred_element_type=jnp.float32,
    )
    out_ref[...] = final[:, : out_ref.shape[1]]


def assemble(got, lat, cols):
    peers, quad, lanes = got.shape
    width = peers * cols // 2
    tokens = quad // 2 * width
    place = np.zeros((quad // 2, peers, (cols + 2) * 128), np.float32)
    for hh in range(quad // 2):
        for s in range(peers):
            for col in range(cols + 2):
                x = s * cols + col - 1
                if 0 <= x < peers * cols:
                    place[hh, s, 128 * col + hh * width + x // 2] = 1.0
    place = np.tile(place.reshape(-1, place.shape[-1]), (3, 1))
    perm = np.zeros((4 * lat, 4 * lat), np.float32)
    for pq in range(4):
        for one in range(lat):
            perm[one * 4 + pq, pq * lat + one] = 1.0
    perm = np.tile(perm, (1, 3))
    return pl.pallas_call(
        functools.partial(assemble_kernel, lat, cols),
        out_shape=jax.ShapeDtypeStruct((4 * lat, tokens), jnp.float32),
        in_specs=vmem(3),
        out_specs=pl.BlockSpec(memory_space=pltpu.VMEM),
        compiler_params=pltpu.CompilerParams(vmem_limit_bytes=8 * MIB),
        name="assemble",
    )(got, jnp.asarray(place, jnp.bfloat16), jnp.asarray(perm, jnp.bfloat16))


def pick(even, one, other):
    return jnp.where(even, one, other)


def exchange(value, send_a, send_b, even):
    tms = lax.axis_size("tm")
    tiles = lax.axis_size(TILE)
    cols = value.shape[-3]
    back = ring(tms)
    swap = [(0, 1), (1, 0)]
    hops = []
    for k in range(1, tiles, 2):
        hops += [(k, (k + 1) % tiles), ((k + 1) % tiles, k)]
    diagonal = [(t * tiles + s, u * tiles + d) for t, u in back for s, d in hops]
    nxt = lax.ppermute(value, "tm", back)
    rb = lax.ppermute(send_b, TILE, hops)
    rbn = lax.ppermute(send_b, TM_TILE, diagonal)
    ra = lax.ppermute(send_a, "tile_2", swap)
    ran = lax.ppermute(pick(even, nxt[..., cols - 1, :, :], nxt[..., 0, :, :]), "tile_2", swap)
    return nxt, ra, rb, ran, rbn


def ring(count):
    return [(t, (t - 1) % count) for t in range(count)]


def everyone(rows):
    return lax.all_to_all(rows, TILE, 0, 0)


def shards(
    first_input,
    second_input,
    output_grad,
    first_gain,
    first_shift,
    first_kernel,
    second_gain,
    second_shift,
    second_kernel,
    latent_kernel,
):
    frames, rows, cols, channels = first_input.shape
    peers = lax.axis_size(TILE)
    cells = rows * cols * peers * (channels // GROUPS)
    core = lax.axis_index("tile_2")
    even = core == 0
    tile, when = lax.axis_index(TILE), lax.axis_index("tm")
    later = when < lax.axis_size("tm") - 1
    side = jnp.where(even, tile > 0, tile < peers - 1)
    par = jnp.stack([core.astype(jnp.int32), side.astype(jnp.int32), later.astype(jnp.int32)])
    turn = lambda x: with_layout_constraint(
        jnp.transpose(x, (0, 2, 1, 3)), Layout(major_to_minor=(0, 1, 2, 3))
    )

    grad = turn(output_grad)
    halo = exchange(
        grad,
        pick(even, grad[:, cols - 1], grad[:, 0]),
        pick(even, grad[:, 0], grad[:, cols - 1]),
        even,
    )
    mom = everyone(moments(second_input, first_input, peers))
    second, first = turn(second_input), turn(first_input)
    upstream = conv_section(par, grad, halo, second_kernel)
    q, sums, stats, pair, send_a, send_b = norm_section(
        par, upstream, grad, second, mom, second_gain, second_shift, cells, 0, peers
    )
    nxt, ra, rb, ran, rbn = exchange(pair, send_a, send_b, even)
    grad, means = dx_section(grad, q, second, stats, everyone(sums), cells)
    later_means = lax.ppermute(means, "tm", ring(lax.axis_size("tm")))
    near = near_section(par, grad, ra, rb, means, first_kernel)
    q, sums, stats = far_section(
        par, near, (nxt, ran, rbn), later_means, first, mom, first_gain, first_shift,
        first_kernel, cells, 2 * frames, peers,
    )
    own, prev = latent_section(grad, q, first, stats, everyone(sums), latent_kernel, cells)
    tms = lax.axis_size("tm")
    own = own + jnp.where(later, lax.ppermute(prev, "tm", ring(tms)), 0.0)
    got = everyone(own.reshape(peers, frames * rows // peers, own.shape[-1]))
    return assemble(got, latent_kernel.shape[1], cols)


def solution(mesh):
    torus = Mesh(
        mesh.devices.reshape(mesh.shape["tm"], 4, 2, 2), ("tm", "tile_0", "tile_1", "tile_2")
    )
    block = P("tm", None, TILE, None)
    placed = (block, block, block) + (P(),) * 7
    return jax.shard_map(
        shards, mesh=torus, in_specs=placed, out_specs=P(None, TM_TILE), check_vma=False
    )
```

```python
import functools

import jax
import jax.numpy as jnp
import numpy as np
from jax import lax
from jax.experimental import pallas as pl
from jax.experimental.pallas import tpu as pltpu
from jax.experimental.layout import Layout, with_layout_constraint
from jax.sharding import Mesh
from jax.sharding import PartitionSpec as P

GROUPS = 32
TILE = ("tile_0", "tile_1", "tile_2")
TM_TILE = ("tm",) + TILE
EPSILON = 1e-05
MIB = 1 << 20


def vmem(count):
    return [pl.BlockSpec(memory_space=pltpu.VMEM)] * count


WEIGHTS_COVER = pl.CostEstimate(flops=1 << 33, bytes_accessed=1 << 23, transcendentals=0)
HBM = [pl.BlockSpec(memory_space=pltpu.HBM)]


def matmul_cost(count, kernel):
    return pl.CostEstimate(
        flops=2 * count * kernel.size, bytes_accessed=2 * kernel.size, transcendentals=0
    )


def in_hbm(value):
    return pltpu.with_memory_space_constraint(value, pltpu.HBM)


def nt_dot(left, right, **kw):
    return lax.dot_general(
        left, right, (((1,), (1,)), ((), ())), preferred_element_type=jnp.float32, **kw
    )


def thirds(value):
    high = value.astype(jnp.bfloat16)
    rest = value - high.astype(jnp.float32)
    middle = rest.astype(jnp.bfloat16)
    return high, middle, (rest - middle.astype(jnp.float32)).astype(jnp.bfloat16)


def group_sum(rows):
    count, channels = rows.shape
    per = channels // GROUPS
    row = lax.broadcasted_iota(jnp.int32, (channels, channels), 0) // per
    col = lax.broadcasted_iota(jnp.int32, (channels, channels), 1) // per
    same = jnp.where(row == col, 1.0, 0.0).astype(jnp.bfloat16)
    if count < 8:
        rows = jnp.concatenate([rows, jnp.zeros((8 - count, channels), jnp.float32)], axis=0)
    split = jnp.concatenate([part.astype(jnp.float32) for part in thirds(rows)], axis=0)
    sums = jnp.dot(split.astype(jnp.bfloat16), same, preferred_element_type=jnp.float32)
    return sums[0:count] + sums[8 : 8 + count] + sums[16 : 16 + count]


def spread(ref, rows):
    ref[...] = jnp.broadcast_to(rows[None], ref.shape)


def moments_kernel(second_hbm, first_hbm, out_ref, second_ref, first_ref, sems):
    pairs = ((second_hbm, second_ref), (first_hbm, first_ref))
    copies = [pltpu.make_async_copy(*pair, sems.at[k]) for k, pair in enumerate(pairs)]
    for copy in copies:
        copy.start()
    rows = []
    for copy, (_, ref) in zip(copies, pairs):
        copy.wait()
        frames = ref.shape[0]
        values = [ref[f].astype(jnp.float32) for f in range(frames)]
        rows += [jnp.sum(v, axis=(0, 1)).reshape(1, -1) for v in values]
        rows += [jnp.sum(v * v, axis=(0, 1)).reshape(1, -1) for v in values]
    spread(out_ref, jnp.concatenate(rows, axis=0))


def moments(second, first, peers):
    frames, _, _, channels = second.shape
    return pl.pallas_call(
        moments_kernel,
        out_shape=jax.ShapeDtypeStruct((peers, 4 * frames, channels), jnp.float32),
        in_specs=[pl.BlockSpec(memory_space=pltpu.HBM)] * 2,
        out_specs=pl.BlockSpec(memory_space=pltpu.VMEM),
        scratch_shapes=[
            pltpu.VMEM(second.shape, jnp.bfloat16),
            pltpu.VMEM(first.shape, jnp.bfloat16),
            pltpu.SemaphoreType.DMA((2,)),
        ],
        compiler_params=pltpu.CompilerParams(vmem_limit_bytes=16 * MIB),
        name="moments",
    )(in_hbm(second), in_hbm(first))


def fill(ext, at, block, a, b, even):
    frames, cols = block.shape[:2]
    ext[at : at + frames, 1 : cols + 1] = block
    ext[at : at + frames, 0] = jnp.where(even, b, a)
    ext[at : at + frames, cols + 1] = jnp.where(even, a, b)


def time_taps(ext, w_ref, taps, frames, cols):
    _, channels = ext.shape[2:]
    pairs = [(a, c) for a in taps for c in range(3)]
    left = jnp.concatenate(
        [
            ext[2 - a : 2 - a + frames, 2 - c : 2 - c + cols].reshape(-1, channels)
            for a, c in pairs
        ],
        axis=1,
    )
    right = jnp.concatenate(
        [
            jnp.concatenate([w_ref[9 * a + 3 * b + c] for a, c in pairs], axis=1)
            for b in range(3)
        ],
        axis=0,
    )
    return nt_dot(left, right)


def row_taps(wide, rows):
    count, channels = wide.shape[0], wide.shape[1] // 3
    row = lax.broadcasted_iota(jnp.int32, (count, 1), 0) % rows
    up = jnp.where(row < rows - 1, pltpu.roll(wide[:, :channels], count - 1, 0), 0.0)
    down = jnp.where(row > 0, pltpu.roll(wide[:, 2 * channels :], 1, 0), 0.0)
    return wide[:, channels : 2 * channels] + up + down


def window(par_ref, own_ref, next_ref, ra_ref, rb_ref, ran_ref, rbn_ref, ext):
    frames = own_ref.shape[0]
    even, side, later = par_ref[0] == 0, par_ref[1] == 1, par_ref[2] == 1
    zero = jnp.bfloat16(0)
    own = lambda v: jnp.where(side, v, zero)
    nxt = lambda v: jnp.where(later, v, zero)
    fill(ext, 0, own_ref[...], ra_ref[...], own(rb_ref[...]), even)
    fill(ext, frames, nxt(next_ref[...]), nxt(ran_ref[...]), nxt(own(rbn_ref[...])), even)


def conv_kernel(
    par_ref,
    own_ref,
    next_ref,
    ra_ref,
    rb_ref,
    ran_ref,
    rbn_ref,
    w_hbm,
    u_ref,
    ext,
    acc,
    w_ref,
    sems,
):
    frames, cols, rows, _ = own_ref.shape
    copies = {
        a: pltpu.make_async_copy(
            w_hbm.at[pl.ds(9 * a, 9)], w_ref.at[pl.ds(9 * a, 9)], sems.at[a]
        )
        for a in (2, 1, 0)
    }
    for copy in copies.values():
        copy.start()
    window(par_ref, own_ref, next_ref, ra_ref, rb_ref, ran_ref, rbn_ref, ext)
    for a, copy in copies.items():
        copy.wait()
        part = time_taps(ext, w_ref, (a,), frames, cols)
        acc[...] = part if a == 2 else acc[...] + part
    u_ref[...] = row_taps(acc, rows)


def conv_section(par, grad, halo, kernel):
    frames, cols, rows, channels = grad.shape
    count = frames * cols * rows
    return pl.pallas_call(
        conv_kernel,
        out_shape=jax.ShapeDtypeStruct((count, channels), jnp.float32),
        in_specs=[pl.BlockSpec(memory_space=pltpu.SMEM)] + vmem(6) + HBM,
        out_specs=vmem(1)[0],
        scratch_shapes=[
            pltpu.VMEM((2 * frames, cols + 2, rows, channels), jnp.bfloat16),
            pltpu.VMEM((count, 3 * channels), jnp.float32),
            pltpu.VMEM(kernel.shape, jnp.bfloat16),
            pltpu.SemaphoreType.DMA((3,)),
        ],
        compiler_params=pltpu.CompilerParams(vmem_limit_bytes=16 * MIB),
        cost_estimate=matmul_cost(count, kernel),
        name="conv",
    )(par, grad, *halo, in_hbm(kernel))


def norm_stats(cells, base, frames, mom_ref):
    totals = group_sum(jnp.sum(mom_ref[...], axis=0)) * (1.0 / cells)
    means, scales = [], []
    for f in range(frames):
        mean = totals[base + f : base + f + 1]
        var = totals[base + frames + f : base + frames + f + 1] - mean * mean
        means.append(mean)
        scales.append(lax.rsqrt(var + EPSILON))
    return means, scales


def through(upstream, normed, gain, shift):
    pre = normed * gain + shift
    sig = jax.nn.sigmoid(pre)
    return upstream * sig * (1.0 + pre * (1.0 - sig)) * gain


def finish(cells, base, upstream, x_ref, mom_ref, affine_ref, at, q_ref, sums_ref, stats_ref):
    frames, cols, rows, channels = x_ref.shape
    means, scales = norm_stats(cells, base, frames, mom_ref)
    gain, shift = affine_ref[at : at + 1], affine_ref[at + 1 : at + 2]
    half = cols * rows
    sums, crosses = [], []
    for f in range(frames):
        normed = (x_ref[f].astype(jnp.float32).reshape(half, channels) - means[f]) * scales[f]
        q = through(upstream[f * half : (f + 1) * half], normed, gain, shift)
        q_ref[f] = q.reshape(cols, rows, channels)
        sums.append(jnp.sum(q, axis=0, keepdims=True))
        crosses.append(jnp.sum(q * normed, axis=0, keepdims=True))
    spread(sums_ref, jnp.concatenate(sums + crosses, axis=0))
    stats_ref[...] = jnp.concatenate(means + scales, axis=0)


def finish_shapes(stored, peers):
    frames, _, _, channels = stored.shape
    return (
        jax.ShapeDtypeStruct(stored.shape, jnp.float32),
        jax.ShapeDtypeStruct((peers, 2 * frames, channels), jnp.float32),
        jax.ShapeDtypeStruct((2 * frames, channels), jnp.float32),
    )


def norm_kernel(cells, u_ref, x_ref, mom_ref, affine_ref, q_ref, sums_ref, stats_ref):
    finish(cells, 0, u_ref, x_ref, mom_ref, affine_ref, 0, q_ref, sums_ref, stats_ref)


def norm_section(upstream, stored, mom, affine, cells, peers):
    return pl.pallas_call(
        functools.partial(norm_kernel, cells),
        out_shape=finish_shapes(stored, peers),
        in_specs=vmem(4),
        out_specs=tuple(vmem(3)),
        compiler_params=pltpu.CompilerParams(vmem_limit_bytes=16 * MIB),
        name="norm",
    )(upstream, stored, mom, affine)


def block_grad(cells, grad_ref, q_ref, x_ref, stats_ref, sums_ref):
    frames, cols, rows, channels = grad_ref.shape
    totals = group_sum(jnp.sum(sums_ref[...], axis=0)) * (1.0 / cells)
    result = []
    for f in range(frames):
        mean = stats_ref[f : f + 1]
        scale = stats_ref[frames + f : frames + f + 1]
        flat = (cols * rows, channels)
        normed = (x_ref[f].astype(jnp.float32).reshape(flat) - mean) * scale
        value = grad_ref[f].astype(jnp.float32).reshape(flat) + scale * (
            q_ref[f].reshape(flat)
            - totals[f : f + 1]
            - normed * totals[frames + f : frames + f + 1]
        )
        result.append(value.astype(jnp.bfloat16))
    return result


def dx_kernel(cells, par_ref, grad_ref, q_ref, x_ref, stats_ref, sums_ref, dx_ref, sa_ref, sb_ref):
    _, cols, rows, channels = grad_ref.shape
    even = par_ref[0] == 0
    for f, value in enumerate(block_grad(cells, grad_ref, q_ref, x_ref, stats_ref, sums_ref)):
        value = value.reshape(cols, rows, channels)
        dx_ref[f] = value
        sa_ref[f] = jnp.where(even, value[cols - 1], value[0])
        sb_ref[f] = jnp.where(even, value[0], value[cols - 1])


def dx_section(par, grad, q, stored, stats, sums, cells):
    frames, _, rows, channels = grad.shape
    edge = jax.ShapeDtypeStruct((frames, rows, channels), jnp.bfloat16)
    return pl.pallas_call(
        functools.partial(dx_kernel, cells),
        out_shape=(jax.ShapeDtypeStruct(grad.shape, jnp.bfloat16), edge, edge),
        in_specs=[pl.BlockSpec(memory_space=pltpu.SMEM)] + vmem(5),
        out_specs=tuple(vmem(3)),
        compiler_params=pltpu.CompilerParams(vmem_limit_bytes=16 * MIB),
        cost_estimate=WEIGHTS_COVER,
        name="dx",
    )(par, grad, q, stored, stats, sums)


def conv_norm_kernel(
    cells,
    base,
    par_ref,
    own_ref,
    next_ref,
    ra_ref,
    rb_ref,
    ran_ref,
    rbn_ref,
    w_ref,
    x_ref,
    mom_ref,
    affine_ref,
    q_ref,
    sums_ref,
    stats_ref,
    ext,
    acc,
):
    rows = own_ref.shape[2]
    window(par_ref, own_ref, next_ref, ra_ref, rb_ref, ran_ref, rbn_ref, ext)
    acc[...] = time_taps(ext, w_ref, (2, 1, 0), *own_ref.shape[:2])
    upstream = row_taps(acc, rows)
    finish(cells, base, upstream, x_ref, mom_ref, affine_ref, 2, q_ref, sums_ref, stats_ref)


def conv_norm_section(par, grad, halo, kernel, stored, mom, affine, cells, base, peers):
    frames, cols, rows, channels = grad.shape
    count = frames * cols * rows
    return pl.pallas_call(
        functools.partial(conv_norm_kernel, cells, base),
        out_shape=finish_shapes(stored, peers),
        in_specs=[pl.BlockSpec(memory_space=pltpu.SMEM)] + vmem(10),
        out_specs=tuple(vmem(3)),
        scratch_shapes=[
            pltpu.VMEM((2 * frames, cols + 2, rows, channels), jnp.bfloat16),
            pltpu.VMEM((count, 3 * channels), jnp.float32),
        ],
        compiler_params=pltpu.CompilerParams(vmem_limit_bytes=16 * MIB),
        cost_estimate=matmul_cost(count, kernel),
        name="convnorm",
    )(par, grad, *halo, kernel, stored, mom, affine)


def edge_kernel(par_ref, block_ref, sa_ref, sb_ref):
    cols = block_ref.shape[1]
    even = par_ref[0] == 0
    first, last = block_ref[:, 0], block_ref[:, cols - 1]
    sa_ref[...] = jnp.where(even, last, first)
    sb_ref[...] = jnp.where(even, first, last)


def edge_section(par, block):
    frames, _, rows, channels = block.shape
    edge = jax.ShapeDtypeStruct((frames, rows, channels), block.dtype)
    return pl.pallas_call(
        edge_kernel,
        out_shape=(edge, edge),
        in_specs=[pl.BlockSpec(memory_space=pltpu.SMEM)] + vmem(1),
        out_specs=tuple(vmem(2)),
        compiler_params=pltpu.CompilerParams(vmem_limit_bytes=4 * MIB),
        name="edge",
    )(par, block)


def latent_kernel_body(cells, grad_ref, q_ref, x_ref, stats_ref, sums_ref, k_ref, own_ref, prev_ref, wide):
    frames, cols, rows, channels = grad_ref.shape
    lat = k_ref.shape[1]
    lanes = wide.shape[1]
    values = block_grad(cells, grad_ref, q_ref, x_ref, stats_ref, sums_ref)
    grad = jnp.concatenate(values, axis=0)
    count = frames * cols * rows
    wide[...] = jnp.zeros_like(wide)
    for k in range(9):
        wide[k, 0 : 3 * lat] = k_ref[3 * k : 3 * k + 3].reshape(3 * lat, channels)
    row = lax.broadcasted_iota(jnp.int32, (count, 1), 0) % rows
    placed = {}
    for a in range(3):
        z = [nt_dot(grad, wide[3 * a + b]) for b in range(3)]
        up = jnp.where(row < rows - 1, pltpu.roll(z[0], count - 1, 0), 0.0)
        down = jnp.where(row > 0, pltpu.roll(z[2], 1, 0), 0.0)
        total = (z[1] + up + down).reshape(frames, cols, rows, lanes)
        for f in range(frames):
            out = total[f, 0]
            for w in range(1, cols):
                out = out + pltpu.roll(total[f, w], lat * w, 1)
            at = f + a - 2
            placed[at] = placed[at] + out if at in placed else out
    for f in range(frames):
        own_ref[f] = placed[f]
        prev_ref[f] = placed[f - 2]


def latent_section(grad, q, stored, stats, sums, kernel, cells):
    frames, _, rows, channels = grad.shape
    lanes = 128
    out = jax.ShapeDtypeStruct((frames, rows, lanes), jnp.float32)
    return pl.pallas_call(
        functools.partial(latent_kernel_body, cells),
        out_shape=(out, out),
        in_specs=vmem(6),
        out_specs=tuple(vmem(2)),
        scratch_shapes=[pltpu.VMEM((9, lanes, channels), jnp.bfloat16)],
        compiler_params=pltpu.CompilerParams(vmem_limit_bytes=16 * MIB),
        name="latent",
    )(grad, q, stored, stats, sums, kernel)


def assemble_kernel(lat, cols, got_ref, e_ref, perm_ref, out_ref):
    parts = {}
    for p in range(2):
        rows = jnp.concatenate([got_ref[:, p, :], got_ref[:, 2 + p, :]], axis=0)
        spots = lax.dot_general(
            jnp.concatenate(thirds(rows), axis=0),
            e_ref[...],
            (((0,), (0,)), ((), ())),
            preferred_element_type=jnp.float32,
        )
        for col in range(cols + 2):
            q = (col + 1) % 2
            piece = spots[lat * col : lat * (col + 1), 128 * col : 128 * (col + 1)]
            parts[p, q] = parts[p, q] + piece if (p, q) in parts else piece
    stacked = jnp.concatenate([parts[p, q] for p in range(2) for q in range(2)], axis=0)
    final = jnp.dot(
        perm_ref[...],
        jnp.concatenate(thirds(stacked), axis=0),
        preferred_element_type=jnp.float32,
    )
    out_ref[...] = final[:, : out_ref.shape[1]]


def assemble(got, lat, cols):
    peers, quad, _ = got.shape
    width = peers * cols // 2
    tokens = quad // 2 * width
    place = np.zeros((quad // 2, peers, (cols + 2) * 128), np.float32)
    for hh in range(quad // 2):
        for s in range(peers):
            for col in range(cols + 2):
                x = s * cols + col - 1
                if 0 <= x < peers * cols:
                    place[hh, s, 128 * col + hh * width + x // 2] = 1.0
    place = np.tile(place.reshape(-1, place.shape[-1]), (3, 1))
    perm = np.zeros((4 * lat, 4 * lat), np.float32)
    for pq in range(4):
        for one in range(lat):
            perm[one * 4 + pq, pq * lat + one] = 1.0
    perm = np.tile(perm, (1, 3))
    return pl.pallas_call(
        functools.partial(assemble_kernel, lat, cols),
        out_shape=jax.ShapeDtypeStruct((4 * lat, tokens), jnp.float32),
        in_specs=vmem(3),
        out_specs=pl.BlockSpec(memory_space=pltpu.VMEM),
        compiler_params=pltpu.CompilerParams(vmem_limit_bytes=16 * MIB),
        name="assemble",
    )(got, jnp.asarray(place, jnp.bfloat16), jnp.asarray(perm, jnp.bfloat16))


def exchange(par, value, send_a, send_b):
    tms = lax.axis_size("tm")
    tiles = lax.axis_size(TILE)
    back = ring(tms)
    swap = [(0, 1), (1, 0)]
    hops = []
    for k in range(1, tiles, 2):
        hops += [(k, (k + 1) % tiles), ((k + 1) % tiles, k)]
    diagonal = [(t * tiles + s, u * tiles + d) for t, u in back for s, d in hops]
    nxt = lax.ppermute(value, "tm", back)
    rb = lax.ppermute(send_b, TILE, hops)
    rbn = lax.ppermute(send_b, TM_TILE, diagonal)
    ra = lax.ppermute(send_a, "tile_2", swap)
    corner = edge_section(par, nxt)[0]
    ran = lax.ppermute(corner, "tile_2", swap)
    return nxt, ra, rb, ran, rbn


def ring(count):
    return [(t, (t - 1) % count) for t in range(count)]


def everyone(rows):
    return lax.all_to_all(rows, TILE, 0, 0)


def shards(
    first_input,
    second_input,
    output_grad,
    first_gain,
    first_shift,
    first_kernel,
    second_gain,
    second_shift,
    second_kernel,
    latent_kernel,
):
    frames, rows, cols, channels = first_input.shape
    peers = lax.axis_size(TILE)
    cells = rows * cols * peers * (channels // GROUPS)
    core = lax.axis_index("tile_2")
    even = core == 0
    tile, when = lax.axis_index(TILE), lax.axis_index("tm")
    later = when < lax.axis_size("tm") - 1
    side = jnp.where(even, tile > 0, tile < peers - 1)
    par = jnp.stack([core.astype(jnp.int32), side.astype(jnp.int32), later.astype(jnp.int32)])
    affine = jnp.stack([second_gain, second_shift, first_gain, first_shift])
    par, later, affine, output_grad, second_input, first_input = lax.optimization_barrier(
        (par, later, affine, output_grad, second_input, first_input)
    )
    turn = lambda x: with_layout_constraint(
        jnp.transpose(x, (0, 2, 1, 3)), Layout(major_to_minor=(0, 1, 2, 3))
    )

    grad = turn(output_grad)
    mine = moments(second_input, first_input, peers)
    mom = everyone(mine)
    halo = exchange(par, grad, *edge_section(par, grad))
    second, first = turn(second_input), turn(first_input)
    upstream = conv_section(par, grad, halo, second_kernel)
    q, sums, stats = norm_section(upstream, second, mom, affine, cells, peers)
    grad, send_a, send_b = dx_section(par, grad, q, second, stats, everyone(sums), cells)
    nxt, ra, rb, ran, rbn = exchange(par, grad, send_a, send_b)
    q, sums, stats = conv_norm_section(
        par, grad, (nxt, ra, rb, ran, rbn), first_kernel, first, mom, affine, cells,
        2 * frames, peers,
    )
    own, prev = latent_section(grad, q, first, stats, everyone(sums), latent_kernel, cells)
    tms = lax.axis_size("tm")
    own = own + jnp.where(later, lax.ppermute(prev, "tm", ring(tms)), 0.0)
    got = everyone(own.reshape(peers, frames * rows // peers, own.shape[-1]))
    return assemble(got, latent_kernel.shape[1], cols)


def solution(mesh):
    torus = Mesh(
        mesh.devices.reshape(mesh.shape["tm"], 4, 2, 2), ("tm", "tile_0", "tile_1", "tile_2")
    )
    block = P("tm", None, TILE, None)
    placed = (block, block, block) + (P(),) * 7
    return jax.shard_map(
        shards, mesh=torus, in_specs=placed, out_specs=P(None, TM_TILE), check_vma=False
    )
```

```python
import functools

import jax
import jax.numpy as jnp
import numpy as np
from jax import lax
from jax.experimental import pallas as pl
from jax.experimental.pallas import tpu as pltpu
from jax.experimental.layout import Layout, with_layout_constraint
from jax.sharding import Mesh
from jax.sharding import PartitionSpec as P

GROUPS = 32
TILE = ("tile_0", "tile_1", "tile_2")
TM_TILE = ("tm",) + TILE
EPSILON = 1e-05
MIB = 1 << 20


def vmem(count):
    return [pl.BlockSpec(memory_space=pltpu.VMEM)] * count


WEIGHTS_COVER = pl.CostEstimate(flops=1 << 33, bytes_accessed=1 << 23, transcendentals=0)
HBM = [pl.BlockSpec(memory_space=pltpu.HBM)]


def matmul_cost(count, kernel):
    return pl.CostEstimate(
        flops=2 * count * kernel.size, bytes_accessed=2 * kernel.size, transcendentals=0
    )


def in_hbm(value):
    return pltpu.with_memory_space_constraint(value, pltpu.HBM)


def nt_dot(left, right, **kw):
    return lax.dot_general(
        left, right, (((1,), (1,)), ((), ())), preferred_element_type=jnp.float32, **kw
    )


def thirds(value):
    high = value.astype(jnp.bfloat16)
    rest = value - high.astype(jnp.float32)
    middle = rest.astype(jnp.bfloat16)
    return high, middle, (rest - middle.astype(jnp.float32)).astype(jnp.bfloat16)


def group_sum(rows):
    count, channels = rows.shape
    per = channels // GROUPS
    row = lax.broadcasted_iota(jnp.int32, (channels, channels), 0) // per
    col = lax.broadcasted_iota(jnp.int32, (channels, channels), 1) // per
    same = jnp.where(row == col, 1.0, 0.0).astype(jnp.bfloat16)
    if count < 8:
        rows = jnp.concatenate([rows, jnp.zeros((8 - count, channels), jnp.float32)], axis=0)
    split = jnp.concatenate([part.astype(jnp.float32) for part in thirds(rows)], axis=0)
    sums = jnp.dot(split.astype(jnp.bfloat16), same, preferred_element_type=jnp.float32)
    return sums[0:count] + sums[8 : 8 + count] + sums[16 : 16 + count]


def spread(ref, rows):
    ref[...] = jnp.broadcast_to(rows[None], ref.shape)


def moments_kernel(second_hbm, first_hbm, *refs):
    vectors, (out_ref, affine_ref), scratch = refs[:4], refs[4:6], refs[6:]
    second_ref, first_ref, lines, sems = *scratch[:2], scratch[2:6], scratch[6]
    pairs = ((second_hbm, second_ref), (first_hbm, first_ref))
    copies = [
        pltpu.make_async_copy(*pair, sems.at[k])
        for k, pair in enumerate(pairs + tuple(zip(vectors, lines)))
    ]
    for copy in copies:
        copy.start()
    rows = []
    for copy, (_, ref) in zip(copies, pairs):
        copy.wait()
        frames = ref.shape[0]
        values = [ref[f].astype(jnp.float32) for f in range(frames)]
        rows += [jnp.sum(v, axis=(0, 1)).reshape(1, -1) for v in values]
        rows += [jnp.sum(v * v, axis=(0, 1)).reshape(1, -1) for v in values]
    spread(out_ref, jnp.concatenate(rows, axis=0))
    for k, (copy, line) in enumerate(zip(copies[2:], lines)):
        copy.wait()
        affine_ref[k : k + 1] = line[...].reshape(1, -1)


def moments(second, first, vectors, peers):
    frames, _, _, channels = second.shape
    return pl.pallas_call(
        moments_kernel,
        out_shape=(
            jax.ShapeDtypeStruct((peers, 4 * frames, channels), jnp.float32),
            jax.ShapeDtypeStruct((len(vectors), channels), jnp.float32),
        ),
        in_specs=HBM * (2 + len(vectors)),
        out_specs=tuple(vmem(2)),
        scratch_shapes=[
            pltpu.VMEM(second.shape, jnp.bfloat16),
            pltpu.VMEM(first.shape, jnp.bfloat16),
            *[pltpu.VMEM(v.shape, jnp.float32) for v in vectors],
            pltpu.SemaphoreType.DMA((2 + len(vectors),)),
        ],
        compiler_params=pltpu.CompilerParams(vmem_limit_bytes=16 * MIB),
        name="moments",
    )(*map(in_hbm, (second, first, *vectors)))


def fill(ext, at, block, a, b, even):
    frames, cols = block.shape[:2]
    ext[at : at + frames, 1 : cols + 1] = block
    right, left = swapped(even, a, b)
    ext[at : at + frames, 0] = left
    ext[at : at + frames, cols + 1] = right


def time_taps(ext, w_ref, taps, frames, cols):
    _, channels = ext.shape[2:]
    pairs = [(a, c) for a in taps for c in range(3)]
    left = jnp.concatenate(
        [
            ext[2 - a : 2 - a + frames, 2 - c : 2 - c + cols].reshape(-1, channels)
            for a, c in pairs
        ],
        axis=1,
    )
    right = jnp.concatenate(
        [
            jnp.concatenate([w_ref[9 * a + 3 * b + c] for a, c in pairs], axis=1)
            for b in range(3)
        ],
        axis=0,
    )
    return nt_dot(left, right)


def row_taps(wide, rows):
    count, channels = wide.shape[0], wide.shape[1] // 3
    row = lax.broadcasted_iota(jnp.int32, (count, 1), 0) % rows
    up = jnp.where(row < rows - 1, pltpu.roll(wide[:, :channels], count - 1, 0), 0.0)
    down = jnp.where(row > 0, pltpu.roll(wide[:, 2 * channels :], 1, 0), 0.0)
    return wide[:, channels : 2 * channels] + up + down


def flags(par_ref):
    return [par_ref[k : k + 1] for k in range(3)]


def swapped(even, a, b):
    odd = 1 - even
    return a * even + b * odd, b * even + a * odd


def window(par_ref, own_ref, next_ref, ra_ref, rb_ref, ran_ref, rbn_ref, ext):
    frames = own_ref.shape[0]
    even, side, later = flags(par_ref)
    fill(ext, 0, own_ref[...], ra_ref[...], rb_ref[...] * side, even)
    fill(
        ext,
        frames,
        next_ref[...] * later,
        ran_ref[...] * later,
        rbn_ref[...] * (later * side),
        even,
    )


def conv_kernel(
    par_ref,
    own_ref,
    next_ref,
    ra_ref,
    rb_ref,
    ran_ref,
    rbn_ref,
    w_hbm,
    u_ref,
    ext,
    acc,
    w_ref,
    sems,
):
    frames, cols, rows, _ = own_ref.shape
    copies = {
        a: pltpu.make_async_copy(
            w_hbm.at[pl.ds(9 * a, 9)], w_ref.at[pl.ds(9 * a, 9)], sems.at[a]
        )
        for a in (2, 1, 0)
    }
    for copy in copies.values():
        copy.start()
    window(par_ref, own_ref, next_ref, ra_ref, rb_ref, ran_ref, rbn_ref, ext)
    for a, copy in copies.items():
        copy.wait()
        part = time_taps(ext, w_ref, (a,), frames, cols)
        acc[...] = part if a == 2 else acc[...] + part
    u_ref[...] = row_taps(acc, rows)


def conv_section(par, grad, halo, kernel):
    frames, cols, rows, channels = grad.shape
    count = frames * cols * rows
    return pl.pallas_call(
        conv_kernel,
        out_shape=jax.ShapeDtypeStruct((count, channels), jnp.float32),
        in_specs=vmem(7) + HBM,
        out_specs=vmem(1)[0],
        scratch_shapes=[
            pltpu.VMEM((2 * frames, cols + 2, rows, channels), jnp.bfloat16),
            pltpu.VMEM((count, 3 * channels), jnp.float32),
            pltpu.VMEM(kernel.shape, jnp.bfloat16),
            pltpu.SemaphoreType.DMA((3,)),
        ],
        compiler_params=pltpu.CompilerParams(vmem_limit_bytes=16 * MIB),
        cost_estimate=matmul_cost(count, kernel),
        name="conv",
    )(par, grad, *halo, in_hbm(kernel))


def norm_stats(cells, base, frames, mom_ref):
    totals = group_sum(jnp.sum(mom_ref[...], axis=0)) * (1.0 / cells)
    means, scales = [], []
    for f in range(frames):
        mean = totals[base + f : base + f + 1]
        var = totals[base + frames + f : base + frames + f + 1] - mean * mean
        means.append(mean)
        scales.append(lax.rsqrt(var + EPSILON))
    return means, scales


def through(upstream, normed, gain, shift):
    pre = normed * gain + shift
    sig = jax.nn.sigmoid(pre)
    return upstream * sig * (1.0 + pre * (1.0 - sig)) * gain


def finish(cells, base, upstream, x_ref, mom_ref, affine_ref, at, q_ref, sums_ref, stats_ref):
    frames, cols, rows, channels = x_ref.shape
    means, scales = norm_stats(cells, base, frames, mom_ref)
    gain, shift = affine_ref[at : at + 1], affine_ref[at + 1 : at + 2]
    half = cols * rows
    sums, crosses = [], []
    for f in range(frames):
        normed = (x_ref[f].astype(jnp.float32).reshape(half, channels) - means[f]) * scales[f]
        q = through(upstream[f * half : (f + 1) * half], normed, gain, shift)
        q_ref[f] = q.reshape(cols, rows, channels)
        sums.append(jnp.sum(q, axis=0, keepdims=True))
        crosses.append(jnp.sum(q * normed, axis=0, keepdims=True))
    spread(sums_ref, jnp.concatenate(sums + crosses, axis=0))
    stats_ref[...] = jnp.concatenate(means + scales, axis=0)


def finish_shapes(stored, peers):
    frames, _, _, channels = stored.shape
    return (
        jax.ShapeDtypeStruct(stored.shape, jnp.float32),
        jax.ShapeDtypeStruct((peers, 2 * frames, channels), jnp.float32),
        jax.ShapeDtypeStruct((2 * frames, channels), jnp.float32),
    )


def norm_kernel(cells, u_ref, x_ref, mom_ref, affine_ref, q_ref, sums_ref, stats_ref):
    finish(cells, 0, u_ref, x_ref, mom_ref, affine_ref, 0, q_ref, sums_ref, stats_ref)


def norm_section(upstream, stored, mom, affine, cells, peers):
    return pl.pallas_call(
        functools.partial(norm_kernel, cells),
        out_shape=finish_shapes(stored, peers),
        in_specs=vmem(4),
        out_specs=tuple(vmem(3)),
        compiler_params=pltpu.CompilerParams(vmem_limit_bytes=16 * MIB),
        name="norm",
    )(upstream, stored, mom, affine)


def block_grad(cells, grad_ref, q_ref, x_ref, stats_ref, sums_ref):
    frames, cols, rows, channels = grad_ref.shape
    totals = group_sum(jnp.sum(sums_ref[...], axis=0)) * (1.0 / cells)
    result = []
    for f in range(frames):
        mean = stats_ref[f : f + 1]
        scale = stats_ref[frames + f : frames + f + 1]
        flat = (cols * rows, channels)
        normed = (x_ref[f].astype(jnp.float32).reshape(flat) - mean) * scale
        value = grad_ref[f].astype(jnp.float32).reshape(flat) + scale * (
            q_ref[f].reshape(flat)
            - totals[f : f + 1]
            - normed * totals[frames + f : frames + f + 1]
        )
        result.append(value.astype(jnp.bfloat16))
    return result


def dx_kernel(cells, par_ref, grad_ref, q_ref, x_ref, stats_ref, sums_ref, dx_ref, sa_ref, sb_ref):
    _, cols, rows, channels = grad_ref.shape
    even, _, _ = flags(par_ref)
    for f, value in enumerate(block_grad(cells, grad_ref, q_ref, x_ref, stats_ref, sums_ref)):
        value = value.reshape(cols, rows, channels)
        dx_ref[f] = value
        sa_ref[f], sb_ref[f] = swapped(even, value[cols - 1], value[0])


def dx_section(par, grad, q, stored, stats, sums, cells):
    frames, _, rows, channels = grad.shape
    edge = jax.ShapeDtypeStruct((frames, rows, channels), jnp.bfloat16)
    return pl.pallas_call(
        functools.partial(dx_kernel, cells),
        out_shape=(jax.ShapeDtypeStruct(grad.shape, jnp.bfloat16), edge, edge),
        in_specs=vmem(6),
        out_specs=tuple(vmem(3)),
        compiler_params=pltpu.CompilerParams(vmem_limit_bytes=16 * MIB),
        cost_estimate=WEIGHTS_COVER,
        name="dx",
    )(par, grad, q, stored, stats, sums)


def conv_norm_kernel(
    cells,
    base,
    par_ref,
    own_ref,
    next_ref,
    ra_ref,
    rb_ref,
    ran_ref,
    rbn_ref,
    w_ref,
    x_ref,
    mom_ref,
    affine_ref,
    q_ref,
    sums_ref,
    stats_ref,
    ext,
    acc,
):
    rows = own_ref.shape[2]
    window(par_ref, own_ref, next_ref, ra_ref, rb_ref, ran_ref, rbn_ref, ext)
    acc[...] = time_taps(ext, w_ref, (2, 1, 0), *own_ref.shape[:2])
    upstream = row_taps(acc, rows)
    finish(cells, base, upstream, x_ref, mom_ref, affine_ref, 2, q_ref, sums_ref, stats_ref)


def conv_norm_section(par, grad, halo, kernel, stored, mom, affine, cells, base, peers):
    frames, cols, rows, channels = grad.shape
    count = frames * cols * rows
    return pl.pallas_call(
        functools.partial(conv_norm_kernel, cells, base),
        out_shape=finish_shapes(stored, peers),
        in_specs=vmem(11),
        out_specs=tuple(vmem(3)),
        scratch_shapes=[
            pltpu.VMEM((2 * frames, cols + 2, rows, channels), jnp.bfloat16),
            pltpu.VMEM((count, 3 * channels), jnp.float32),
        ],
        compiler_params=pltpu.CompilerParams(vmem_limit_bytes=16 * MIB),
        cost_estimate=matmul_cost(count, kernel),
        name="convnorm",
    )(par, grad, *halo, kernel, stored, mom, affine)


def edge_kernel(par_ref, block_ref, sa_ref, sb_ref):
    cols = block_ref.shape[1]
    even, _, _ = flags(par_ref)
    sa_ref[...], sb_ref[...] = swapped(even, block_ref[:, cols - 1], block_ref[:, 0])


def edge_section(par, block):
    frames, _, rows, channels = block.shape
    edge = jax.ShapeDtypeStruct((frames, rows, channels), block.dtype)
    return pl.pallas_call(
        edge_kernel,
        out_shape=(edge, edge),
        in_specs=vmem(2),
        out_specs=tuple(vmem(2)),
        compiler_params=pltpu.CompilerParams(vmem_limit_bytes=4 * MIB),
        name="edge",
    )(par, block)


def latent_kernel_body(cells, grad_ref, q_ref, x_ref, stats_ref, sums_ref, k_ref, own_ref, prev_ref, wide):
    frames, cols, rows, channels = grad_ref.shape
    lat = k_ref.shape[1]
    lanes = own_ref.shape[-1]
    values = block_grad(cells, grad_ref, q_ref, x_ref, stats_ref, sums_ref)
    grad = jnp.concatenate(values, axis=0)
    count = frames * cols * rows
    wide[...] = jnp.zeros_like(wide)
    width = 3 * lat
    spots = (0, width, lanes)
    for b in range(3):
        for a in range(3):
            k = 9 * a + 3 * b
            wide[b, spots[a] : spots[a] + width] = k_ref[k : k + 3].reshape(width, channels)
    row = lax.broadcasted_iota(jnp.int32, (count, 1), 0) % rows
    z = [nt_dot(grad, wide[b]) for b in range(3)]
    up = jnp.where(row < rows - 1, pltpu.roll(z[0], count - 1, 0), 0.0)
    down = jnp.where(row > 0, pltpu.roll(z[2], 1, 0), 0.0)
    total = z[1] + up + down
    lane = lax.broadcasted_iota(jnp.int32, (1, lanes), 1)
    both, third = total[:, :lanes], total[:, lanes:]
    parts = (
        jnp.where(lane < width, both, 0.0),
        jnp.where(lane < width, 0.0, both),
        third,
    )
    placed = {}
    for a in range(3):
        part = parts[a].reshape(frames, cols, rows, lanes)
        base = width if a == 1 else 0
        for f in range(frames):
            out = None
            for w in range(cols):
                shift = (lat * w - base) % lanes
                one = pltpu.roll(part[f, w], shift, 1) if shift else part[f, w]
                out = one if out is None else out + one
            at = f + a - 2
            placed[at] = placed[at] + out if at in placed else out
    for f in range(frames):
        own_ref[f] = placed[f]
        prev_ref[f] = placed[f - 2]


def latent_section(grad, q, stored, stats, sums, kernel, cells):
    frames, _, rows, channels = grad.shape
    lanes = 128
    out = jax.ShapeDtypeStruct((frames, rows, lanes), jnp.float32)
    return pl.pallas_call(
        functools.partial(latent_kernel_body, cells),
        out_shape=(out, out),
        in_specs=vmem(6),
        out_specs=tuple(vmem(2)),
        scratch_shapes=[pltpu.VMEM((3, 2 * lanes, channels), jnp.bfloat16)],
        compiler_params=pltpu.CompilerParams(vmem_limit_bytes=16 * MIB),
        name="latent",
    )(grad, q, stored, stats, sums, kernel)


def assemble_kernel(lat, cols, got_ref, e_ref, perm_ref, out_ref):
    parts = {}
    for p in range(2):
        rows = jnp.concatenate([got_ref[:, p, :], got_ref[:, 2 + p, :]], axis=0)
        spots = lax.dot_general(
            jnp.concatenate(thirds(rows), axis=0),
            e_ref[...],
            (((0,), (0,)), ((), ())),
            preferred_element_type=jnp.float32,
        )
        for col in range(cols + 2):
            q = (col + 1) % 2
            piece = spots[lat * col : lat * (col + 1), 128 * col : 128 * (col + 1)]
            parts[p, q] = parts[p, q] + piece if (p, q) in parts else piece
    stacked = jnp.concatenate([parts[p, q] for p in range(2) for q in range(2)], axis=0)
    final = jnp.dot(
        perm_ref[...],
        jnp.concatenate(thirds(stacked), axis=0),
        preferred_element_type=jnp.float32,
    )
    out_ref[...] = final[:, : out_ref.shape[1]]


def assemble(got, lat, cols):
    peers, quad, _ = got.shape
    width = peers * cols // 2
    tokens = quad // 2 * width
    place = np.zeros((quad // 2, peers, (cols + 2) * 128), np.float32)
    for hh in range(quad // 2):
        for s in range(peers):
            for col in range(cols + 2):
                x = s * cols + col - 1
                if 0 <= x < peers * cols:
                    place[hh, s, 128 * col + hh * width + x // 2] = 1.0
    place = np.tile(place.reshape(-1, place.shape[-1]), (3, 1))
    perm = np.zeros((4 * lat, 4 * lat), np.float32)
    for pq in range(4):
        for one in range(lat):
            perm[one * 4 + pq, pq * lat + one] = 1.0
    perm = np.tile(perm, (1, 3))
    return pl.pallas_call(
        functools.partial(assemble_kernel, lat, cols),
        out_shape=jax.ShapeDtypeStruct((4 * lat, tokens), jnp.float32),
        in_specs=vmem(3),
        out_specs=pl.BlockSpec(memory_space=pltpu.VMEM),
        compiler_params=pltpu.CompilerParams(vmem_limit_bytes=16 * MIB),
        name="assemble",
    )(got, jnp.asarray(place, jnp.bfloat16), jnp.asarray(perm, jnp.bfloat16))


def exchange(value, send_a, send_b):
    tms = lax.axis_size("tm")
    tiles = lax.axis_size(TILE)
    back = ring(tms)
    swap = [(0, 1), (1, 0)]
    hops = []
    for k in range(1, tiles, 2):
        hops += [(k, (k + 1) % tiles), ((k + 1) % tiles, k)]
    diagonal = [(t * tiles + s, u * tiles + d) for t, u in back for s, d in hops]
    partner = [
        (t * tiles + s, u * tiles + (s ^ 1)) for t, u in back for s in range(tiles)
    ]
    nxt = lax.ppermute(value, "tm", back)
    rb = lax.ppermute(send_b, TILE, hops)
    rbn = lax.ppermute(send_b, TM_TILE, diagonal)
    ran = lax.ppermute(send_a, TM_TILE, partner)
    ra = lax.ppermute(send_a, "tile_2", swap)
    return nxt, ra, rb, ran, rbn


def ring(count):
    return [(t, (t - 1) % count) for t in range(count)]


def everyone(rows):
    return lax.all_to_all(rows, TILE, 0, 0)


def shards(
    first_input,
    second_input,
    output_grad,
    first_gain,
    first_shift,
    first_kernel,
    second_gain,
    second_shift,
    second_kernel,
    latent_kernel,
):
    frames, rows, cols, channels = first_input.shape
    peers = lax.axis_size(TILE)
    cells = rows * cols * peers * (channels // GROUPS)
    core = lax.axis_index("tile_2")
    even = core == 0
    tile, when = lax.axis_index(TILE), lax.axis_index("tm")
    later = when < lax.axis_size("tm") - 1
    side = jnp.where(even, tile > 0, tile < peers - 1)
    ones = jnp.stack([even, side, later]).astype(jnp.bfloat16)
    par = jnp.broadcast_to(ones[:, None], (3, channels))
    par, later, output_grad, second_input, first_input = lax.optimization_barrier(
        (par, later, output_grad, second_input, first_input)
    )
    turn = lambda x: with_layout_constraint(
        jnp.transpose(x, (0, 2, 1, 3)), Layout(major_to_minor=(0, 1, 2, 3))
    )

    grad = turn(output_grad)
    vectors = (second_gain, second_shift, first_gain, first_shift)
    mine, affine = moments(second_input, first_input, vectors, peers)
    mom = everyone(mine)
    halo = exchange(grad, *edge_section(par, grad))
    second, first = turn(second_input), turn(first_input)
    upstream = conv_section(par, grad, halo, second_kernel)
    q, sums, stats = norm_section(upstream, second, mom, affine, cells, peers)
    grad, send_a, send_b = dx_section(par, grad, q, second, stats, everyone(sums), cells)
    nxt, ra, rb, ran, rbn = exchange(grad, send_a, send_b)
    q, sums, stats = conv_norm_section(
        par, grad, (nxt, ra, rb, ran, rbn), first_kernel, first, mom, affine, cells,
        2 * frames, peers,
    )
    own, prev = latent_section(grad, q, first, stats, everyone(sums), latent_kernel, cells)
    tms = lax.axis_size("tm")
    own = own + jnp.where(later, lax.ppermute(prev, "tm", ring(tms)), 0.0)
    got = everyone(own.reshape(peers, frames * rows // peers, own.shape[-1]))
    return assemble(got, latent_kernel.shape[1], cols)


def solution(mesh):
    torus = Mesh(
        mesh.devices.reshape(mesh.shape["tm"], 4, 2, 2), ("tm", "tile_0", "tile_1", "tile_2")
    )
    block = P("tm", None, TILE, None)
    placed = (block, block, block) + (P(),) * 7
    return jax.shard_map(
        shards, mesh=torus, in_specs=placed, out_specs=P(None, TM_TILE), check_vma=False
    )
```

```python
import functools

import jax
import jax.numpy as jnp
import numpy as np
from jax import lax
from jax.experimental import pallas as pl
from jax.experimental.pallas import tpu as pltpu
from jax.experimental.layout import Layout, with_layout_constraint
from jax.sharding import Mesh
from jax.sharding import PartitionSpec as P

GROUPS = 32
TILE = ("tile_0", "tile_1", "tile_2")
TM_TILE = ("tm",) + TILE
EPSILON = 1e-05
MIB = 1 << 20


def vmem(count):
    return [pl.BlockSpec(memory_space=pltpu.VMEM)] * count


WEIGHTS_COVER = pl.CostEstimate(flops=1 << 33, bytes_accessed=1 << 23, transcendentals=0)
INPUTS_COVER = pl.CostEstimate(flops=1 << 31, bytes_accessed=1 << 20, transcendentals=0)
HBM = [pl.BlockSpec(memory_space=pltpu.HBM)]


def matmul_cost(count, kernel):
    return pl.CostEstimate(
        flops=2 * count * kernel.size, bytes_accessed=2 * kernel.size, transcendentals=0
    )


def in_hbm(value):
    return pltpu.with_memory_space_constraint(value, pltpu.HBM)


def nt_dot(left, right, **kw):
    return lax.dot_general(
        left, right, (((1,), (1,)), ((), ())), preferred_element_type=jnp.float32, **kw
    )


def thirds(value):
    high = value.astype(jnp.bfloat16)
    rest = value - high.astype(jnp.float32)
    middle = rest.astype(jnp.bfloat16)
    return high, middle, (rest - middle.astype(jnp.float32)).astype(jnp.bfloat16)


def group_sum(rows):
    count, channels = rows.shape
    per = channels // GROUPS
    row = lax.broadcasted_iota(jnp.int32, (channels, channels), 0) // per
    col = lax.broadcasted_iota(jnp.int32, (channels, channels), 1) // per
    same = jnp.where(row == col, 1.0, 0.0).astype(jnp.bfloat16)
    if count < 8:
        rows = jnp.concatenate([rows, jnp.zeros((8 - count, channels), jnp.float32)], axis=0)
    split = jnp.concatenate([part.astype(jnp.float32) for part in thirds(rows)], axis=0)
    sums = jnp.dot(split.astype(jnp.bfloat16), same, preferred_element_type=jnp.float32)
    return sums[0:count] + sums[8 : 8 + count] + sums[16 : 16 + count]


def spread(ref, rows):
    ref[...] = jnp.broadcast_to(rows[None], ref.shape)


def moments_kernel(second_ref, first_ref, *refs):
    vectors, (out_ref, affine_ref), (*lines, sems) = refs[:4], refs[4:6], refs[6:]
    copies = [
        pltpu.make_async_copy(*pair, sems.at[k]) for k, pair in enumerate(zip(vectors, lines))
    ]
    for copy in copies:
        copy.start()
    rows = []
    for ref in (second_ref, first_ref):
        frames = ref.shape[0]
        values = [ref[f].astype(jnp.float32) for f in range(frames)]
        rows += [jnp.sum(v, axis=(0, 1)).reshape(1, -1) for v in values]
        rows += [jnp.sum(v * v, axis=(0, 1)).reshape(1, -1) for v in values]
    spread(out_ref, jnp.concatenate(rows, axis=0))
    for k, (copy, line) in enumerate(zip(copies, lines)):
        copy.wait()
        affine_ref[k : k + 1] = line[...].reshape(1, -1)


def moments(second, first, vectors, peers):
    frames, _, _, channels = second.shape
    return pl.pallas_call(
        moments_kernel,
        out_shape=(
            jax.ShapeDtypeStruct((peers, 4 * frames, channels), jnp.float32),
            jax.ShapeDtypeStruct((len(vectors), channels), jnp.float32),
        ),
        in_specs=vmem(2) + HBM * len(vectors),
        out_specs=tuple(vmem(2)),
        scratch_shapes=[
            *[pltpu.VMEM(v.shape, jnp.float32) for v in vectors],
            pltpu.SemaphoreType.DMA((len(vectors),)),
        ],
        compiler_params=pltpu.CompilerParams(vmem_limit_bytes=16 * MIB),
        name="moments",
    )(second, first, *map(in_hbm, vectors))


def fill(ext, at, block, a, b, even):
    frames, cols = block.shape[:2]
    ext[at : at + frames, 1 : cols + 1] = block
    right, left = swapped(even, a, b)
    ext[at : at + frames, 0] = left
    ext[at : at + frames, cols + 1] = right


def time_taps(ext, w_ref, taps, frames, cols):
    _, channels = ext.shape[2:]
    pairs = [(a, c) for a in taps for c in range(3)]
    left = jnp.concatenate(
        [
            ext[2 - a : 2 - a + frames, 2 - c : 2 - c + cols].reshape(-1, channels)
            for a, c in pairs
        ],
        axis=1,
    )
    right = jnp.concatenate(
        [
            jnp.concatenate([w_ref[9 * a + 3 * b + c] for a, c in pairs], axis=1)
            for b in range(3)
        ],
        axis=0,
    )
    return nt_dot(left, right)


def row_taps(wide, rows):
    count, channels = wide.shape[0], wide.shape[1] // 3
    row = lax.broadcasted_iota(jnp.int32, (count, 1), 0) % rows
    up = jnp.where(row < rows - 1, pltpu.roll(wide[:, :channels], count - 1, 0), 0.0)
    down = jnp.where(row > 0, pltpu.roll(wide[:, 2 * channels :], 1, 0), 0.0)
    return wide[:, channels : 2 * channels] + up + down


def flags(par_ref):
    return [par_ref[k : k + 1] for k in range(3)]


def swapped(even, a, b):
    odd = 1 - even
    return a * even + b * odd, b * even + a * odd


def window(par_ref, own_ref, next_ref, ra_ref, rb_ref, ran_ref, rbn_ref, ext):
    frames = own_ref.shape[0]
    even, side, later = flags(par_ref)
    fill(ext, 0, own_ref[...], ra_ref[...], rb_ref[...] * side, even)
    fill(
        ext,
        frames,
        next_ref[...] * later,
        ran_ref[...] * later,
        rbn_ref[...] * (later * side),
        even,
    )


def conv_kernel(
    par_ref,
    own_ref,
    next_ref,
    ra_ref,
    rb_ref,
    ran_ref,
    rbn_ref,
    w_hbm,
    u_ref,
    ext,
    acc,
    w_ref,
    sems,
):
    frames, cols, rows, _ = own_ref.shape
    copies = {
        a: pltpu.make_async_copy(
            w_hbm.at[pl.ds(9 * a, 9)], w_ref.at[pl.ds(9 * a, 9)], sems.at[a]
        )
        for a in (2, 1, 0)
    }
    for copy in copies.values():
        copy.start()
    window(par_ref, own_ref, next_ref, ra_ref, rb_ref, ran_ref, rbn_ref, ext)
    for a, copy in copies.items():
        copy.wait()
        part = time_taps(ext, w_ref, (a,), frames, cols)
        acc[...] = part if a == 2 else acc[...] + part
    u_ref[...] = row_taps(acc, rows)


def conv_section(par, grad, halo, kernel):
    frames, cols, rows, channels = grad.shape
    count = frames * cols * rows
    return pl.pallas_call(
        conv_kernel,
        out_shape=jax.ShapeDtypeStruct((count, channels), jnp.float32),
        in_specs=vmem(7) + HBM,
        out_specs=vmem(1)[0],
        scratch_shapes=[
            pltpu.VMEM((2 * frames, cols + 2, rows, channels), jnp.bfloat16),
            pltpu.VMEM((count, 3 * channels), jnp.float32),
            pltpu.VMEM(kernel.shape, jnp.bfloat16),
            pltpu.SemaphoreType.DMA((3,)),
        ],
        compiler_params=pltpu.CompilerParams(vmem_limit_bytes=16 * MIB),
        cost_estimate=matmul_cost(count, kernel),
        name="conv",
    )(par, grad, *halo, in_hbm(kernel))


def norm_stats(cells, base, frames, mom_ref):
    totals = group_sum(jnp.sum(mom_ref[...], axis=0)) * (1.0 / cells)
    means, scales = [], []
    for f in range(frames):
        mean = totals[base + f : base + f + 1]
        var = totals[base + frames + f : base + frames + f + 1] - mean * mean
        means.append(mean)
        scales.append(lax.rsqrt(var + EPSILON))
    return means, scales


def through(upstream, normed, gain, shift):
    pre = normed * gain + shift
    sig = jax.nn.sigmoid(pre)
    return upstream * sig * (1.0 + pre * (1.0 - sig)) * gain


def finish(cells, base, upstream, x_ref, mom_ref, affine_ref, at, q_ref, sums_ref, stats_ref):
    frames, cols, rows, channels = x_ref.shape
    means, scales = norm_stats(cells, base, frames, mom_ref)
    gain, shift = affine_ref[at : at + 1], affine_ref[at + 1 : at + 2]
    half = cols * rows
    sums, crosses = [], []
    for f in range(frames):
        normed = (x_ref[f].astype(jnp.float32).reshape(half, channels) - means[f]) * scales[f]
        q = through(upstream[f * half : (f + 1) * half], normed, gain, shift)
        q_ref[f] = q.reshape(cols, rows, channels)
        sums.append(jnp.sum(q, axis=0, keepdims=True))
        crosses.append(jnp.sum(q * normed, axis=0, keepdims=True))
    spread(sums_ref, jnp.concatenate(sums + crosses, axis=0))
    stats_ref[...] = jnp.concatenate(means + scales, axis=0)


def finish_shapes(stored, peers):
    frames, _, _, channels = stored.shape
    return (
        jax.ShapeDtypeStruct(stored.shape, jnp.float32),
        jax.ShapeDtypeStruct((peers, 2 * frames, channels), jnp.float32),
        jax.ShapeDtypeStruct((2 * frames, channels), jnp.float32),
    )


def norm_kernel(cells, u_ref, x_ref, mom_ref, affine_ref, q_ref, sums_ref, stats_ref):
    finish(cells, 0, u_ref, x_ref, mom_ref, affine_ref, 0, q_ref, sums_ref, stats_ref)


def norm_section(upstream, stored, mom, affine, cells, peers):
    return pl.pallas_call(
        functools.partial(norm_kernel, cells),
        out_shape=finish_shapes(stored, peers),
        in_specs=vmem(4),
        out_specs=tuple(vmem(3)),
        compiler_params=pltpu.CompilerParams(vmem_limit_bytes=16 * MIB),
        name="norm",
    )(upstream, stored, mom, affine)


def block_grad(cells, grad_ref, q_ref, x_ref, stats_ref, sums_ref):
    frames, cols, rows, channels = grad_ref.shape
    totals = group_sum(jnp.sum(sums_ref[...], axis=0)) * (1.0 / cells)
    result = []
    for f in range(frames):
        mean = stats_ref[f : f + 1]
        scale = stats_ref[frames + f : frames + f + 1]
        flat = (cols * rows, channels)
        normed = (x_ref[f].astype(jnp.float32).reshape(flat) - mean) * scale
        value = grad_ref[f].astype(jnp.float32).reshape(flat) + scale * (
            q_ref[f].reshape(flat)
            - totals[f : f + 1]
            - normed * totals[frames + f : frames + f + 1]
        )
        result.append(value.astype(jnp.bfloat16))
    return result


def dx_kernel(cells, par_ref, grad_ref, q_ref, x_ref, stats_ref, sums_ref, dx_ref, sa_ref, sb_ref):
    _, cols, rows, channels = grad_ref.shape
    even, _, _ = flags(par_ref)
    for f, value in enumerate(block_grad(cells, grad_ref, q_ref, x_ref, stats_ref, sums_ref)):
        value = value.reshape(cols, rows, channels)
        dx_ref[f] = value
        sa_ref[f], sb_ref[f] = swapped(even, value[cols - 1], value[0])


def dx_section(par, grad, q, stored, stats, sums, cells):
    frames, _, rows, channels = grad.shape
    edge = jax.ShapeDtypeStruct((frames, rows, channels), jnp.bfloat16)
    return pl.pallas_call(
        functools.partial(dx_kernel, cells),
        out_shape=(jax.ShapeDtypeStruct(grad.shape, jnp.bfloat16), edge, edge),
        in_specs=vmem(6),
        out_specs=tuple(vmem(3)),
        compiler_params=pltpu.CompilerParams(vmem_limit_bytes=16 * MIB),
        cost_estimate=WEIGHTS_COVER,
        name="dx",
    )(par, grad, q, stored, stats, sums)


def conv_norm_kernel(
    cells,
    base,
    par_ref,
    own_ref,
    next_ref,
    ra_ref,
    rb_ref,
    ran_ref,
    rbn_ref,
    w_ref,
    x_ref,
    mom_ref,
    affine_ref,
    q_ref,
    sums_ref,
    stats_ref,
    ext,
    acc,
):
    rows = own_ref.shape[2]
    window(par_ref, own_ref, next_ref, ra_ref, rb_ref, ran_ref, rbn_ref, ext)
    acc[...] = time_taps(ext, w_ref, (2, 1, 0), *own_ref.shape[:2])
    upstream = row_taps(acc, rows)
    finish(cells, base, upstream, x_ref, mom_ref, affine_ref, 2, q_ref, sums_ref, stats_ref)


def conv_norm_section(par, grad, halo, kernel, stored, mom, affine, cells, base, peers):
    frames, cols, rows, channels = grad.shape
    count = frames * cols * rows
    return pl.pallas_call(
        functools.partial(conv_norm_kernel, cells, base),
        out_shape=finish_shapes(stored, peers),
        in_specs=vmem(11),
        out_specs=tuple(vmem(3)),
        scratch_shapes=[
            pltpu.VMEM((2 * frames, cols + 2, rows, channels), jnp.bfloat16),
            pltpu.VMEM((count, 3 * channels), jnp.float32),
        ],
        compiler_params=pltpu.CompilerParams(vmem_limit_bytes=16 * MIB),
        cost_estimate=matmul_cost(count, kernel),
        name="convnorm",
    )(par, grad, *halo, kernel, stored, mom, affine)


def edge_kernel(par_ref, block_ref, *out_refs):
    cols = block_ref.shape[1]
    even, _, _ = flags(par_ref)
    for ref, value in zip(out_refs, swapped(even, block_ref[:, cols - 1], block_ref[:, 0])):
        ref[...] = value


def edge_section(par, block, count, cost):
    frames, _, rows, channels = block.shape
    edge = jax.ShapeDtypeStruct((frames, rows, channels), block.dtype)
    return pl.pallas_call(
        edge_kernel,
        out_shape=(edge,) * count,
        in_specs=vmem(2),
        out_specs=tuple(vmem(count)),
        compiler_params=pltpu.CompilerParams(vmem_limit_bytes=4 * MIB),
        cost_estimate=cost,
        name="edge",
    )(par, block)


def latent_kernel_body(cells, grad_ref, q_ref, x_ref, stats_ref, sums_ref, k_ref, own_ref, prev_ref, wide):
    frames, cols, rows, channels = grad_ref.shape
    lat = k_ref.shape[1]
    lanes = own_ref.shape[-1]
    values = block_grad(cells, grad_ref, q_ref, x_ref, stats_ref, sums_ref)
    grad = jnp.concatenate(values, axis=0)
    count = frames * cols * rows
    wide[...] = jnp.zeros_like(wide)
    width = 3 * lat
    spots = (0, width, lanes)
    for b in range(3):
        for a in range(3):
            k = 9 * a + 3 * b
            wide[b, spots[a] : spots[a] + width] = k_ref[k : k + 3].reshape(width, channels)
    row = lax.broadcasted_iota(jnp.int32, (count, 1), 0) % rows
    z = [nt_dot(grad, wide[b]) for b in range(3)]
    up = jnp.where(row < rows - 1, pltpu.roll(z[0], count - 1, 0), 0.0)
    down = jnp.where(row > 0, pltpu.roll(z[2], 1, 0), 0.0)
    total = z[1] + up + down
    lane = lax.broadcasted_iota(jnp.int32, (1, lanes), 1)
    both, third = total[:, :lanes], total[:, lanes:]
    parts = (
        jnp.where(lane < width, both, 0.0),
        jnp.where(lane < width, 0.0, both),
        third,
    )
    placed = {}
    for a in range(3):
        part = parts[a].reshape(frames, cols, rows, lanes)
        base = width if a == 1 else 0
        for f in range(frames):
            out = None
            for w in range(cols):
                shift = (lat * w - base) % lanes
                one = pltpu.roll(part[f, w], shift, 1) if shift else part[f, w]
                out = one if out is None else out + one
            at = f + a - 2
            placed[at] = placed[at] + out if at in placed else out
    for f in range(frames):
        own_ref[f] = placed[f]
        prev_ref[f] = placed[f - 2]


def latent_section(grad, q, stored, stats, sums, kernel, cells):
    frames, _, rows, channels = grad.shape
    lanes = 128
    out = jax.ShapeDtypeStruct((frames, rows, lanes), jnp.float32)
    return pl.pallas_call(
        functools.partial(latent_kernel_body, cells),
        out_shape=(out, out),
        in_specs=vmem(6),
        out_specs=tuple(vmem(2)),
        scratch_shapes=[pltpu.VMEM((3, 2 * lanes, channels), jnp.bfloat16)],
        compiler_params=pltpu.CompilerParams(vmem_limit_bytes=16 * MIB),
        name="latent",
    )(grad, q, stored, stats, sums, kernel)


def assemble_kernel(lat, cols, got_ref, e_ref, perm_ref, out_ref):
    parts = {}
    for p in range(2):
        rows = jnp.concatenate([got_ref[:, p, :], got_ref[:, 2 + p, :]], axis=0)
        spots = lax.dot_general(
            jnp.concatenate(thirds(rows), axis=0),
            e_ref[...],
            (((0,), (0,)), ((), ())),
            preferred_element_type=jnp.float32,
        )
        for col in range(cols + 2):
            q = (col + 1) % 2
            piece = spots[lat * col : lat * (col + 1), 128 * col : 128 * (col + 1)]
            parts[p, q] = parts[p, q] + piece if (p, q) in parts else piece
    stacked = jnp.concatenate([parts[p, q] for p in range(2) for q in range(2)], axis=0)
    final = jnp.dot(
        perm_ref[...],
        jnp.concatenate(thirds(stacked), axis=0),
        preferred_element_type=jnp.float32,
    )
    out_ref[...] = final[:, : out_ref.shape[1]]


def assemble(got, lat, cols):
    peers, quad, _ = got.shape
    width = peers * cols // 2
    tokens = quad // 2 * width
    place = np.zeros((quad // 2, peers, (cols + 2) * 128), np.float32)
    for hh in range(quad // 2):
        for s in range(peers):
            for col in range(cols + 2):
                x = s * cols + col - 1
                if 0 <= x < peers * cols:
                    place[hh, s, 128 * col + hh * width + x // 2] = 1.0
    place = np.tile(place.reshape(-1, place.shape[-1]), (3, 1))
    perm = np.zeros((4 * lat, 4 * lat), np.float32)
    for pq in range(4):
        for one in range(lat):
            perm[one * 4 + pq, pq * lat + one] = 1.0
    perm = np.tile(perm, (1, 3))
    return pl.pallas_call(
        functools.partial(assemble_kernel, lat, cols),
        out_shape=jax.ShapeDtypeStruct((4 * lat, tokens), jnp.float32),
        in_specs=vmem(3),
        out_specs=pl.BlockSpec(memory_space=pltpu.VMEM),
        compiler_params=pltpu.CompilerParams(vmem_limit_bytes=16 * MIB),
        name="assemble",
    )(got, jnp.asarray(place, jnp.bfloat16), jnp.asarray(perm, jnp.bfloat16))


def exchange(par, value, send_a, send_b):
    tms = lax.axis_size("tm")
    tiles = lax.axis_size(TILE)
    back = ring(tms)
    swap = [(0, 1), (1, 0)]
    hops = []
    for k in range(1, tiles, 2):
        hops += [(k, (k + 1) % tiles), ((k + 1) % tiles, k)]
    diagonal = [(t * tiles + s, u * tiles + d) for t, u in back for s, d in hops]
    nxt = lax.ppermute(value, "tm", back)
    rb = lax.ppermute(send_b, TILE, hops)
    rbn = lax.ppermute(send_b, TM_TILE, diagonal)
    ra = lax.ppermute(send_a, "tile_2", swap)
    (corner,) = edge_section(par, nxt, 1, None)
    ran = lax.ppermute(corner, "tile_2", swap)
    return nxt, ra, rb, ran, rbn


def ring(count):
    return [(t, (t - 1) % count) for t in range(count)]


def everyone(rows):
    return lax.all_to_all(rows, TILE, 0, 0)


def shards(
    first_input,
    second_input,
    output_grad,
    first_gain,
    first_shift,
    first_kernel,
    second_gain,
    second_shift,
    second_kernel,
    latent_kernel,
):
    frames, rows, cols, channels = first_input.shape
    peers = lax.axis_size(TILE)
    cells = rows * cols * peers * (channels // GROUPS)
    core = lax.axis_index("tile_2")
    even = core == 0
    tile, when = lax.axis_index(TILE), lax.axis_index("tm")
    later = when < lax.axis_size("tm") - 1
    side = jnp.where(even, tile > 0, tile < peers - 1)
    ones = jnp.stack([even, side, later]).astype(jnp.bfloat16)
    par = jnp.broadcast_to(ones[:, None], (3, channels))
    par, later, output_grad, second_input, first_input = lax.optimization_barrier(
        (par, later, output_grad, second_input, first_input)
    )
    turn = lambda x: with_layout_constraint(
        jnp.transpose(x, (0, 2, 1, 3)), Layout(major_to_minor=(0, 1, 2, 3))
    )

    grad = turn(output_grad)
    vectors = (second_gain, second_shift, first_gain, first_shift)
    mine, affine = moments(second_input, first_input, vectors, peers)
    mom = everyone(mine)
    halo = exchange(par, grad, *edge_section(par, grad, 2, INPUTS_COVER))
    second, first = turn(second_input), turn(first_input)
    upstream = conv_section(par, grad, halo, second_kernel)
    q, sums, stats = norm_section(upstream, second, mom, affine, cells, peers)
    grad, send_a, send_b = dx_section(par, grad, q, second, stats, everyone(sums), cells)
    nxt, ra, rb, ran, rbn = exchange(par, grad, send_a, send_b)
    q, sums, stats = conv_norm_section(
        par, grad, (nxt, ra, rb, ran, rbn), first_kernel, first, mom, affine, cells,
        2 * frames, peers,
    )
    own, prev = latent_section(grad, q, first, stats, everyone(sums), latent_kernel, cells)
    tms = lax.axis_size("tm")
    own = own + jnp.where(later, lax.ppermute(prev, "tm", ring(tms)), 0.0)
    got = everyone(own.reshape(peers, frames * rows // peers, own.shape[-1]))
    return assemble(got, latent_kernel.shape[1], cols)


def solution(mesh):
    torus = Mesh(
        mesh.devices.reshape(mesh.shape["tm"], 4, 2, 2), ("tm", "tile_0", "tile_1", "tile_2")
    )
    block = P("tm", None, TILE, None)
    placed = (block, block, block) + (P(),) * 7
    return jax.shard_map(
        shards, mesh=torus, in_specs=placed, out_specs=P(None, TM_TILE), check_vma=False
    )
```

```python
import functools

import jax
import jax.numpy as jnp
import numpy as np
from jax import lax
from jax.experimental import pallas as pl
from jax.experimental.pallas import tpu as pltpu
from jax.experimental.layout import Layout, with_layout_constraint
from jax.sharding import Mesh
from jax.sharding import PartitionSpec as P

GROUPS = 32
TILE = ("tile_0", "tile_1", "tile_2")
TM_TILE = ("tm",) + TILE
EPSILON = 1e-05
MIB = 1 << 20


def vmem(count):
    return [pl.BlockSpec(memory_space=pltpu.VMEM)] * count


WEIGHTS_COVER = pl.CostEstimate(flops=1 << 33, bytes_accessed=1 << 23, transcendentals=0)
WEIGHTS_WINDOW = pl.CostEstimate(
    flops=1 << 33, bytes_accessed=1 << 23, transcendentals=300000000
)
INPUTS_COVER = pl.CostEstimate(flops=1 << 31, bytes_accessed=1 << 20, transcendentals=0)
HBM = [pl.BlockSpec(memory_space=pltpu.HBM)]


def matmul_cost(count, kernel):
    return pl.CostEstimate(
        flops=2 * count * kernel.size, bytes_accessed=2 * kernel.size, transcendentals=0
    )


def nt_dot(left, right, **kw):
    return lax.dot_general(
        left, right, (((1,), (1,)), ((), ())), preferred_element_type=jnp.float32, **kw
    )


def thirds(value):
    high = value.astype(jnp.bfloat16)
    rest = value - high.astype(jnp.float32)
    middle = rest.astype(jnp.bfloat16)
    return high, middle, (rest - middle.astype(jnp.float32)).astype(jnp.bfloat16)


def group_sum(rows):
    count, channels = rows.shape
    per = channels // GROUPS
    row = lax.broadcasted_iota(jnp.int32, (channels, channels), 0) // per
    col = lax.broadcasted_iota(jnp.int32, (channels, channels), 1) // per
    same = jnp.where(row == col, 1.0, 0.0).astype(jnp.bfloat16)
    if count < 8:
        rows = jnp.concatenate([rows, jnp.zeros((8 - count, channels), jnp.float32)], axis=0)
    split = jnp.concatenate([part.astype(jnp.float32) for part in thirds(rows)], axis=0)
    sums = jnp.dot(split.astype(jnp.bfloat16), same, preferred_element_type=jnp.float32)
    return sums[0:count] + sums[8 : 8 + count] + sums[16 : 16 + count]


def spread(ref, rows):
    ref[...] = jnp.broadcast_to(rows[None], ref.shape)


def moments_kernel(second_ref, first_ref, *refs):
    *vectors, out_ref, affine_ref = refs
    rows = []
    for ref in (second_ref, first_ref):
        frames = ref.shape[0]
        values = [ref[f].astype(jnp.float32) for f in range(frames)]
        rows += [jnp.sum(v, axis=(0, 1)).reshape(1, -1) for v in values]
        rows += [jnp.sum(v * v, axis=(0, 1)).reshape(1, -1) for v in values]
    spread(out_ref, jnp.concatenate(rows, axis=0))
    for k, line in enumerate(vectors):
        affine_ref[k : k + 1] = line[...].reshape(1, -1)


def moments(second, first, vectors, peers):
    frames, _, _, channels = second.shape
    return pl.pallas_call(
        moments_kernel,
        out_shape=(
            jax.ShapeDtypeStruct((peers, 4 * frames, channels), jnp.float32),
            jax.ShapeDtypeStruct((len(vectors), channels), jnp.float32),
        ),
        in_specs=vmem(2 + len(vectors)),
        out_specs=tuple(vmem(2)),
        compiler_params=pltpu.CompilerParams(vmem_limit_bytes=16 * MIB),
        name="moments",
    )(second, first, *vectors)


def fill(ext, at, block, a, b, even):
    frames, cols = block.shape[:2]
    ext[at : at + frames, 1 : cols + 1] = block
    right, left = swapped(even, a, b)
    ext[at : at + frames, 0] = left
    ext[at : at + frames, cols + 1] = right


def time_taps(ext, w_ref, taps, frames, cols):
    _, channels = ext.shape[2:]
    pairs = [(a, c) for a in taps for c in range(3)]
    left = jnp.concatenate(
        [
            ext[2 - a : 2 - a + frames, 2 - c : 2 - c + cols].reshape(-1, channels)
            for a, c in pairs
        ],
        axis=1,
    )
    right = jnp.concatenate(
        [
            jnp.concatenate([w_ref[9 * a + 3 * b + c] for a, c in pairs], axis=1)
            for b in range(3)
        ],
        axis=0,
    )
    return nt_dot(left, right)


def row_taps(wide, rows):
    count, channels = wide.shape[0], wide.shape[1] // 3
    row = lax.broadcasted_iota(jnp.int32, (count, 1), 0) % rows
    up = jnp.where(row < rows - 1, pltpu.roll(wide[:, :channels], count - 1, 0), 0.0)
    down = jnp.where(row > 0, pltpu.roll(wide[:, 2 * channels :], 1, 0), 0.0)
    return wide[:, channels : 2 * channels] + up + down


def flags(par_ref):
    return [par_ref[k : k + 1] for k in range(3)]


def swapped(even, a, b):
    odd = 1 - even
    return a * even + b * odd, b * even + a * odd


def window(par_ref, own_ref, next_ref, ra_ref, rb_ref, ran_ref, rbn_ref, ext):
    frames = own_ref.shape[0]
    even, side, later = flags(par_ref)
    fill(ext, 0, own_ref[...], ra_ref[...], rb_ref[...] * side, even)
    fill(
        ext,
        frames,
        next_ref[...] * later,
        jnp.zeros_like(rbn_ref) if ran_ref is None else ran_ref[...] * later,
        rbn_ref[...] * (later * side),
        even,
    )


def gather_kernel(par_ref, own_ref, next_ref, ra_ref, rb_ref, rbn_ref, ext_ref, corner_ref):
    even, _, _ = flags(par_ref)
    cols = own_ref.shape[1]
    window(par_ref, own_ref, next_ref, ra_ref, rb_ref, None, rbn_ref, ext_ref)
    corner_ref[...], _ = swapped(even, next_ref[:, cols - 1], next_ref[:, 0])


def gather_section(par, own, nxt, ra, rb, rbn):
    frames, cols, rows, channels = own.shape
    return pl.pallas_call(
        gather_kernel,
        out_shape=(
            jax.ShapeDtypeStruct((2 * frames, cols + 2, rows, channels), own.dtype),
            jax.ShapeDtypeStruct((frames, rows, channels), own.dtype),
        ),
        in_specs=vmem(6),
        out_specs=tuple(vmem(2)),
        compiler_params=pltpu.CompilerParams(vmem_limit_bytes=4 * MIB),
        cost_estimate=WEIGHTS_WINDOW,
        name="gather",
    )(par, own, nxt, ra, rb, rbn)


def conv_kernel(par_ref, part_ref, ran_ref, w_ref, u_ref, ext, acc):
    frames, rows = ran_ref.shape[:2]
    cols = part_ref.shape[1] - 2
    even, _, later = flags(par_ref)
    ext[...] = part_ref[...]
    right, left = swapped(even, ran_ref[...] * later, jnp.zeros_like(ran_ref))
    ext[frames:, 0] = part_ref[frames:, 0] + left
    ext[frames:, cols + 1] = part_ref[frames:, cols + 1] + right
    acc[...] = time_taps(ext, w_ref, (2, 1, 0), frames, cols)
    u_ref[...] = row_taps(acc, rows)


def conv_section(par, part, ran, kernel):
    frames, rows, channels = ran.shape
    cols = part.shape[1] - 2
    count = frames * cols * rows
    return pl.pallas_call(
        conv_kernel,
        out_shape=jax.ShapeDtypeStruct((count, channels), jnp.float32),
        in_specs=vmem(4),
        out_specs=vmem(1)[0],
        scratch_shapes=[
            pltpu.VMEM(part.shape, jnp.bfloat16),
            pltpu.VMEM((count, 3 * channels), jnp.float32),
        ],
        compiler_params=pltpu.CompilerParams(vmem_limit_bytes=16 * MIB),
        cost_estimate=matmul_cost(count, kernel),
        name="conv",
    )(par, part, ran, kernel)


def norm_stats(cells, base, frames, mom_ref):
    totals = group_sum(jnp.sum(mom_ref[...], axis=0)) * (1.0 / cells)
    means, scales = [], []
    for f in range(frames):
        mean = totals[base + f : base + f + 1]
        var = totals[base + frames + f : base + frames + f + 1] - mean * mean
        means.append(mean)
        scales.append(lax.rsqrt(var + EPSILON))
    return means, scales


def through(upstream, normed, gain, shift):
    pre = normed * gain + shift
    sig = jax.nn.sigmoid(pre)
    return upstream * sig * (1.0 + pre * (1.0 - sig)) * gain


def finish(cells, base, upstream, x_ref, mom_ref, affine_ref, at, q_ref, sums_ref, stats_ref):
    frames, cols, rows, channels = x_ref.shape
    means, scales = norm_stats(cells, base, frames, mom_ref)
    gain, shift = affine_ref[at : at + 1], affine_ref[at + 1 : at + 2]
    half = cols * rows
    sums, crosses = [], []
    for f in range(frames):
        normed = (x_ref[f].astype(jnp.float32).reshape(half, channels) - means[f]) * scales[f]
        q = through(upstream[f * half : (f + 1) * half], normed, gain, shift)
        q_ref[f] = q.reshape(cols, rows, channels)
        sums.append(jnp.sum(q, axis=0, keepdims=True))
        crosses.append(jnp.sum(q * normed, axis=0, keepdims=True))
    spread(sums_ref, jnp.concatenate(sums + crosses, axis=0))
    stats_ref[...] = jnp.concatenate(means + scales, axis=0)


def finish_shapes(stored, peers):
    frames, _, _, channels = stored.shape
    return (
        jax.ShapeDtypeStruct(stored.shape, jnp.float32),
        jax.ShapeDtypeStruct((peers, 2 * frames, channels), jnp.float32),
        jax.ShapeDtypeStruct((2 * frames, channels), jnp.float32),
    )


def norm_kernel(cells, u_ref, x_ref, mom_ref, affine_ref, q_ref, sums_ref, stats_ref):
    finish(cells, 0, u_ref, x_ref, mom_ref, affine_ref, 0, q_ref, sums_ref, stats_ref)


def norm_section(upstream, stored, mom, affine, cells, peers):
    return pl.pallas_call(
        functools.partial(norm_kernel, cells),
        out_shape=finish_shapes(stored, peers),
        in_specs=vmem(4),
        out_specs=tuple(vmem(3)),
        compiler_params=pltpu.CompilerParams(vmem_limit_bytes=16 * MIB),
        name="norm",
    )(upstream, stored, mom, affine)


def block_grad(cells, grad_ref, q_ref, x_ref, stats_ref, sums_ref):
    frames, cols, rows, channels = grad_ref.shape
    totals = group_sum(jnp.sum(sums_ref[...], axis=0)) * (1.0 / cells)
    result = []
    for f in range(frames):
        mean = stats_ref[f : f + 1]
        scale = stats_ref[frames + f : frames + f + 1]
        flat = (cols * rows, channels)
        normed = (x_ref[f].astype(jnp.float32).reshape(flat) - mean) * scale
        value = grad_ref[f].astype(jnp.float32).reshape(flat) + scale * (
            q_ref[f].reshape(flat)
            - totals[f : f + 1]
            - normed * totals[frames + f : frames + f + 1]
        )
        result.append(value.astype(jnp.bfloat16))
    return result


def dx_kernel(cells, par_ref, grad_ref, q_ref, x_ref, stats_ref, sums_ref, dx_ref, sa_ref, sb_ref):
    _, cols, rows, channels = grad_ref.shape
    even, _, _ = flags(par_ref)
    for f, value in enumerate(block_grad(cells, grad_ref, q_ref, x_ref, stats_ref, sums_ref)):
        value = value.reshape(cols, rows, channels)
        dx_ref[f] = value
        sa_ref[f], sb_ref[f] = swapped(even, value[cols - 1], value[0])


def dx_section(par, grad, q, stored, stats, sums, cells):
    frames, _, rows, channels = grad.shape
    edge = jax.ShapeDtypeStruct((frames, rows, channels), jnp.bfloat16)
    return pl.pallas_call(
        functools.partial(dx_kernel, cells),
        out_shape=(jax.ShapeDtypeStruct(grad.shape, jnp.bfloat16), edge, edge),
        in_specs=vmem(6),
        out_specs=tuple(vmem(3)),
        compiler_params=pltpu.CompilerParams(vmem_limit_bytes=16 * MIB),
        cost_estimate=WEIGHTS_COVER,
        name="dx",
    )(par, grad, q, stored, stats, sums)


def conv_norm_kernel(
    cells,
    base,
    par_ref,
    own_ref,
    next_ref,
    ra_ref,
    rb_ref,
    ran_ref,
    rbn_ref,
    w_ref,
    x_ref,
    mom_ref,
    affine_ref,
    q_ref,
    sums_ref,
    stats_ref,
    ext,
    acc,
):
    rows = own_ref.shape[2]
    window(par_ref, own_ref, next_ref, ra_ref, rb_ref, ran_ref, rbn_ref, ext)
    acc[...] = time_taps(ext, w_ref, (2, 1, 0), *own_ref.shape[:2])
    upstream = row_taps(acc, rows)
    finish(cells, base, upstream, x_ref, mom_ref, affine_ref, 2, q_ref, sums_ref, stats_ref)


def conv_norm_section(par, grad, halo, kernel, stored, mom, affine, cells, base, peers):
    frames, cols, rows, channels = grad.shape
    count = frames * cols * rows
    return pl.pallas_call(
        functools.partial(conv_norm_kernel, cells, base),
        out_shape=finish_shapes(stored, peers),
        in_specs=vmem(11),
        out_specs=tuple(vmem(3)),
        scratch_shapes=[
            pltpu.VMEM((2 * frames, cols + 2, rows, channels), jnp.bfloat16),
            pltpu.VMEM((count, 3 * channels), jnp.float32),
        ],
        compiler_params=pltpu.CompilerParams(vmem_limit_bytes=16 * MIB),
        cost_estimate=matmul_cost(count, kernel),
        name="convnorm",
    )(par, grad, *halo, kernel, stored, mom, affine)


def edge_kernel(par_ref, block_ref, *out_refs):
    cols = block_ref.shape[1]
    even, _, _ = flags(par_ref)
    for ref, value in zip(out_refs, swapped(even, block_ref[:, cols - 1], block_ref[:, 0])):
        ref[...] = value


def edge_section(par, block, count, cost):
    frames, _, rows, channels = block.shape
    edge = jax.ShapeDtypeStruct((frames, rows, channels), block.dtype)
    return pl.pallas_call(
        edge_kernel,
        out_shape=(edge,) * count,
        in_specs=vmem(2),
        out_specs=tuple(vmem(count)),
        compiler_params=pltpu.CompilerParams(vmem_limit_bytes=4 * MIB),
        cost_estimate=cost,
        name="edge",
    )(par, block)


def latent_kernel_body(cells, grad_ref, q_ref, x_ref, stats_ref, sums_ref, k_ref, own_ref, prev_ref, wide):
    frames, cols, rows, channels = grad_ref.shape
    lat = k_ref.shape[1]
    lanes = own_ref.shape[-1]
    values = block_grad(cells, grad_ref, q_ref, x_ref, stats_ref, sums_ref)
    grad = jnp.concatenate(values, axis=0)
    count = frames * cols * rows
    wide[...] = jnp.zeros_like(wide)
    width = 3 * lat
    spots = (0, width, lanes)
    for b in range(3):
        for a in range(3):
            k = 9 * a + 3 * b
            wide[b, spots[a] : spots[a] + width] = k_ref[k : k + 3].reshape(width, channels)
    row = lax.broadcasted_iota(jnp.int32, (count, 1), 0) % rows
    z = [nt_dot(grad, wide[b]) for b in range(3)]
    up = jnp.where(row < rows - 1, pltpu.roll(z[0], count - 1, 0), 0.0)
    down = jnp.where(row > 0, pltpu.roll(z[2], 1, 0), 0.0)
    total = z[1] + up + down
    lane = lax.broadcasted_iota(jnp.int32, (1, lanes), 1)
    both, third = total[:, :lanes], total[:, lanes:]
    parts = (
        jnp.where(lane < width, both, 0.0),
        jnp.where(lane < width, 0.0, both),
        third,
    )
    placed = {}
    for a in range(3):
        part = parts[a].reshape(frames, cols, rows, lanes)
        base = width if a == 1 else 0
        for f in range(frames):
            out = None
            for w in range(cols):
                shift = (lat * w - base) % lanes
                one = pltpu.roll(part[f, w], shift, 1) if shift else part[f, w]
                out = one if out is None else out + one
            at = f + a - 2
            placed[at] = placed[at] + out if at in placed else out
    for f in range(frames):
        own_ref[f] = placed[f]
        prev_ref[f] = placed[f - 2]


def latent_section(grad, q, stored, stats, sums, kernel, cells):
    frames, _, rows, channels = grad.shape
    lanes = 128
    out = jax.ShapeDtypeStruct((frames, rows, lanes), jnp.float32)
    return pl.pallas_call(
        functools.partial(latent_kernel_body, cells),
        out_shape=(out, out),
        in_specs=vmem(6),
        out_specs=tuple(vmem(2)),
        scratch_shapes=[pltpu.VMEM((3, 2 * lanes, channels), jnp.bfloat16)],
        compiler_params=pltpu.CompilerParams(vmem_limit_bytes=16 * MIB),
        name="latent",
    )(grad, q, stored, stats, sums, kernel)


def assemble_kernel(lat, cols, got_ref, e_ref, perm_ref, out_ref):
    parts = {}
    for p in range(2):
        rows = jnp.concatenate([got_ref[:, p, :], got_ref[:, 2 + p, :]], axis=0)
        spots = lax.dot_general(
            jnp.concatenate(thirds(rows), axis=0),
            e_ref[...],
            (((0,), (0,)), ((), ())),
            preferred_element_type=jnp.float32,
        )
        for col in range(cols + 2):
            q = (col + 1) % 2
            piece = spots[lat * col : lat * (col + 1), 128 * col : 128 * (col + 1)]
            parts[p, q] = parts[p, q] + piece if (p, q) in parts else piece
    stacked = jnp.concatenate([parts[p, q] for p in range(2) for q in range(2)], axis=0)
    final = jnp.dot(
        perm_ref[...],
        jnp.concatenate(thirds(stacked), axis=0),
        preferred_element_type=jnp.float32,
    )
    out_ref[...] = final[:, : out_ref.shape[1]]


def assemble(got, lat, cols):
    peers, quad, _ = got.shape
    width = peers * cols // 2
    tokens = quad // 2 * width
    place = np.zeros((quad // 2, peers, (cols + 2) * 128), np.float32)
    for hh in range(quad // 2):
        for s in range(peers):
            for col in range(cols + 2):
                x = s * cols + col - 1
                if 0 <= x < peers * cols:
                    place[hh, s, 128 * col + hh * width + x // 2] = 1.0
    place = np.tile(place.reshape(-1, place.shape[-1]), (3, 1))
    perm = np.zeros((4 * lat, 4 * lat), np.float32)
    for pq in range(4):
        for one in range(lat):
            perm[one * 4 + pq, pq * lat + one] = 1.0
    perm = np.tile(perm, (1, 3))
    return pl.pallas_call(
        functools.partial(assemble_kernel, lat, cols),
        out_shape=jax.ShapeDtypeStruct((4 * lat, tokens), jnp.float32),
        in_specs=vmem(3),
        out_specs=pl.BlockSpec(memory_space=pltpu.VMEM),
        compiler_params=pltpu.CompilerParams(vmem_limit_bytes=16 * MIB),
        name="assemble",
    )(got, jnp.asarray(place, jnp.bfloat16), jnp.asarray(perm, jnp.bfloat16))


def routes():
    tms, tiles = lax.axis_size("tm"), lax.axis_size(TILE)
    back = ring(tms)
    hops = []
    for k in range(1, tiles, 2):
        hops += [(k, (k + 1) % tiles), ((k + 1) % tiles, k)]
    diagonal = [(t * tiles + s, u * tiles + d) for t, u in back for s, d in hops]
    return back, hops, diagonal


SWAP = [(0, 1), (1, 0)]


def exchange(value, send_a, send_b):
    back, hops, diagonal = routes()
    nxt = lax.ppermute(value, "tm", back)
    rb = lax.ppermute(send_b, TILE, hops)
    rbn = lax.ppermute(send_b, TM_TILE, diagonal)
    ra = lax.ppermute(send_a, "tile_2", SWAP)
    return nxt, ra, rb, rbn


def ring(count):
    return [(t, (t - 1) % count) for t in range(count)]


def everyone(rows):
    return lax.all_to_all(rows, TILE, 0, 0)


def shards(
    first_input,
    second_input,
    output_grad,
    first_gain,
    first_shift,
    first_kernel,
    second_gain,
    second_shift,
    second_kernel,
    latent_kernel,
):
    frames, rows, cols, channels = first_input.shape
    peers = lax.axis_size(TILE)
    cells = rows * cols * peers * (channels // GROUPS)
    core = lax.axis_index("tile_2")
    even = core == 0
    tile, when = lax.axis_index(TILE), lax.axis_index("tm")
    later = when < lax.axis_size("tm") - 1
    side = jnp.where(even, tile > 0, tile < peers - 1)
    ones = jnp.stack([even, side, later]).astype(jnp.bfloat16)
    par = jnp.broadcast_to(ones[:, None], (3, channels))
    par, later, output_grad, second_input, first_input = lax.optimization_barrier(
        (par, later, output_grad, second_input, first_input)
    )
    turn = lambda x: with_layout_constraint(
        jnp.transpose(x, (0, 2, 1, 3)), Layout(major_to_minor=(0, 1, 2, 3))
    )

    grad = turn(output_grad)
    vectors = (second_gain, second_shift, first_gain, first_shift)
    mine, affine = moments(second_input, first_input, vectors, peers)
    mom = everyone(mine)
    nxt, ra, rb, rbn = exchange(grad, *edge_section(par, grad, 2, INPUTS_COVER))
    part, corner = gather_section(par, grad, nxt, ra, rb, rbn)
    ran = lax.ppermute(corner, "tile_2", SWAP)
    second, first = turn(second_input), turn(first_input)
    upstream = conv_section(par, part, ran, second_kernel)
    q, sums, stats = norm_section(upstream, second, mom, affine, cells, peers)
    grad, send_a, send_b = dx_section(par, grad, q, second, stats, everyone(sums), cells)
    nxt, ra, rb, rbn = exchange(grad, send_a, send_b)
    (corner,) = edge_section(par, nxt, 1, None)
    ran = lax.ppermute(corner, "tile_2", SWAP)
    q, sums, stats = conv_norm_section(
        par, grad, (nxt, ra, rb, ran, rbn), first_kernel, first, mom, affine, cells,
        2 * frames, peers,
    )
    own, prev = latent_section(grad, q, first, stats, everyone(sums), latent_kernel, cells)
    tms = lax.axis_size("tm")
    own = own + jnp.where(later, lax.ppermute(prev, "tm", ring(tms)), 0.0)
    got = everyone(own.reshape(peers, frames * rows // peers, own.shape[-1]))
    return assemble(got, latent_kernel.shape[1], cols)


def solution(mesh):
    torus = Mesh(
        mesh.devices.reshape(mesh.shape["tm"], 4, 2, 2), ("tm", "tile_0", "tile_1", "tile_2")
    )
    block = P("tm", None, TILE, None)
    placed = (block, block, block) + (P(),) * 7
    return jax.shard_map(
        shards, mesh=torus, in_specs=placed, out_specs=P(None, TM_TILE), check_vma=False
    )
```

```python
import functools

import jax
import jax.numpy as jnp
import numpy as np
from jax import lax
from jax.experimental import pallas as pl
from jax.experimental.pallas import tpu as pltpu
from jax.experimental.layout import Layout, with_layout_constraint
from jax.sharding import Mesh
from jax.sharding import PartitionSpec as P

GROUPS = 32
TILE = ("tile_0", "tile_1", "tile_2")
TM_TILE = ("tm",) + TILE
EPSILON = 1e-05
MIB = 1 << 20


def vmem(count):
    return [pl.BlockSpec(memory_space=pltpu.VMEM)] * count


WEIGHTS_COVER = pl.CostEstimate(flops=1 << 33, bytes_accessed=1 << 23, transcendentals=0)
INPUTS_COVER = pl.CostEstimate(flops=1 << 31, bytes_accessed=1 << 20, transcendentals=0)
HBM = [pl.BlockSpec(memory_space=pltpu.HBM)]


def matmul_cost(count, kernel):
    return pl.CostEstimate(
        flops=2 * count * kernel.size, bytes_accessed=2 * kernel.size, transcendentals=0
    )


def in_hbm(value):
    return pltpu.with_memory_space_constraint(value, pltpu.HBM)


def nt_dot(left, right, **kw):
    return lax.dot_general(
        left, right, (((1,), (1,)), ((), ())), preferred_element_type=jnp.float32, **kw
    )


def thirds(value):
    high = value.astype(jnp.bfloat16)
    rest = value - high.astype(jnp.float32)
    middle = rest.astype(jnp.bfloat16)
    return high, middle, (rest - middle.astype(jnp.float32)).astype(jnp.bfloat16)


def group_sum(rows):
    count, channels = rows.shape
    per = channels // GROUPS
    row = lax.broadcasted_iota(jnp.int32, (channels, channels), 0) // per
    col = lax.broadcasted_iota(jnp.int32, (channels, channels), 1) // per
    same = jnp.where(row == col, 1.0, 0.0).astype(jnp.bfloat16)
    if count < 8:
        rows = jnp.concatenate([rows, jnp.zeros((8 - count, channels), jnp.float32)], axis=0)
    split = jnp.concatenate([part.astype(jnp.float32) for part in thirds(rows)], axis=0)
    sums = jnp.dot(split.astype(jnp.bfloat16), same, preferred_element_type=jnp.float32)
    return sums[0:count] + sums[8 : 8 + count] + sums[16 : 16 + count]


def spread(ref, rows):
    ref[...] = jnp.broadcast_to(rows[None], ref.shape)


def moments_kernel(second_ref, first_ref, *refs):
    *vectors, out_ref, affine_ref = refs
    rows = []
    for ref in (second_ref, first_ref):
        frames = ref.shape[0]
        values = [ref[f].astype(jnp.float32) for f in range(frames)]
        rows += [jnp.sum(v, axis=(0, 1)).reshape(1, -1) for v in values]
        rows += [jnp.sum(v * v, axis=(0, 1)).reshape(1, -1) for v in values]
    spread(out_ref, jnp.concatenate(rows, axis=0))
    for k, line in enumerate(vectors):
        affine_ref[k : k + 1] = line[...].reshape(1, -1)


def moments(second, first, vectors, peers):
    frames, _, _, channels = second.shape
    return pl.pallas_call(
        moments_kernel,
        out_shape=(
            jax.ShapeDtypeStruct((peers, 4 * frames, channels), jnp.float32),
            jax.ShapeDtypeStruct((len(vectors), channels), jnp.float32),
        ),
        in_specs=vmem(2 + len(vectors)),
        out_specs=tuple(vmem(2)),
        compiler_params=pltpu.CompilerParams(vmem_limit_bytes=16 * MIB),
        name="moments",
    )(second, first, *vectors)


def fill(ext, at, block, a, b, even):
    frames, cols = block.shape[:2]
    ext[at : at + frames, 1 : cols + 1] = block
    right, left = swapped(even, a, b)
    ext[at : at + frames, 0] = left
    ext[at : at + frames, cols + 1] = right


def time_taps(ext, w_ref, taps, frames, cols, row_taps=(0, 1, 2)):
    _, channels = ext.shape[2:]
    pairs = [(a, c) for a in taps for c in range(3)]
    left = jnp.concatenate(
        [
            ext[2 - a : 2 - a + frames, 2 - c : 2 - c + cols].reshape(-1, channels)
            for a, c in pairs
        ],
        axis=1,
    )
    right = jnp.concatenate(
        [
            jnp.concatenate([w_ref[9 * a + 3 * b + c] for a, c in pairs], axis=1)
            for b in row_taps
        ],
        axis=0,
    )
    return nt_dot(left, right)


def row_taps(wide, rows):
    count, channels = wide.shape[0], wide.shape[1] // 3
    row = lax.broadcasted_iota(jnp.int32, (count, 1), 0) % rows
    up = jnp.where(row < rows - 1, pltpu.roll(wide[:, :channels], count - 1, 0), 0.0)
    down = jnp.where(row > 0, pltpu.roll(wide[:, 2 * channels :], 1, 0), 0.0)
    return wide[:, channels : 2 * channels] + up + down


def flags(par_ref):
    return [par_ref[k : k + 1] for k in range(3)]


def swapped(even, a, b):
    odd = 1 - even
    return a * even + b * odd, b * even + a * odd


def window(par_ref, own_ref, next_ref, ra_ref, rb_ref, ran_ref, rbn_ref, ext):
    frames = own_ref.shape[0]
    even, side, later = flags(par_ref)
    fill(ext, 0, own_ref[...], ra_ref[...], rb_ref[...] * side, even)
    fill(
        ext,
        frames,
        next_ref[...] * later,
        jnp.zeros_like(rbn_ref) if ran_ref is None else ran_ref[...] * later,
        rbn_ref[...] * (later * side),
        even,
    )


def gather_kernel(par_ref, own_ref, next_ref, ra_ref, rb_ref, rbn_ref, ext_ref, corner_ref):
    even, _, _ = flags(par_ref)
    cols = own_ref.shape[1]
    window(par_ref, own_ref, next_ref, ra_ref, rb_ref, None, rbn_ref, ext_ref)
    corner_ref[...], _ = swapped(even, next_ref[:, cols - 1], next_ref[:, 0])


def gather_section(par, own, nxt, ra, rb, rbn):
    frames, cols, rows, channels = own.shape
    return pl.pallas_call(
        gather_kernel,
        out_shape=(
            jax.ShapeDtypeStruct((2 * frames, cols + 2, rows, channels), own.dtype),
            jax.ShapeDtypeStruct((frames, rows, channels), own.dtype),
        ),
        in_specs=vmem(6),
        out_specs=tuple(vmem(2)),
        compiler_params=pltpu.CompilerParams(vmem_limit_bytes=4 * MIB),
        name="gather",
    )(par, own, nxt, ra, rb, rbn)


def conv_kernel(par_ref, part_ref, ran_ref, w_hbm, u_ref, ext, acc, w_ref, sems):
    frames, rows, channels = ran_ref.shape
    cols = part_ref.shape[1] - 2
    pieces = [(2, (0, 1, 2)), (1, (0, 1, 2)), (0, (0,)), (0, (1,)), (0, (2,))]
    copies = []
    for k, (a, bs) in enumerate(pieces):
        span = pl.ds(9 * a + 3 * bs[0], 3 * len(bs))
        copies.append(pltpu.make_async_copy(w_hbm.at[span], w_ref.at[span], sems.at[k]))
        copies[-1].start()
    even, _, later = flags(par_ref)
    ext[...] = part_ref[...]
    right, left = swapped(even, ran_ref[...] * later, jnp.zeros_like(ran_ref))
    ext[frames:, 0] = part_ref[frames:, 0] + left
    ext[frames:, cols + 1] = part_ref[frames:, cols + 1] + right
    for copy, (a, bs) in zip(copies, pieces):
        copy.wait()
        lanes = slice(bs[0] * channels, (bs[-1] + 1) * channels)
        part = time_taps(ext, w_ref, (a,), frames, cols, bs)
        acc[:, lanes] = part if a == 2 else acc[:, lanes] + part
    u_ref[...] = row_taps(acc, rows)


def conv_section(par, part, ran, kernel):
    frames, rows, channels = ran.shape
    cols = part.shape[1] - 2
    count = frames * cols * rows
    return pl.pallas_call(
        conv_kernel,
        out_shape=jax.ShapeDtypeStruct((count, channels), jnp.float32),
        in_specs=vmem(3) + HBM,
        out_specs=vmem(1)[0],
        scratch_shapes=[
            pltpu.VMEM(part.shape, jnp.bfloat16),
            pltpu.VMEM((count, 3 * channels), jnp.float32),
            pltpu.VMEM(kernel.shape, jnp.bfloat16),
            pltpu.SemaphoreType.DMA((5,)),
        ],
        compiler_params=pltpu.CompilerParams(vmem_limit_bytes=16 * MIB),
        cost_estimate=matmul_cost(count, kernel),
        name="conv",
    )(par, part, ran, in_hbm(kernel))


def norm_stats(cells, frames, mom_ref):
    totals = group_sum(jnp.sum(mom_ref[...], axis=0)) * (1.0 / cells)
    rows = []
    for base in (0, 2 * frames):
        mean = totals[base : base + frames]
        rows += [mean, lax.rsqrt(totals[base + frames : base + 2 * frames] - mean * mean + EPSILON)]
    return jnp.concatenate(rows, axis=0)


def through(upstream, normed, gain, shift):
    pre = normed * gain + shift
    sig = jax.nn.sigmoid(pre)
    return upstream * sig * (1.0 + pre * (1.0 - sig)) * gain


def finish(stats, upstream, x_ref, affine_ref, at, q_ref, sums_ref):
    frames, cols, rows, channels = x_ref.shape
    gain, shift = affine_ref[at : at + 1], affine_ref[at + 1 : at + 2]
    half = cols * rows
    sums, crosses = [], []
    for f in range(frames):
        mean, scale = stats[f : f + 1], stats[frames + f : frames + f + 1]
        normed = (x_ref[f].astype(jnp.float32).reshape(half, channels) - mean) * scale
        q = through(upstream[f * half : (f + 1) * half], normed, gain, shift)
        q_ref[f] = q.reshape(cols, rows, channels)
        sums.append(jnp.sum(q, axis=0, keepdims=True))
        crosses.append(jnp.sum(q * normed, axis=0, keepdims=True))
    spread(sums_ref, jnp.concatenate(sums + crosses, axis=0))


def finish_shapes(stored, peers):
    frames, _, _, channels = stored.shape
    return (
        jax.ShapeDtypeStruct(stored.shape, jnp.float32),
        jax.ShapeDtypeStruct((peers, 2 * frames, channels), jnp.float32),
    )


def norm_kernel(cells, u_ref, x_ref, mom_ref, affine_ref, q_ref, sums_ref, stats_ref):
    frames = x_ref.shape[0]
    stats = norm_stats(cells, frames, mom_ref)
    finish(stats[: 2 * frames], u_ref, x_ref, affine_ref, 0, q_ref, sums_ref)
    stats_ref[...] = stats


def norm_section(upstream, stored, mom, affine, cells, peers):
    frames, _, _, channels = stored.shape
    stats = jax.ShapeDtypeStruct((4 * frames, channels), jnp.float32)
    return pl.pallas_call(
        functools.partial(norm_kernel, cells),
        out_shape=(*finish_shapes(stored, peers), stats),
        in_specs=vmem(4),
        out_specs=tuple(vmem(3)),
        compiler_params=pltpu.CompilerParams(vmem_limit_bytes=4 * MIB),
        name="norm",
    )(upstream, stored, mom, affine)


def block_grad(cells, base, grad_ref, q_ref, x_ref, stats_ref, sums_ref):
    frames, cols, rows, channels = grad_ref.shape
    totals = group_sum(jnp.sum(sums_ref[...], axis=0)) * (1.0 / cells)
    result = []
    for f in range(frames):
        mean = stats_ref[base + f : base + f + 1]
        scale = stats_ref[base + frames + f : base + frames + f + 1]
        flat = (cols * rows, channels)
        normed = (x_ref[f].astype(jnp.float32).reshape(flat) - mean) * scale
        value = grad_ref[f].astype(jnp.float32).reshape(flat) + scale * (
            q_ref[f].reshape(flat)
            - totals[f : f + 1]
            - normed * totals[frames + f : frames + f + 1]
        )
        result.append(value.astype(jnp.bfloat16))
    return result


def dx_kernel(cells, par_ref, grad_ref, q_ref, x_ref, stats_ref, sums_ref, dx_ref, sa_ref, sb_ref):
    _, cols, rows, channels = grad_ref.shape
    even, _, _ = flags(par_ref)
    for f, value in enumerate(block_grad(cells, 0, grad_ref, q_ref, x_ref, stats_ref, sums_ref)):
        value = value.reshape(cols, rows, channels)
        dx_ref[f] = value
        sa_ref[f], sb_ref[f] = swapped(even, value[cols - 1], value[0])


def dx_section(par, grad, q, stored, stats, sums, cells):
    frames, _, rows, channels = grad.shape
    edge = jax.ShapeDtypeStruct((frames, rows, channels), jnp.bfloat16)
    return pl.pallas_call(
        functools.partial(dx_kernel, cells),
        out_shape=(jax.ShapeDtypeStruct(grad.shape, jnp.bfloat16), edge, edge),
        in_specs=vmem(6),
        out_specs=tuple(vmem(3)),
        compiler_params=pltpu.CompilerParams(vmem_limit_bytes=16 * MIB),
        cost_estimate=WEIGHTS_COVER,
        name="dx",
    )(par, grad, q, stored, stats, sums)


def conv_norm_kernel(
    par_ref,
    own_ref,
    next_ref,
    ra_ref,
    rb_ref,
    ran_ref,
    rbn_ref,
    w_ref,
    x_ref,
    stats_ref,
    affine_ref,
    q_ref,
    sums_ref,
    ext,
    acc,
):
    rows = own_ref.shape[2]
    window(par_ref, own_ref, next_ref, ra_ref, rb_ref, ran_ref, rbn_ref, ext)
    acc[...] = time_taps(ext, w_ref, (2, 1, 0), *own_ref.shape[:2])
    upstream = row_taps(acc, rows)
    stats = stats_ref[2 * own_ref.shape[0] :]
    finish(stats, upstream, x_ref, affine_ref, 2, q_ref, sums_ref)


def conv_norm_section(par, grad, halo, kernel, stored, stats, affine, peers):
    frames, cols, rows, channels = grad.shape
    count = frames * cols * rows
    return pl.pallas_call(
        conv_norm_kernel,
        out_shape=finish_shapes(stored, peers),
        in_specs=vmem(11),
        out_specs=tuple(vmem(2)),
        scratch_shapes=[
            pltpu.VMEM((2 * frames, cols + 2, rows, channels), jnp.bfloat16),
            pltpu.VMEM((count, 3 * channels), jnp.float32),
        ],
        compiler_params=pltpu.CompilerParams(vmem_limit_bytes=16 * MIB),
        cost_estimate=matmul_cost(count, kernel),
        name="convnorm",
    )(par, grad, *halo, kernel, stored, stats, affine)


def edge_kernel(par_ref, block_ref, *out_refs):
    cols = block_ref.shape[1]
    even, _, _ = flags(par_ref)
    for ref, value in zip(out_refs, swapped(even, block_ref[:, cols - 1], block_ref[:, 0])):
        ref[...] = value


def edge_section(par, block, count, cost):
    frames, _, rows, channels = block.shape
    edge = jax.ShapeDtypeStruct((frames, rows, channels), block.dtype)
    return pl.pallas_call(
        edge_kernel,
        out_shape=(edge,) * count,
        in_specs=vmem(2),
        out_specs=tuple(vmem(count)),
        compiler_params=pltpu.CompilerParams(vmem_limit_bytes=4 * MIB),
        cost_estimate=cost,
        name="edge",
    )(par, block)


def latent_kernel_body(cells, grad_ref, q_ref, x_ref, stats_ref, sums_ref, k_ref, own_ref, prev_ref, wide):
    frames, cols, rows, channels = grad_ref.shape
    lat = k_ref.shape[1]
    lanes = own_ref.shape[-1]
    values = block_grad(cells, 2 * frames, grad_ref, q_ref, x_ref, stats_ref, sums_ref)
    grad = jnp.concatenate(values, axis=0)
    count = frames * cols * rows
    wide[...] = jnp.zeros_like(wide)
    width = 3 * lat
    spots = (0, width, lanes)
    for b in range(3):
        for a in range(3):
            k = 9 * a + 3 * b
            wide[b, spots[a] : spots[a] + width] = k_ref[k : k + 3].reshape(width, channels)
    row = lax.broadcasted_iota(jnp.int32, (count, 1), 0) % rows
    z = [nt_dot(grad, wide[b]) for b in range(3)]
    up = jnp.where(row < rows - 1, pltpu.roll(z[0], count - 1, 0), 0.0)
    down = jnp.where(row > 0, pltpu.roll(z[2], 1, 0), 0.0)
    total = z[1] + up + down
    lane = lax.broadcasted_iota(jnp.int32, (1, lanes), 1)
    both, third = total[:, :lanes], total[:, lanes:]
    parts = (
        jnp.where(lane < width, both, 0.0),
        jnp.where(lane < width, 0.0, both),
        third,
    )
    placed = {}
    for a in range(3):
        part = parts[a].reshape(frames, cols, rows, lanes)
        base = width if a == 1 else 0
        for f in range(frames):
            out = None
            for w in range(cols):
                shift = (lat * w - base) % lanes
                one = pltpu.roll(part[f, w], shift, 1) if shift else part[f, w]
                out = one if out is None else out + one
            at = f + a - 2
            placed[at] = placed[at] + out if at in placed else out
    for f in range(frames):
        own_ref[f] = placed[f]
        prev_ref[f] = placed[f - 2]


def latent_section(grad, q, stored, stats, sums, kernel, cells):
    frames, _, rows, channels = grad.shape
    lanes = 128
    out = jax.ShapeDtypeStruct((frames, rows, lanes), jnp.float32)
    return pl.pallas_call(
        functools.partial(latent_kernel_body, cells),
        out_shape=(out, out),
        in_specs=vmem(6),
        out_specs=tuple(vmem(2)),
        scratch_shapes=[pltpu.VMEM((3, 2 * lanes, channels), jnp.bfloat16)],
        compiler_params=pltpu.CompilerParams(vmem_limit_bytes=16 * MIB),
        name="latent",
    )(grad, q, stored, stats, sums, kernel)


def assemble_kernel(lat, cols, got_ref, e_ref, perm_ref, out_ref):
    parts = {}
    for p in range(2):
        rows = jnp.concatenate([got_ref[:, p, :], got_ref[:, 2 + p, :]], axis=0)
        spots = lax.dot_general(
            jnp.concatenate(thirds(rows), axis=0),
            e_ref[...],
            (((0,), (0,)), ((), ())),
            preferred_element_type=jnp.float32,
        )
        for col in range(cols + 2):
            q = (col + 1) % 2
            piece = spots[lat * col : lat * (col + 1), 128 * col : 128 * (col + 1)]
            parts[p, q] = parts[p, q] + piece if (p, q) in parts else piece
    stacked = jnp.concatenate([parts[p, q] for p in range(2) for q in range(2)], axis=0)
    final = jnp.dot(
        perm_ref[...],
        jnp.concatenate(thirds(stacked), axis=0),
        preferred_element_type=jnp.float32,
    )
    out_ref[...] = final[:, : out_ref.shape[1]]


def assemble(got, lat, cols):
    peers, quad, _ = got.shape
    width = peers * cols // 2
    tokens = quad // 2 * width
    place = np.zeros((quad // 2, peers, (cols + 2) * 128), np.float32)
    for hh in range(quad // 2):
        for s in range(peers):
            for col in range(cols + 2):
                x = s * cols + col - 1
                if 0 <= x < peers * cols:
                    place[hh, s, 128 * col + hh * width + x // 2] = 1.0
    place = np.tile(place.reshape(-1, place.shape[-1]), (3, 1))
    perm = np.zeros((4 * lat, 4 * lat), np.float32)
    for pq in range(4):
        for one in range(lat):
            perm[one * 4 + pq, pq * lat + one] = 1.0
    perm = np.tile(perm, (1, 3))
    return pl.pallas_call(
        functools.partial(assemble_kernel, lat, cols),
        out_shape=jax.ShapeDtypeStruct((4 * lat, tokens), jnp.float32),
        in_specs=vmem(3),
        out_specs=pl.BlockSpec(memory_space=pltpu.VMEM),
        compiler_params=pltpu.CompilerParams(vmem_limit_bytes=16 * MIB),
        name="assemble",
    )(got, jnp.asarray(place, jnp.bfloat16), jnp.asarray(perm, jnp.bfloat16))


def routes():
    tms, tiles = lax.axis_size("tm"), lax.axis_size(TILE)
    back = ring(tms)
    hops = []
    for k in range(1, tiles, 2):
        hops += [(k, (k + 1) % tiles), ((k + 1) % tiles, k)]
    diagonal = [(t * tiles + s, u * tiles + d) for t, u in back for s, d in hops]
    return back, hops, diagonal


SWAP = [(0, 1), (1, 0)]


def exchange(value, send_a, send_b):
    back, hops, diagonal = routes()
    rb = lax.ppermute(send_b, TILE, hops)
    ra = lax.ppermute(send_a, "tile_2", SWAP)
    nxt = lax.ppermute(value, "tm", back)
    rbn = lax.ppermute(send_b, TM_TILE, diagonal)
    return nxt, ra, rb, rbn


def ring(count):
    return [(t, (t - 1) % count) for t in range(count)]


def everyone(rows):
    return lax.all_to_all(rows, TILE, 0, 0)


def shards(
    first_input,
    second_input,
    output_grad,
    first_gain,
    first_shift,
    first_kernel,
    second_gain,
    second_shift,
    second_kernel,
    latent_kernel,
):
    frames, rows, cols, channels = first_input.shape
    peers = lax.axis_size(TILE)
    cells = rows * cols * peers * (channels // GROUPS)
    core = lax.axis_index("tile_2")
    even = core == 0
    tile, when = lax.axis_index(TILE), lax.axis_index("tm")
    later = when < lax.axis_size("tm") - 1
    side = jnp.where(even, tile > 0, tile < peers - 1)
    ones = jnp.stack([even, side, later]).astype(jnp.bfloat16)
    par = jnp.broadcast_to(ones[:, None], (3, channels))
    par, later, output_grad, second_input, first_input = lax.optimization_barrier(
        (par, later, output_grad, second_input, first_input)
    )
    turn = lambda x: with_layout_constraint(
        jnp.transpose(x, (0, 2, 1, 3)), Layout(major_to_minor=(0, 1, 2, 3))
    )

    grad = turn(output_grad)
    vectors = (second_gain, second_shift, first_gain, first_shift)
    mine, affine = moments(second_input, first_input, vectors, peers)
    mom = everyone(mine)
    nxt, ra, rb, rbn = exchange(grad, *edge_section(par, grad, 2, INPUTS_COVER))
    part, corner = gather_section(par, grad, nxt, ra, rb, rbn)
    ran = lax.ppermute(corner, "tile_2", SWAP)
    second, first = turn(second_input), turn(first_input)
    upstream = conv_section(par, part, ran, second_kernel)
    q, sums, stats = norm_section(upstream, second, mom, affine, cells, peers)
    grad, send_a, send_b = dx_section(par, grad, q, second, stats, everyone(sums), cells)
    nxt, ra, rb, rbn = exchange(grad, send_a, send_b)
    (corner,) = edge_section(par, nxt, 1, None)
    ran = lax.ppermute(corner, "tile_2", SWAP)
    q, sums = conv_norm_section(
        par, grad, (nxt, ra, rb, ran, rbn), first_kernel, first, stats, affine, peers
    )
    own, prev = latent_section(grad, q, first, stats, everyone(sums), latent_kernel, cells)
    tms = lax.axis_size("tm")
    own = own + jnp.where(later, lax.ppermute(prev, "tm", ring(tms)), 0.0)
    got = everyone(own.reshape(peers, frames * rows // peers, own.shape[-1]))
    return assemble(got, latent_kernel.shape[1], cols)


def solution(mesh):
    torus = Mesh(
        mesh.devices.reshape(mesh.shape["tm"], 4, 2, 2), ("tm", "tile_0", "tile_1", "tile_2")
    )
    block = P("tm", None, TILE, None)
    placed = (block, block, block) + (P(),) * 7
    return jax.shard_map(
        shards, mesh=torus, in_specs=placed, out_specs=P(None, TM_TILE), check_vma=False
    )
```

```python
import functools

import jax
import jax.numpy as jnp
import numpy as np
from jax import lax
from jax.experimental import pallas as pl
from jax.experimental.pallas import tpu as pltpu
from jax.experimental.layout import Layout, with_layout_constraint
from jax.sharding import Mesh
from jax.sharding import PartitionSpec as P

GROUPS = 32
TILE = ("tile_0", "tile_1", "tile_2")
TM_TILE = ("tm",) + TILE
EPSILON = 1e-05
MIB = 1 << 20


def vmem(count):
    return [pl.BlockSpec(memory_space=pltpu.VMEM)] * count


WEIGHTS_COVER = pl.CostEstimate(flops=1 << 33, bytes_accessed=1 << 23, transcendentals=0)
INPUTS_COVER = pl.CostEstimate(flops=1 << 31, bytes_accessed=1 << 20, transcendentals=0)
HBM = [pl.BlockSpec(memory_space=pltpu.HBM)]


def matmul_cost(count, kernel):
    return pl.CostEstimate(
        flops=2 * count * kernel.size, bytes_accessed=2 * kernel.size, transcendentals=0
    )


def in_hbm(value):
    return pltpu.with_memory_space_constraint(value, pltpu.HBM)


def nt_dot(left, right, **kw):
    return lax.dot_general(
        left, right, (((1,), (1,)), ((), ())), preferred_element_type=jnp.float32, **kw
    )


def thirds(value):
    high = value.astype(jnp.bfloat16)
    rest = value - high.astype(jnp.float32)
    middle = rest.astype(jnp.bfloat16)
    return high, middle, (rest - middle.astype(jnp.float32)).astype(jnp.bfloat16)


def group_sum(rows):
    count, channels = rows.shape
    per = channels // GROUPS
    row = lax.broadcasted_iota(jnp.int32, (channels, channels), 0) // per
    col = lax.broadcasted_iota(jnp.int32, (channels, channels), 1) // per
    same = jnp.where(row == col, 1.0, 0.0).astype(jnp.bfloat16)
    if count < 8:
        rows = jnp.concatenate([rows, jnp.zeros((8 - count, channels), jnp.float32)], axis=0)
    split = jnp.concatenate([part.astype(jnp.float32) for part in thirds(rows)], axis=0)
    sums = jnp.dot(split.astype(jnp.bfloat16), same, preferred_element_type=jnp.float32)
    return sums[0:count] + sums[8 : 8 + count] + sums[16 : 16 + count]


def spread(ref, rows):
    ref[...] = jnp.broadcast_to(rows[None], ref.shape)


def moments_kernel(second_ref, first_ref, *refs):
    *vectors, out_ref, affine_ref = refs
    rows = []
    for ref in (second_ref, first_ref):
        frames = ref.shape[0]
        values = [ref[f].astype(jnp.float32) for f in range(frames)]
        rows += [jnp.sum(v, axis=(0, 1)).reshape(1, -1) for v in values]
        rows += [jnp.sum(v * v, axis=(0, 1)).reshape(1, -1) for v in values]
    spread(out_ref, jnp.concatenate(rows, axis=0))
    for k, line in enumerate(vectors):
        affine_ref[k : k + 1] = line[...].reshape(1, -1)


def moments(second, first, vectors, peers):
    frames, _, _, channels = second.shape
    return pl.pallas_call(
        moments_kernel,
        out_shape=(
            jax.ShapeDtypeStruct((peers, 4 * frames, channels), jnp.float32),
            jax.ShapeDtypeStruct((len(vectors), channels), jnp.float32),
        ),
        in_specs=vmem(2 + len(vectors)),
        out_specs=tuple(vmem(2)),
        compiler_params=pltpu.CompilerParams(vmem_limit_bytes=16 * MIB),
        name="moments",
    )(second, first, *vectors)


def fill(ext, at, block, a, b, even):
    frames, cols = block.shape[:2]
    ext[at : at + frames, 1 : cols + 1] = block
    right, left = swapped(even, a, b)
    ext[at : at + frames, 0] = left
    ext[at : at + frames, cols + 1] = right


def time_taps(ext, w_ref, taps, frames, cols):
    _, channels = ext.shape[2:]
    pairs = [(a, c) for a in taps for c in range(3)]
    left = jnp.concatenate(
        [
            ext[2 - a : 2 - a + frames, 2 - c : 2 - c + cols].reshape(-1, channels)
            for a, c in pairs
        ],
        axis=1,
    )
    right = jnp.concatenate(
        [
            jnp.concatenate([w_ref[9 * a + 3 * b + c] for a, c in pairs], axis=1)
            for b in range(3)
        ],
        axis=0,
    )
    return nt_dot(left, right)


def row_taps(wide, rows):
    count, channels = wide.shape[0], wide.shape[1] // 3
    row = lax.broadcasted_iota(jnp.int32, (count, 1), 0) % rows
    up = jnp.where(row < rows - 1, pltpu.roll(wide[:, :channels], count - 1, 0), 0.0)
    down = jnp.where(row > 0, pltpu.roll(wide[:, 2 * channels :], 1, 0), 0.0)
    return wide[:, channels : 2 * channels] + up + down


def flags(par_ref):
    return [par_ref[k : k + 1] for k in range(3)]


def swapped(even, a, b):
    odd = 1 - even
    return a * even + b * odd, b * even + a * odd


def window(par_ref, own_ref, next_ref, ra_ref, rb_ref, ran_ref, rbn_ref, ext):
    frames = own_ref.shape[0]
    even, side, later = flags(par_ref)
    fill(ext, 0, own_ref[...], ra_ref[...], rb_ref[...] * side, even)
    fill(
        ext,
        frames,
        next_ref[...] * later,
        jnp.zeros_like(rbn_ref) if ran_ref is None else ran_ref[...] * later,
        rbn_ref[...] * (later * side),
        even,
    )


def gather_kernel(par_ref, own_ref, next_ref, ra_ref, rb_ref, rbn_ref, ext_ref, corner_ref):
    even, _, _ = flags(par_ref)
    cols = own_ref.shape[1]
    window(par_ref, own_ref, next_ref, ra_ref, rb_ref, None, rbn_ref, ext_ref)
    corner_ref[...], _ = swapped(even, next_ref[:, cols - 1], next_ref[:, 0])


def gather_section(par, own, nxt, ra, rb, rbn):
    frames, cols, rows, channels = own.shape
    return pl.pallas_call(
        gather_kernel,
        out_shape=(
            jax.ShapeDtypeStruct((2 * frames, cols + 2, rows, channels), own.dtype),
            jax.ShapeDtypeStruct((frames, rows, channels), own.dtype),
        ),
        in_specs=vmem(6),
        out_specs=tuple(vmem(2)),
        compiler_params=pltpu.CompilerParams(vmem_limit_bytes=4 * MIB),
        name="gather",
    )(par, own, nxt, ra, rb, rbn)


def conv_kernel(par_ref, part_ref, ran_ref, w_hbm, u_ref, ext, acc, w_ref, sems):
    frames, rows, _ = ran_ref.shape
    cols = part_ref.shape[1] - 2
    copies = {}
    for a in (2, 1, 0):
        span = pl.ds(9 * a, 9)
        copies[a] = pltpu.make_async_copy(w_hbm.at[span], w_ref.at[span], sems.at[a])
        copies[a].start()
    even, _, later = flags(par_ref)
    ext[...] = part_ref[...]
    right, left = swapped(even, ran_ref[...] * later, jnp.zeros_like(ran_ref))
    ext[frames:, 0] = part_ref[frames:, 0] + left
    ext[frames:, cols + 1] = part_ref[frames:, cols + 1] + right
    for a, copy in copies.items():
        copy.wait()
        part = time_taps(ext, w_ref, (a,), frames, cols)
        acc[...] = part if a == 2 else acc[...] + part
    u_ref[...] = row_taps(acc, rows)


def conv_section(par, part, ran, kernel):
    frames, rows, channels = ran.shape
    cols = part.shape[1] - 2
    count = frames * cols * rows
    return pl.pallas_call(
        conv_kernel,
        out_shape=jax.ShapeDtypeStruct((count, channels), jnp.float32),
        in_specs=vmem(3) + HBM,
        out_specs=vmem(1)[0],
        scratch_shapes=[
            pltpu.VMEM(part.shape, jnp.bfloat16),
            pltpu.VMEM((count, 3 * channels), jnp.float32),
            pltpu.VMEM(kernel.shape, jnp.bfloat16),
            pltpu.SemaphoreType.DMA((3,)),
        ],
        compiler_params=pltpu.CompilerParams(vmem_limit_bytes=16 * MIB),
        cost_estimate=matmul_cost(count, kernel),
        name="conv",
    )(par, part, ran, in_hbm(kernel))


def norm_stats(cells, frames, mom_ref):
    totals = group_sum(jnp.sum(mom_ref[...], axis=0)) * (1.0 / cells)
    rows = []
    for base in (0, 2 * frames):
        mean = totals[base : base + frames]
        rows += [mean, lax.rsqrt(totals[base + frames : base + 2 * frames] - mean * mean + EPSILON)]
    return jnp.concatenate(rows, axis=0)


def through(upstream, normed, gain, shift):
    pre = normed * gain + shift
    sig = jax.nn.sigmoid(pre)
    return upstream * sig * (1.0 + pre * (1.0 - sig)) * gain


def finish(stats, upstream, x_ref, affine_ref, at, q_ref, sums_ref):
    frames, cols, rows, channels = x_ref.shape
    gain, shift = affine_ref[at : at + 1], affine_ref[at + 1 : at + 2]
    half = cols * rows
    sums, crosses = [], []
    for f in range(frames):
        mean, scale = stats[f : f + 1], stats[frames + f : frames + f + 1]
        normed = (x_ref[f].astype(jnp.float32).reshape(half, channels) - mean) * scale
        q = through(upstream[f * half : (f + 1) * half], normed, gain, shift)
        q_ref[f] = q.reshape(cols, rows, channels)
        sums.append(jnp.sum(q, axis=0, keepdims=True))
        crosses.append(jnp.sum(q * normed, axis=0, keepdims=True))
    spread(sums_ref, jnp.concatenate(sums + crosses, axis=0))


def finish_shapes(stored, peers):
    frames, _, _, channels = stored.shape
    return (
        jax.ShapeDtypeStruct(stored.shape, jnp.float32),
        jax.ShapeDtypeStruct((peers, 2 * frames, channels), jnp.float32),
    )


def norm_kernel(cells, u_ref, x_ref, mom_ref, affine_ref, q_ref, sums_ref, stats_ref):
    frames = x_ref.shape[0]
    stats = norm_stats(cells, frames, mom_ref)
    finish(stats[: 2 * frames], u_ref, x_ref, affine_ref, 0, q_ref, sums_ref)
    stats_ref[...] = stats


def norm_section(upstream, stored, mom, affine, cells, peers):
    frames, _, _, channels = stored.shape
    stats = jax.ShapeDtypeStruct((4 * frames, channels), jnp.float32)
    return pl.pallas_call(
        functools.partial(norm_kernel, cells),
        out_shape=(*finish_shapes(stored, peers), stats),
        in_specs=vmem(4),
        out_specs=tuple(vmem(3)),
        compiler_params=pltpu.CompilerParams(vmem_limit_bytes=4 * MIB),
        name="norm",
    )(upstream, stored, mom, affine)


def block_grad(cells, base, grad_ref, q_ref, x_ref, stats_ref, sums_ref):
    frames, cols, rows, channels = grad_ref.shape
    totals = group_sum(jnp.sum(sums_ref[...], axis=0)) * (1.0 / cells)
    result = []
    for f in range(frames):
        mean = stats_ref[base + f : base + f + 1]
        scale = stats_ref[base + frames + f : base + frames + f + 1]
        flat = (cols * rows, channels)
        normed = (x_ref[f].astype(jnp.float32).reshape(flat) - mean) * scale
        value = grad_ref[f].astype(jnp.float32).reshape(flat) + scale * (
            q_ref[f].reshape(flat)
            - totals[f : f + 1]
            - normed * totals[frames + f : frames + f + 1]
        )
        result.append(value.astype(jnp.bfloat16))
    return result


def dx_kernel(cells, par_ref, grad_ref, q_ref, x_ref, stats_ref, sums_ref, dx_ref, sa_ref, sb_ref):
    _, cols, rows, channels = grad_ref.shape
    even, _, _ = flags(par_ref)
    for f, value in enumerate(block_grad(cells, 0, grad_ref, q_ref, x_ref, stats_ref, sums_ref)):
        value = value.reshape(cols, rows, channels)
        dx_ref[f] = value
        sa_ref[f], sb_ref[f] = swapped(even, value[cols - 1], value[0])


def dx_section(par, grad, q, stored, stats, sums, cells):
    frames, _, rows, channels = grad.shape
    edge = jax.ShapeDtypeStruct((frames, rows, channels), jnp.bfloat16)
    return pl.pallas_call(
        functools.partial(dx_kernel, cells),
        out_shape=(jax.ShapeDtypeStruct(grad.shape, jnp.bfloat16), edge, edge),
        in_specs=vmem(6),
        out_specs=tuple(vmem(3)),
        compiler_params=pltpu.CompilerParams(vmem_limit_bytes=16 * MIB),
        cost_estimate=WEIGHTS_COVER,
        name="dx",
    )(par, grad, q, stored, stats, sums)


def conv_norm_kernel(
    par_ref,
    own_ref,
    next_ref,
    ra_ref,
    rb_ref,
    ran_ref,
    rbn_ref,
    w_ref,
    x_ref,
    stats_ref,
    affine_ref,
    q_ref,
    sums_ref,
    ext,
    acc,
):
    rows = own_ref.shape[2]
    window(par_ref, own_ref, next_ref, ra_ref, rb_ref, ran_ref, rbn_ref, ext)
    acc[...] = time_taps(ext, w_ref, (2, 1, 0), *own_ref.shape[:2])
    upstream = row_taps(acc, rows)
    stats = stats_ref[2 * own_ref.shape[0] :]
    finish(stats, upstream, x_ref, affine_ref, 2, q_ref, sums_ref)


def conv_norm_section(par, grad, halo, kernel, stored, stats, affine, peers):
    frames, cols, rows, channels = grad.shape
    count = frames * cols * rows
    return pl.pallas_call(
        conv_norm_kernel,
        out_shape=finish_shapes(stored, peers),
        in_specs=vmem(11),
        out_specs=tuple(vmem(2)),
        scratch_shapes=[
            pltpu.VMEM((2 * frames, cols + 2, rows, channels), jnp.bfloat16),
            pltpu.VMEM((count, 3 * channels), jnp.float32),
        ],
        compiler_params=pltpu.CompilerParams(vmem_limit_bytes=16 * MIB),
        cost_estimate=matmul_cost(count, kernel),
        name="convnorm",
    )(par, grad, *halo, kernel, stored, stats, affine)


def edge_kernel(par_ref, block_ref, *out_refs):
    cols = block_ref.shape[1]
    even, _, _ = flags(par_ref)
    for ref, value in zip(out_refs, swapped(even, block_ref[:, cols - 1], block_ref[:, 0])):
        ref[...] = value


def edge_section(par, block, count, cost):
    frames, _, rows, channels = block.shape
    edge = jax.ShapeDtypeStruct((frames, rows, channels), block.dtype)
    return pl.pallas_call(
        edge_kernel,
        out_shape=(edge,) * count,
        in_specs=vmem(2),
        out_specs=tuple(vmem(count)),
        compiler_params=pltpu.CompilerParams(vmem_limit_bytes=4 * MIB),
        cost_estimate=cost,
        name="edge",
    )(par, block)


def latent_kernel_body(cells, grad_ref, q_ref, x_ref, stats_ref, sums_ref, k_ref, own_ref, prev_ref, wide):
    frames, cols, rows, channels = grad_ref.shape
    lat = k_ref.shape[1]
    lanes = own_ref.shape[-1]
    values = block_grad(cells, 2 * frames, grad_ref, q_ref, x_ref, stats_ref, sums_ref)
    grad = jnp.concatenate(values, axis=0)
    count = frames * cols * rows
    wide[...] = jnp.zeros_like(wide)
    width = 3 * lat
    spots = (0, width, lanes)
    for b in range(3):
        for a in range(3):
            k = 9 * a + 3 * b
            wide[b, spots[a] : spots[a] + width] = k_ref[k : k + 3].reshape(width, channels)
    row = lax.broadcasted_iota(jnp.int32, (count, 1), 0) % rows
    z = [nt_dot(grad, wide[b]) for b in range(3)]
    up = jnp.where(row < rows - 1, pltpu.roll(z[0], count - 1, 0), 0.0)
    down = jnp.where(row > 0, pltpu.roll(z[2], 1, 0), 0.0)
    total = z[1] + up + down
    lane = lax.broadcasted_iota(jnp.int32, (1, lanes), 1)
    both, third = total[:, :lanes], total[:, lanes:]
    parts = (
        jnp.where(lane < width, both, 0.0),
        jnp.where(lane < width, 0.0, both),
        third,
    )
    placed = {}
    for a in range(3):
        part = parts[a].reshape(frames, cols, rows, lanes)
        base = width if a == 1 else 0
        for f in range(frames):
            out = None
            for w in range(cols):
                shift = (lat * w - base) % lanes
                one = pltpu.roll(part[f, w], shift, 1) if shift else part[f, w]
                out = one if out is None else out + one
            at = f + a - 2
            placed[at] = placed[at] + out if at in placed else out
    for f in range(frames):
        own_ref[f] = placed[f]
        prev_ref[f] = placed[f - 2]


def latent_section(grad, q, stored, stats, sums, kernel, cells):
    frames, _, rows, channels = grad.shape
    lanes = 128
    out = jax.ShapeDtypeStruct((frames, rows, lanes), jnp.float32)
    return pl.pallas_call(
        functools.partial(latent_kernel_body, cells),
        out_shape=(out, out),
        in_specs=vmem(6),
        out_specs=tuple(vmem(2)),
        scratch_shapes=[pltpu.VMEM((3, 2 * lanes, channels), jnp.bfloat16)],
        compiler_params=pltpu.CompilerParams(vmem_limit_bytes=16 * MIB),
        name="latent",
    )(grad, q, stored, stats, sums, kernel)


def assemble_kernel(lat, cols, got_ref, e_ref, perm_ref, out_ref):
    parts = {}
    for p in range(2):
        rows = jnp.concatenate([got_ref[:, p, :], got_ref[:, 2 + p, :]], axis=0)
        spots = lax.dot_general(
            jnp.concatenate(thirds(rows), axis=0),
            e_ref[...],
            (((0,), (0,)), ((), ())),
            preferred_element_type=jnp.float32,
        )
        for col in range(cols + 2):
            q = (col + 1) % 2
            piece = spots[lat * col : lat * (col + 1), 128 * col : 128 * (col + 1)]
            parts[p, q] = parts[p, q] + piece if (p, q) in parts else piece
    stacked = jnp.concatenate([parts[p, q] for p in range(2) for q in range(2)], axis=0)
    final = jnp.dot(
        perm_ref[...],
        jnp.concatenate(thirds(stacked), axis=0),
        preferred_element_type=jnp.float32,
    )
    out_ref[...] = final[:, : out_ref.shape[1]]


def assemble(got, lat, cols):
    peers, quad, _ = got.shape
    width = peers * cols // 2
    tokens = quad // 2 * width
    place = np.zeros((quad // 2, peers, (cols + 2) * 128), np.float32)
    for hh in range(quad // 2):
        for s in range(peers):
            for col in range(cols + 2):
                x = s * cols + col - 1
                if 0 <= x < peers * cols:
                    place[hh, s, 128 * col + hh * width + x // 2] = 1.0
    place = np.tile(place.reshape(-1, place.shape[-1]), (3, 1))
    perm = np.zeros((4 * lat, 4 * lat), np.float32)
    for pq in range(4):
        for one in range(lat):
            perm[one * 4 + pq, pq * lat + one] = 1.0
    perm = np.tile(perm, (1, 3))
    return pl.pallas_call(
        functools.partial(assemble_kernel, lat, cols),
        out_shape=jax.ShapeDtypeStruct((4 * lat, tokens), jnp.float32),
        in_specs=vmem(3),
        out_specs=pl.BlockSpec(memory_space=pltpu.VMEM),
        compiler_params=pltpu.CompilerParams(vmem_limit_bytes=16 * MIB),
        name="assemble",
    )(got, jnp.asarray(place, jnp.bfloat16), jnp.asarray(perm, jnp.bfloat16))


def routes():
    tms, tiles = lax.axis_size("tm"), lax.axis_size(TILE)
    back = ring(tms)
    hops = []
    for k in range(1, tiles, 2):
        hops += [(k, (k + 1) % tiles), ((k + 1) % tiles, k)]
    diagonal = [(t * tiles + s, u * tiles + d) for t, u in back for s, d in hops]
    return back, hops, diagonal


SWAP = [(0, 1), (1, 0)]


def frames_on(value):
    return lax.ppermute(value, "tm", routes()[0])


def columns_on(send_a, send_b):
    _, hops, diagonal = routes()
    rb = lax.ppermute(send_b, TILE, hops)
    rbn = lax.ppermute(send_b, TM_TILE, diagonal)
    ra = lax.ppermute(send_a, "tile_2", SWAP)
    return ra, rb, rbn


def ring(count):
    return [(t, (t - 1) % count) for t in range(count)]


def everyone(rows):
    return lax.all_to_all(rows, TILE, 0, 0)


def shards(
    first_input,
    second_input,
    output_grad,
    first_gain,
    first_shift,
    first_kernel,
    second_gain,
    second_shift,
    second_kernel,
    latent_kernel,
):
    frames, rows, cols, channels = first_input.shape
    peers = lax.axis_size(TILE)
    cells = rows * cols * peers * (channels // GROUPS)
    core = lax.axis_index("tile_2")
    even = core == 0
    tile, when = lax.axis_index(TILE), lax.axis_index("tm")
    later = when < lax.axis_size("tm") - 1
    side = jnp.where(even, tile > 0, tile < peers - 1)
    ones = jnp.stack([even, side, later]).astype(jnp.bfloat16)
    par = jnp.broadcast_to(ones[:, None], (3, channels))
    par, later, output_grad, second_input, first_input = lax.optimization_barrier(
        (par, later, output_grad, second_input, first_input)
    )
    turn = lambda x: with_layout_constraint(
        jnp.transpose(x, (0, 2, 1, 3)), Layout(major_to_minor=(0, 1, 2, 3))
    )

    grad = turn(output_grad)
    vectors = (second_gain, second_shift, first_gain, first_shift)
    mine, affine = moments(second_input, first_input, vectors, peers)
    mom = everyone(mine)
    nxt = turn(frames_on(output_grad))
    ra, rb, rbn = columns_on(*edge_section(par, grad, 2, INPUTS_COVER))
    part, corner = gather_section(par, grad, nxt, ra, rb, rbn)
    ran = lax.ppermute(corner, "tile_2", SWAP)
    second, first = turn(second_input), turn(first_input)
    upstream = conv_section(par, part, ran, second_kernel)
    q, sums, stats = norm_section(upstream, second, mom, affine, cells, peers)
    grad, send_a, send_b = dx_section(par, grad, q, second, stats, everyone(sums), cells)
    nxt = frames_on(grad)
    ra, rb, rbn = columns_on(send_a, send_b)
    (corner,) = edge_section(par, nxt, 1, None)
    ran = lax.ppermute(corner, "tile_2", SWAP)
    q, sums = conv_norm_section(
        par, grad, (nxt, ra, rb, ran, rbn), first_kernel, first, stats, affine, peers
    )
    own, prev = latent_section(grad, q, first, stats, everyone(sums), latent_kernel, cells)
    tms = lax.axis_size("tm")
    own = own + jnp.where(later, lax.ppermute(prev, "tm", ring(tms)), 0.0)
    got = everyone(own.reshape(peers, frames * rows // peers, own.shape[-1]))
    return assemble(got, latent_kernel.shape[1], cols)


def solution(mesh):
    torus = Mesh(
        mesh.devices.reshape(mesh.shape["tm"], 4, 2, 2), ("tm", "tile_0", "tile_1", "tile_2")
    )
    block = P("tm", None, TILE, None)
    placed = (block, block, block) + (P(),) * 7
    return jax.shard_map(
        shards, mesh=torus, in_specs=placed, out_specs=P(None, TM_TILE), check_vma=False
    )
```

```python
import functools

import jax
import jax.numpy as jnp
import numpy as np
from jax import lax
from jax.experimental import pallas as pl
from jax.experimental.pallas import tpu as pltpu
from jax.experimental.layout import Layout, with_layout_constraint
from jax.sharding import Mesh
from jax.sharding import PartitionSpec as P

GROUPS = 32
TILE = ("tile_0", "tile_1", "tile_2")
TM_TILE = ("tm",) + TILE
EPSILON = 1e-05
MIB = 1 << 20


def vmem(count):
    return [pl.BlockSpec(memory_space=pltpu.VMEM)] * count


WEIGHTS_COVER = pl.CostEstimate(flops=1 << 33, bytes_accessed=1 << 23, transcendentals=0)
WEIGHTS_WINDOW = pl.CostEstimate(
    flops=1 << 33, bytes_accessed=1 << 23, transcendentals=262000000
)
INPUTS_COVER = pl.CostEstimate(flops=1 << 31, bytes_accessed=1 << 20, transcendentals=0)
HBM = [pl.BlockSpec(memory_space=pltpu.HBM)]


def matmul_cost(count, kernel):
    return pl.CostEstimate(
        flops=2 * count * kernel.size, bytes_accessed=2 * kernel.size, transcendentals=0
    )


def nt_dot(left, right, **kw):
    return lax.dot_general(
        left, right, (((1,), (1,)), ((), ())), preferred_element_type=jnp.float32, **kw
    )


def thirds(value):
    high = value.astype(jnp.bfloat16)
    rest = value - high.astype(jnp.float32)
    middle = rest.astype(jnp.bfloat16)
    return high, middle, (rest - middle.astype(jnp.float32)).astype(jnp.bfloat16)


def group_sum(rows):
    count, channels = rows.shape
    per = channels // GROUPS
    row = lax.broadcasted_iota(jnp.int32, (channels, channels), 0) // per
    col = lax.broadcasted_iota(jnp.int32, (channels, channels), 1) // per
    same = jnp.where(row == col, 1.0, 0.0).astype(jnp.bfloat16)
    if count < 8:
        rows = jnp.concatenate([rows, jnp.zeros((8 - count, channels), jnp.float32)], axis=0)
    split = jnp.concatenate([part.astype(jnp.float32) for part in thirds(rows)], axis=0)
    sums = jnp.dot(split.astype(jnp.bfloat16), same, preferred_element_type=jnp.float32)
    return sums[0:count] + sums[8 : 8 + count] + sums[16 : 16 + count]


def spread(ref, rows):
    ref[...] = jnp.broadcast_to(rows[None], ref.shape)


def moments_kernel(second_ref, first_ref, *refs):
    *vectors, out_ref, affine_ref = refs
    rows = []
    for ref in (second_ref, first_ref):
        frames = ref.shape[0]
        values = [ref[f].astype(jnp.float32) for f in range(frames)]
        rows += [jnp.sum(v, axis=(0, 1)).reshape(1, -1) for v in values]
        rows += [jnp.sum(v * v, axis=(0, 1)).reshape(1, -1) for v in values]
    spread(out_ref, jnp.concatenate(rows, axis=0))
    for k, line in enumerate(vectors):
        affine_ref[k : k + 1] = line[...].reshape(1, -1)


def moments(second, first, vectors, peers):
    frames, _, _, channels = second.shape
    return pl.pallas_call(
        moments_kernel,
        out_shape=(
            jax.ShapeDtypeStruct((peers, 4 * frames, channels), jnp.float32),
            jax.ShapeDtypeStruct((len(vectors), channels), jnp.float32),
        ),
        in_specs=vmem(2 + len(vectors)),
        out_specs=tuple(vmem(2)),
        compiler_params=pltpu.CompilerParams(vmem_limit_bytes=16 * MIB),
        name="moments",
    )(second, first, *vectors)


def fill(ext, at, block, a, b, even):
    frames, cols = block.shape[:2]
    ext[at : at + frames, 1 : cols + 1] = block
    right, left = swapped(even, a, b)
    ext[at : at + frames, 0] = left
    ext[at : at + frames, cols + 1] = right


def time_taps(ext, w_ref, taps, frames, cols):
    _, channels = ext.shape[2:]
    pairs = [(a, c) for a in taps for c in range(3)]
    left = jnp.concatenate(
        [
            ext[2 - a : 2 - a + frames, 2 - c : 2 - c + cols].reshape(-1, channels)
            for a, c in pairs
        ],
        axis=1,
    )
    right = jnp.concatenate(
        [
            jnp.concatenate([w_ref[9 * a + 3 * b + c] for a, c in pairs], axis=1)
            for b in range(3)
        ],
        axis=0,
    )
    return nt_dot(left, right)


def row_taps(wide, rows):
    count, channels = wide.shape[0], wide.shape[1] // 3
    row = lax.broadcasted_iota(jnp.int32, (count, 1), 0) % rows
    up = jnp.where(row < rows - 1, pltpu.roll(wide[:, :channels], count - 1, 0), 0.0)
    down = jnp.where(row > 0, pltpu.roll(wide[:, 2 * channels :], 1, 0), 0.0)
    return wide[:, channels : 2 * channels] + up + down


def flags(par_ref):
    return [par_ref[k : k + 1] for k in range(3)]


def swapped(even, a, b):
    odd = 1 - even
    return a * even + b * odd, b * even + a * odd


def window(par_ref, own_ref, next_ref, ra_ref, rb_ref, ran_ref, rbn_ref, ext):
    frames = own_ref.shape[0]
    even, side, later = flags(par_ref)
    fill(ext, 0, own_ref[...], ra_ref[...], rb_ref[...] * side, even)
    fill(
        ext,
        frames,
        next_ref[...] * later,
        jnp.zeros_like(rbn_ref) if ran_ref is None else ran_ref[...] * later,
        rbn_ref[...] * (later * side),
        even,
    )


def gather_kernel(par_ref, own_ref, next_ref, ra_ref, rb_ref, rbn_ref, ext_ref, corner_ref):
    even, _, _ = flags(par_ref)
    cols = own_ref.shape[1]
    window(par_ref, own_ref, next_ref, ra_ref, rb_ref, None, rbn_ref, ext_ref)
    corner_ref[...], _ = swapped(even, next_ref[:, cols - 1], next_ref[:, 0])


def gather_section(par, own, nxt, ra, rb, rbn):
    frames, cols, rows, channels = own.shape
    return pl.pallas_call(
        gather_kernel,
        out_shape=(
            jax.ShapeDtypeStruct((2 * frames, cols + 2, rows, channels), own.dtype),
            jax.ShapeDtypeStruct((frames, rows, channels), own.dtype),
        ),
        in_specs=vmem(6),
        out_specs=tuple(vmem(2)),
        compiler_params=pltpu.CompilerParams(vmem_limit_bytes=4 * MIB),
        cost_estimate=WEIGHTS_WINDOW,
        name="gather",
    )(par, own, nxt, ra, rb, rbn)


def conv_kernel(par_ref, part_ref, ran_ref, w_ref, u_ref, ext, acc):
    frames, rows = ran_ref.shape[:2]
    cols = part_ref.shape[1] - 2
    even, _, later = flags(par_ref)
    ext[...] = part_ref[...]
    right, left = swapped(even, ran_ref[...] * later, jnp.zeros_like(ran_ref))
    ext[frames:, 0] = part_ref[frames:, 0] + left
    ext[frames:, cols + 1] = part_ref[frames:, cols + 1] + right
    acc[...] = time_taps(ext, w_ref, (2, 1, 0), frames, cols)
    u_ref[...] = row_taps(acc, rows)


def conv_section(par, part, ran, kernel):
    frames, rows, channels = ran.shape
    cols = part.shape[1] - 2
    count = frames * cols * rows
    return pl.pallas_call(
        conv_kernel,
        out_shape=jax.ShapeDtypeStruct((count, channels), jnp.float32),
        in_specs=vmem(4),
        out_specs=vmem(1)[0],
        scratch_shapes=[
            pltpu.VMEM(part.shape, jnp.bfloat16),
            pltpu.VMEM((count, 3 * channels), jnp.float32),
        ],
        compiler_params=pltpu.CompilerParams(vmem_limit_bytes=16 * MIB),
        cost_estimate=matmul_cost(count, kernel),
        name="conv",
    )(par, part, ran, kernel)


def norm_stats(cells, frames, mom_ref):
    totals = group_sum(jnp.sum(mom_ref[...], axis=0)) * (1.0 / cells)
    rows = []
    for base in (0, 2 * frames):
        mean = totals[base : base + frames]
        rows += [mean, lax.rsqrt(totals[base + frames : base + 2 * frames] - mean * mean + EPSILON)]
    return jnp.concatenate(rows, axis=0)


def through(upstream, normed, gain, shift):
    pre = normed * gain + shift
    sig = jax.nn.sigmoid(pre)
    return upstream * sig * (1.0 + pre * (1.0 - sig)) * gain


def finish(stats, upstream, x_ref, affine_ref, at, q_ref, sums_ref):
    frames, cols, rows, channels = x_ref.shape
    gain, shift = affine_ref[at : at + 1], affine_ref[at + 1 : at + 2]
    half = cols * rows
    sums, crosses = [], []
    for f in range(frames):
        mean, scale = stats[f : f + 1], stats[frames + f : frames + f + 1]
        normed = (x_ref[f].astype(jnp.float32).reshape(half, channels) - mean) * scale
        q = through(upstream[f * half : (f + 1) * half], normed, gain, shift)
        q_ref[f] = q.reshape(cols, rows, channels)
        sums.append(jnp.sum(q, axis=0, keepdims=True))
        crosses.append(jnp.sum(q * normed, axis=0, keepdims=True))
    spread(sums_ref, jnp.concatenate(sums + crosses, axis=0))


def finish_shapes(stored, peers):
    frames, _, _, channels = stored.shape
    return (
        jax.ShapeDtypeStruct(stored.shape, jnp.float32),
        jax.ShapeDtypeStruct((peers, 2 * frames, channels), jnp.float32),
    )


def norm_kernel(cells, u_ref, x_ref, mom_ref, affine_ref, q_ref, sums_ref, stats_ref):
    frames = x_ref.shape[0]
    stats = norm_stats(cells, frames, mom_ref)
    finish(stats[: 2 * frames], u_ref, x_ref, affine_ref, 0, q_ref, sums_ref)
    stats_ref[...] = stats


def norm_section(upstream, stored, mom, affine, cells, peers):
    frames, _, _, channels = stored.shape
    stats = jax.ShapeDtypeStruct((4 * frames, channels), jnp.float32)
    return pl.pallas_call(
        functools.partial(norm_kernel, cells),
        out_shape=(*finish_shapes(stored, peers), stats),
        in_specs=vmem(4),
        out_specs=tuple(vmem(3)),
        compiler_params=pltpu.CompilerParams(vmem_limit_bytes=4 * MIB),
        name="norm",
    )(upstream, stored, mom, affine)


def block_grad(cells, base, grad_ref, q_ref, x_ref, stats_ref, sums_ref):
    frames, cols, rows, channels = grad_ref.shape
    totals = group_sum(jnp.sum(sums_ref[...], axis=0)) * (1.0 / cells)
    result = []
    for f in range(frames):
        mean = stats_ref[base + f : base + f + 1]
        scale = stats_ref[base + frames + f : base + frames + f + 1]
        flat = (cols * rows, channels)
        normed = (x_ref[f].astype(jnp.float32).reshape(flat) - mean) * scale
        value = grad_ref[f].astype(jnp.float32).reshape(flat) + scale * (
            q_ref[f].reshape(flat)
            - totals[f : f + 1]
            - normed * totals[frames + f : frames + f + 1]
        )
        result.append(value.astype(jnp.bfloat16))
    return result


def dx_kernel(cells, par_ref, grad_ref, q_ref, x_ref, stats_ref, sums_ref, dx_ref, sa_ref, sb_ref):
    _, cols, rows, channels = grad_ref.shape
    even, _, _ = flags(par_ref)
    for f, value in enumerate(block_grad(cells, 0, grad_ref, q_ref, x_ref, stats_ref, sums_ref)):
        value = value.reshape(cols, rows, channels)
        dx_ref[f] = value
        sa_ref[f], sb_ref[f] = swapped(even, value[cols - 1], value[0])


def dx_section(par, grad, q, stored, stats, sums, cells):
    frames, _, rows, channels = grad.shape
    edge = jax.ShapeDtypeStruct((frames, rows, channels), jnp.bfloat16)
    return pl.pallas_call(
        functools.partial(dx_kernel, cells),
        out_shape=(jax.ShapeDtypeStruct(grad.shape, jnp.bfloat16), edge, edge),
        in_specs=vmem(6),
        out_specs=tuple(vmem(3)),
        compiler_params=pltpu.CompilerParams(vmem_limit_bytes=16 * MIB),
        cost_estimate=WEIGHTS_COVER,
        name="dx",
    )(par, grad, q, stored, stats, sums)


def conv_norm_kernel(
    par_ref,
    own_ref,
    next_ref,
    ra_ref,
    rb_ref,
    ran_ref,
    rbn_ref,
    w_ref,
    x_ref,
    stats_ref,
    affine_ref,
    q_ref,
    sums_ref,
    ext,
    acc,
):
    rows = own_ref.shape[2]
    window(par_ref, own_ref, next_ref, ra_ref, rb_ref, ran_ref, rbn_ref, ext)
    acc[...] = time_taps(ext, w_ref, (2, 1, 0), *own_ref.shape[:2])
    upstream = row_taps(acc, rows)
    stats = stats_ref[2 * own_ref.shape[0] :]
    finish(stats, upstream, x_ref, affine_ref, 2, q_ref, sums_ref)


def conv_norm_section(par, grad, halo, kernel, stored, stats, affine, peers):
    frames, cols, rows, channels = grad.shape
    count = frames * cols * rows
    return pl.pallas_call(
        conv_norm_kernel,
        out_shape=finish_shapes(stored, peers),
        in_specs=vmem(11),
        out_specs=tuple(vmem(2)),
        scratch_shapes=[
            pltpu.VMEM((2 * frames, cols + 2, rows, channels), jnp.bfloat16),
            pltpu.VMEM((count, 3 * channels), jnp.float32),
        ],
        compiler_params=pltpu.CompilerParams(vmem_limit_bytes=16 * MIB),
        cost_estimate=matmul_cost(count, kernel),
        name="convnorm",
    )(par, grad, *halo, kernel, stored, stats, affine)


def edge_kernel(par_ref, block_ref, *out_refs):
    cols = block_ref.shape[1]
    even, _, _ = flags(par_ref)
    for ref, value in zip(out_refs, swapped(even, block_ref[:, cols - 1], block_ref[:, 0])):
        ref[...] = value


def edge_section(par, block, count, cost):
    frames, _, rows, channels = block.shape
    edge = jax.ShapeDtypeStruct((frames, rows, channels), block.dtype)
    return pl.pallas_call(
        edge_kernel,
        out_shape=(edge,) * count,
        in_specs=vmem(2),
        out_specs=tuple(vmem(count)),
        compiler_params=pltpu.CompilerParams(vmem_limit_bytes=4 * MIB),
        cost_estimate=cost,
        name="edge",
    )(par, block)


def latent_kernel_body(cells, grad_ref, q_ref, x_ref, stats_ref, sums_ref, k_ref, own_ref, prev_ref, wide):
    frames, cols, rows, channels = grad_ref.shape
    lat = k_ref.shape[1]
    lanes = own_ref.shape[-1]
    values = block_grad(cells, 2 * frames, grad_ref, q_ref, x_ref, stats_ref, sums_ref)
    grad = jnp.concatenate(values, axis=0)
    count = frames * cols * rows
    wide[...] = jnp.zeros_like(wide)
    width = 3 * lat
    spots = (0, width, lanes)
    for b in range(3):
        for a in range(3):
            k = 9 * a + 3 * b
            wide[b, spots[a] : spots[a] + width] = k_ref[k : k + 3].reshape(width, channels)
    row = lax.broadcasted_iota(jnp.int32, (count, 1), 0) % rows
    z = [nt_dot(grad, wide[b]) for b in range(3)]
    up = jnp.where(row < rows - 1, pltpu.roll(z[0], count - 1, 0), 0.0)
    down = jnp.where(row > 0, pltpu.roll(z[2], 1, 0), 0.0)
    total = z[1] + up + down
    lane = lax.broadcasted_iota(jnp.int32, (1, lanes), 1)
    both, third = total[:, :lanes], total[:, lanes:]
    parts = (
        jnp.where(lane < width, both, 0.0),
        jnp.where(lane < width, 0.0, both),
        third,
    )
    placed = {}
    for a in range(3):
        part = parts[a].reshape(frames, cols, rows, lanes)
        base = width if a == 1 else 0
        for f in range(frames):
            out = None
            for w in range(cols):
                shift = (lat * w - base) % lanes
                one = pltpu.roll(part[f, w], shift, 1) if shift else part[f, w]
                out = one if out is None else out + one
            at = f + a - 2
            placed[at] = placed[at] + out if at in placed else out
    for f in range(frames):
        own_ref[f] = placed[f]
        prev_ref[f] = placed[f - 2]


def latent_section(grad, q, stored, stats, sums, kernel, cells):
    frames, _, rows, channels = grad.shape
    lanes = 128
    out = jax.ShapeDtypeStruct((frames, rows, lanes), jnp.float32)
    return pl.pallas_call(
        functools.partial(latent_kernel_body, cells),
        out_shape=(out, out),
        in_specs=vmem(6),
        out_specs=tuple(vmem(2)),
        scratch_shapes=[pltpu.VMEM((3, 2 * lanes, channels), jnp.bfloat16)],
        compiler_params=pltpu.CompilerParams(vmem_limit_bytes=16 * MIB),
        name="latent",
    )(grad, q, stored, stats, sums, kernel)


def assemble_kernel(lat, cols, got_ref, e_ref, perm_ref, out_ref):
    parts = {}
    for p in range(2):
        rows = jnp.concatenate([got_ref[:, p, :], got_ref[:, 2 + p, :]], axis=0)
        spots = lax.dot_general(
            jnp.concatenate(thirds(rows), axis=0),
            e_ref[...],
            (((0,), (0,)), ((), ())),
            preferred_element_type=jnp.float32,
        )
        for col in range(cols + 2):
            q = (col + 1) % 2
            piece = spots[lat * col : lat * (col + 1), 128 * col : 128 * (col + 1)]
            parts[p, q] = parts[p, q] + piece if (p, q) in parts else piece
    stacked = jnp.concatenate([parts[p, q] for p in range(2) for q in range(2)], axis=0)
    final = jnp.dot(
        perm_ref[...],
        jnp.concatenate(thirds(stacked), axis=0),
        preferred_element_type=jnp.float32,
    )
    out_ref[...] = final[:, : out_ref.shape[1]]


def assemble(got, lat, cols):
    peers, quad, _ = got.shape
    width = peers * cols // 2
    tokens = quad // 2 * width
    place = np.zeros((quad // 2, peers, (cols + 2) * 128), np.float32)
    for hh in range(quad // 2):
        for s in range(peers):
            for col in range(cols + 2):
                x = s * cols + col - 1
                if 0 <= x < peers * cols:
                    place[hh, s, 128 * col + hh * width + x // 2] = 1.0
    place = np.tile(place.reshape(-1, place.shape[-1]), (3, 1))
    perm = np.zeros((4 * lat, 4 * lat), np.float32)
    for pq in range(4):
        for one in range(lat):
            perm[one * 4 + pq, pq * lat + one] = 1.0
    perm = np.tile(perm, (1, 3))
    return pl.pallas_call(
        functools.partial(assemble_kernel, lat, cols),
        out_shape=jax.ShapeDtypeStruct((4 * lat, tokens), jnp.float32),
        in_specs=vmem(3),
        out_specs=pl.BlockSpec(memory_space=pltpu.VMEM),
        compiler_params=pltpu.CompilerParams(vmem_limit_bytes=16 * MIB),
        name="assemble",
    )(got, jnp.asarray(place, jnp.bfloat16), jnp.asarray(perm, jnp.bfloat16))


def routes():
    tms, tiles = lax.axis_size("tm"), lax.axis_size(TILE)
    back = ring(tms)
    hops = []
    for k in range(1, tiles, 2):
        hops += [(k, (k + 1) % tiles), ((k + 1) % tiles, k)]
    diagonal = [(t * tiles + s, u * tiles + d) for t, u in back for s, d in hops]
    return back, hops, diagonal


SWAP = [(0, 1), (1, 0)]


def frames_on(value):
    return lax.ppermute(value, "tm", routes()[0])


def columns_on(send_a, send_b):
    _, hops, diagonal = routes()
    rb = lax.ppermute(send_b, TILE, hops)
    rbn = lax.ppermute(send_b, TM_TILE, diagonal)
    ra = lax.ppermute(send_a, "tile_2", SWAP)
    return ra, rb, rbn


def ring(count):
    return [(t, (t - 1) % count) for t in range(count)]


def everyone(rows):
    return lax.all_to_all(rows, TILE, 0, 0)


def shards(
    first_input,
    second_input,
    output_grad,
    first_gain,
    first_shift,
    first_kernel,
    second_gain,
    second_shift,
    second_kernel,
    latent_kernel,
):
    frames, rows, cols, channels = first_input.shape
    peers = lax.axis_size(TILE)
    cells = rows * cols * peers * (channels // GROUPS)
    core = lax.axis_index("tile_2")
    even = core == 0
    tile, when = lax.axis_index(TILE), lax.axis_index("tm")
    later = when < lax.axis_size("tm") - 1
    side = jnp.where(even, tile > 0, tile < peers - 1)
    ones = jnp.stack([even, side, later]).astype(jnp.bfloat16)
    par = jnp.broadcast_to(ones[:, None], (3, channels))
    par, later, output_grad, second_input, first_input = lax.optimization_barrier(
        (par, later, output_grad, second_input, first_input)
    )
    turn = lambda x: with_layout_constraint(
        jnp.transpose(x, (0, 2, 1, 3)), Layout(major_to_minor=(0, 1, 2, 3))
    )

    grad = turn(output_grad)
    vectors = (second_gain, second_shift, first_gain, first_shift)
    mine, affine = moments(second_input, first_input, vectors, peers)
    mom = everyone(mine)
    nxt = turn(frames_on(output_grad))
    ra, rb, rbn = columns_on(*edge_section(par, grad, 2, INPUTS_COVER))
    part, corner = gather_section(par, grad, nxt, ra, rb, rbn)
    ran = lax.ppermute(corner, "tile_2", SWAP)
    second, first = turn(second_input), turn(first_input)
    upstream = conv_section(par, part, ran, second_kernel)
    q, sums, stats = norm_section(upstream, second, mom, affine, cells, peers)
    grad, send_a, send_b = dx_section(par, grad, q, second, stats, everyone(sums), cells)
    nxt = jnp.concatenate([frames_on(grad[f : f + 1]) for f in range(frames)], axis=0)
    ra, rb, rbn = columns_on(send_a, send_b)
    (corner,) = edge_section(par, nxt, 1, None)
    ran = lax.ppermute(corner, "tile_2", SWAP)
    q, sums = conv_norm_section(
        par, grad, (nxt, ra, rb, ran, rbn), first_kernel, first, stats, affine, peers
    )
    own, prev = latent_section(grad, q, first, stats, everyone(sums), latent_kernel, cells)
    tms = lax.axis_size("tm")
    own = own + jnp.where(later, lax.ppermute(prev, "tm", ring(tms)), 0.0)
    got = everyone(own.reshape(peers, frames * rows // peers, own.shape[-1]))
    return assemble(got, latent_kernel.shape[1], cols)


def solution(mesh):
    torus = Mesh(
        mesh.devices.reshape(mesh.shape["tm"], 4, 2, 2), ("tm", "tile_0", "tile_1", "tile_2")
    )
    block = P("tm", None, TILE, None)
    placed = (block, block, block) + (P(),) * 7
    return jax.shard_map(
        shards, mesh=torus, in_specs=placed, out_specs=P(None, TM_TILE), check_vma=False
    )
```

```python
import functools

import jax
import jax.numpy as jnp
import numpy as np
from jax import lax
from jax.experimental import pallas as pl
from jax.experimental.pallas import tpu as pltpu
from jax.experimental.layout import Layout, with_layout_constraint
from jax.sharding import Mesh
from jax.sharding import PartitionSpec as P

GROUPS = 32
TILE = ("tile_0", "tile_1", "tile_2")
TM_TILE = ("tm",) + TILE
EPSILON = 1e-05
MIB = 1 << 20


def vmem(count):
    return [pl.BlockSpec(memory_space=pltpu.VMEM)] * count


WEIGHTS_COVER = pl.CostEstimate(flops=1 << 33, bytes_accessed=1 << 23, transcendentals=0)
WEIGHTS_WINDOW = pl.CostEstimate(
    flops=1 << 33, bytes_accessed=1 << 23, transcendentals=262000000
)
INPUTS_COVER = pl.CostEstimate(flops=1 << 31, bytes_accessed=1 << 20, transcendentals=0)
HBM = [pl.BlockSpec(memory_space=pltpu.HBM)]


def matmul_cost(count, kernel):
    return pl.CostEstimate(
        flops=2 * count * kernel.size, bytes_accessed=2 * kernel.size, transcendentals=0
    )


def nt_dot(left, right, **kw):
    return lax.dot_general(
        left, right, (((1,), (1,)), ((), ())), preferred_element_type=jnp.float32, **kw
    )


def thirds(value):
    high = value.astype(jnp.bfloat16)
    rest = value - high.astype(jnp.float32)
    middle = rest.astype(jnp.bfloat16)
    return high, middle, (rest - middle.astype(jnp.float32)).astype(jnp.bfloat16)


def group_sum(rows):
    count, channels = rows.shape
    per = channels // GROUPS
    row = lax.broadcasted_iota(jnp.int32, (channels, channels), 0) // per
    col = lax.broadcasted_iota(jnp.int32, (channels, channels), 1) // per
    same = jnp.where(row == col, 1.0, 0.0).astype(jnp.bfloat16)
    if count < 8:
        rows = jnp.concatenate([rows, jnp.zeros((8 - count, channels), jnp.float32)], axis=0)
    split = jnp.concatenate([part.astype(jnp.float32) for part in thirds(rows)], axis=0)
    sums = jnp.dot(split.astype(jnp.bfloat16), same, preferred_element_type=jnp.float32)
    return sums[0:count] + sums[8 : 8 + count] + sums[16 : 16 + count]


def spread(ref, rows):
    ref[...] = jnp.broadcast_to(rows[None], ref.shape)


def moments_kernel(second_ref, first_ref, *refs):
    *vectors, out_ref, affine_ref = refs
    rows = []
    for ref in (second_ref, first_ref):
        frames = ref.shape[0]
        values = [ref[f].astype(jnp.float32) for f in range(frames)]
        rows += [jnp.sum(v, axis=(0, 1)).reshape(1, -1) for v in values]
        rows += [jnp.sum(v * v, axis=(0, 1)).reshape(1, -1) for v in values]
    spread(out_ref, jnp.concatenate(rows, axis=0))
    for k, line in enumerate(vectors):
        affine_ref[k : k + 1] = line[...].reshape(1, -1)


def moments(second, first, vectors, peers):
    frames, _, _, channels = second.shape
    return pl.pallas_call(
        moments_kernel,
        out_shape=(
            jax.ShapeDtypeStruct((peers, 4 * frames, channels), jnp.float32),
            jax.ShapeDtypeStruct((len(vectors), channels), jnp.float32),
        ),
        in_specs=vmem(2 + len(vectors)),
        out_specs=tuple(vmem(2)),
        compiler_params=pltpu.CompilerParams(vmem_limit_bytes=16 * MIB),
        name="moments",
    )(second, first, *vectors)


def fill(ext, at, block, a, b, even):
    frames, cols = block.shape[:2]
    ext[at : at + frames, 1 : cols + 1] = block
    right, left = swapped(even, a, b)
    ext[at : at + frames, 0] = left
    ext[at : at + frames, cols + 1] = right


def time_taps(ext, w_ref, taps, frames, cols):
    _, channels = ext.shape[2:]
    pairs = [(a, c) for a in taps for c in range(3)]
    left = jnp.concatenate(
        [
            ext[2 - a : 2 - a + frames, 2 - c : 2 - c + cols].reshape(-1, channels)
            for a, c in pairs
        ],
        axis=1,
    )
    right = jnp.concatenate(
        [
            jnp.concatenate([w_ref[9 * a + 3 * b + c] for a, c in pairs], axis=1)
            for b in range(3)
        ],
        axis=0,
    )
    return nt_dot(left, right)


def row_taps(wide, rows):
    count, channels = wide.shape[0], wide.shape[1] // 3
    row = lax.broadcasted_iota(jnp.int32, (count, 1), 0) % rows
    up = jnp.where(row < rows - 1, pltpu.roll(wide[:, :channels], count - 1, 0), 0.0)
    down = jnp.where(row > 0, pltpu.roll(wide[:, 2 * channels :], 1, 0), 0.0)
    return wide[:, channels : 2 * channels] + up + down


def flags(par_ref):
    return [par_ref[k : k + 1] for k in range(3)]


def swapped(even, a, b):
    odd = 1 - even
    return a * even + b * odd, b * even + a * odd


def window(par_ref, own_ref, next_ref, ra_ref, rb_ref, ran_ref, rbn_ref, ext):
    frames = own_ref.shape[0]
    even, side, later = flags(par_ref)
    fill(ext, 0, own_ref[...], ra_ref[...], rb_ref[...] * side, even)
    fill(
        ext,
        frames,
        next_ref[...] * later,
        jnp.zeros_like(rbn_ref) if ran_ref is None else ran_ref[...] * later,
        rbn_ref[...] * (later * side),
        even,
    )


def gather_kernel(par_ref, own_ref, next_ref, ra_ref, rb_ref, rbn_ref, ext_ref, corner_ref):
    even, _, _ = flags(par_ref)
    cols = own_ref.shape[1]
    window(par_ref, own_ref, next_ref, ra_ref, rb_ref, None, rbn_ref, ext_ref)
    corner_ref[...], _ = swapped(even, next_ref[:, cols - 1], next_ref[:, 0])


def gather_section(par, own, nxt, ra, rb, rbn):
    frames, cols, rows, channels = own.shape
    return pl.pallas_call(
        gather_kernel,
        out_shape=(
            jax.ShapeDtypeStruct((2 * frames, cols + 2, rows, channels), own.dtype),
            jax.ShapeDtypeStruct((frames, rows, channels), own.dtype),
        ),
        in_specs=vmem(6),
        out_specs=tuple(vmem(2)),
        compiler_params=pltpu.CompilerParams(vmem_limit_bytes=4 * MIB),
        cost_estimate=WEIGHTS_WINDOW,
        name="gather",
    )(par, own, nxt, ra, rb, rbn)


def conv_kernel(par_ref, part_ref, ran_ref, w_ref, u_ref, ext, acc):
    frames, rows = ran_ref.shape[:2]
    cols = part_ref.shape[1] - 2
    even, _, later = flags(par_ref)
    ext[...] = part_ref[...]
    right, left = swapped(even, ran_ref[...] * later, jnp.zeros_like(ran_ref))
    ext[frames:, 0] = part_ref[frames:, 0] + left
    ext[frames:, cols + 1] = part_ref[frames:, cols + 1] + right
    acc[...] = time_taps(ext, w_ref, (2, 1, 0), frames, cols)
    u_ref[...] = row_taps(acc, rows)


def conv_section(par, part, ran, kernel):
    frames, rows, channels = ran.shape
    cols = part.shape[1] - 2
    count = frames * cols * rows
    return pl.pallas_call(
        conv_kernel,
        out_shape=jax.ShapeDtypeStruct((count, channels), jnp.float32),
        in_specs=vmem(4),
        out_specs=vmem(1)[0],
        scratch_shapes=[
            pltpu.VMEM(part.shape, jnp.bfloat16),
            pltpu.VMEM((count, 3 * channels), jnp.float32),
        ],
        compiler_params=pltpu.CompilerParams(vmem_limit_bytes=16 * MIB),
        cost_estimate=matmul_cost(count, kernel),
        name="conv",
    )(par, part, ran, kernel)


def norm_stats(cells, frames, mom_ref):
    totals = group_sum(jnp.sum(mom_ref[...], axis=0)) * (1.0 / cells)
    rows = []
    for base in (0, 2 * frames):
        mean = totals[base : base + frames]
        rows += [mean, lax.rsqrt(totals[base + frames : base + 2 * frames] - mean * mean + EPSILON)]
    return jnp.concatenate(rows, axis=0)


def through(upstream, normed, gain, shift):
    pre = normed * gain + shift
    sig = jax.nn.sigmoid(pre)
    return upstream * sig * (1.0 + pre * (1.0 - sig)) * gain


def finish(stats, upstream, x_ref, affine_ref, at, q_ref, sums_ref):
    frames, cols, rows, channels = x_ref.shape
    gain, shift = affine_ref[at : at + 1], affine_ref[at + 1 : at + 2]
    half = cols * rows
    sums, crosses = [], []
    for f in range(frames):
        mean, scale = stats[f : f + 1], stats[frames + f : frames + f + 1]
        normed = (x_ref[f].astype(jnp.float32).reshape(half, channels) - mean) * scale
        q = through(upstream[f * half : (f + 1) * half], normed, gain, shift)
        q_ref[f] = q.reshape(cols, rows, channels)
        sums.append(jnp.sum(q, axis=0, keepdims=True))
        crosses.append(jnp.sum(q * normed, axis=0, keepdims=True))
    spread(sums_ref, jnp.concatenate(sums + crosses, axis=0))


def finish_shapes(stored, peers):
    frames, _, _, channels = stored.shape
    return (
        jax.ShapeDtypeStruct(stored.shape, jnp.float32),
        jax.ShapeDtypeStruct((peers, 2 * frames, channels), jnp.float32),
    )


def norm_kernel(cells, u_ref, x_ref, mom_ref, affine_ref, q_ref, sums_ref, stats_ref):
    frames = x_ref.shape[0]
    stats = norm_stats(cells, frames, mom_ref)
    finish(stats[: 2 * frames], u_ref, x_ref, affine_ref, 0, q_ref, sums_ref)
    stats_ref[...] = stats


def norm_section(upstream, stored, mom, affine, cells, peers):
    frames, _, _, channels = stored.shape
    stats = jax.ShapeDtypeStruct((4 * frames, channels), jnp.float32)
    return pl.pallas_call(
        functools.partial(norm_kernel, cells),
        out_shape=(*finish_shapes(stored, peers), stats),
        in_specs=vmem(4),
        out_specs=tuple(vmem(3)),
        compiler_params=pltpu.CompilerParams(vmem_limit_bytes=4 * MIB),
        name="norm",
    )(upstream, stored, mom, affine)


def block_grad(cells, base, grad_ref, q_ref, x_ref, stats_ref, sums_ref):
    frames, cols, rows, channels = grad_ref.shape
    totals = group_sum(jnp.sum(sums_ref[...], axis=0)) * (1.0 / cells)
    result = []
    for f in range(frames):
        mean = stats_ref[base + f : base + f + 1]
        scale = stats_ref[base + frames + f : base + frames + f + 1]
        flat = (cols * rows, channels)
        normed = (x_ref[f].astype(jnp.float32).reshape(flat) - mean) * scale
        value = grad_ref[f].astype(jnp.float32).reshape(flat) + scale * (
            q_ref[f].reshape(flat)
            - totals[f : f + 1]
            - normed * totals[frames + f : frames + f + 1]
        )
        result.append(value.astype(jnp.bfloat16))
    return result


def dx_kernel(cells, par_ref, grad_ref, q_ref, x_ref, stats_ref, sums_ref, dx_ref, sa_ref, sb_ref):
    _, cols, rows, channels = grad_ref.shape
    even, _, _ = flags(par_ref)
    for f, value in enumerate(block_grad(cells, 0, grad_ref, q_ref, x_ref, stats_ref, sums_ref)):
        value = value.reshape(cols, rows, channels)
        dx_ref[f] = value
        sa_ref[f], sb_ref[f] = swapped(even, value[cols - 1], value[0])


def dx_section(par, grad, q, stored, stats, sums, cells):
    frames, _, rows, channels = grad.shape
    edge = jax.ShapeDtypeStruct((frames, rows, channels), jnp.bfloat16)
    return pl.pallas_call(
        functools.partial(dx_kernel, cells),
        out_shape=(jax.ShapeDtypeStruct(grad.shape, jnp.bfloat16), edge, edge),
        in_specs=vmem(6),
        out_specs=tuple(vmem(3)),
        compiler_params=pltpu.CompilerParams(vmem_limit_bytes=16 * MIB),
        cost_estimate=WEIGHTS_COVER,
        name="dx",
    )(par, grad, q, stored, stats, sums)


def conv_norm_kernel(
    par_ref,
    own_ref,
    next_ref,
    ra_ref,
    rb_ref,
    ran_ref,
    rbn_ref,
    w_ref,
    x_ref,
    stats_ref,
    affine_ref,
    q_ref,
    sums_ref,
    ext,
    acc,
):
    rows = own_ref.shape[2]
    window(par_ref, own_ref, next_ref, ra_ref, rb_ref, ran_ref, rbn_ref, ext)
    acc[...] = time_taps(ext, w_ref, (2, 1, 0), *own_ref.shape[:2])
    upstream = row_taps(acc, rows)
    stats = stats_ref[2 * own_ref.shape[0] :]
    finish(stats, upstream, x_ref, affine_ref, 2, q_ref, sums_ref)


def conv_norm_section(par, grad, halo, kernel, stored, stats, affine, peers):
    frames, cols, rows, channels = grad.shape
    count = frames * cols * rows
    return pl.pallas_call(
        conv_norm_kernel,
        out_shape=finish_shapes(stored, peers),
        in_specs=vmem(11),
        out_specs=tuple(vmem(2)),
        scratch_shapes=[
            pltpu.VMEM((2 * frames, cols + 2, rows, channels), jnp.bfloat16),
            pltpu.VMEM((count, 3 * channels), jnp.float32),
        ],
        compiler_params=pltpu.CompilerParams(vmem_limit_bytes=16 * MIB),
        cost_estimate=matmul_cost(count, kernel),
        name="convnorm",
    )(par, grad, *halo, kernel, stored, stats, affine)


def edge_kernel(par_ref, block_ref, *out_refs):
    cols = block_ref.shape[1]
    even, _, _ = flags(par_ref)
    for ref, value in zip(out_refs, swapped(even, block_ref[:, cols - 1], block_ref[:, 0])):
        ref[...] = value


def edge_section(par, block, count, cost):
    frames, _, rows, channels = block.shape
    edge = jax.ShapeDtypeStruct((frames, rows, channels), block.dtype)
    return pl.pallas_call(
        edge_kernel,
        out_shape=(edge,) * count,
        in_specs=vmem(2),
        out_specs=tuple(vmem(count)),
        compiler_params=pltpu.CompilerParams(vmem_limit_bytes=4 * MIB),
        cost_estimate=cost,
        name="edge",
    )(par, block)


def latent_kernel_body(cells, grad_ref, q_ref, x_ref, stats_ref, sums_ref, k_ref, own_ref, prev_ref, wide):
    frames, cols, rows, channels = grad_ref.shape
    lat = k_ref.shape[1]
    lanes = own_ref.shape[-1]
    values = block_grad(cells, 2 * frames, grad_ref, q_ref, x_ref, stats_ref, sums_ref)
    grad = jnp.concatenate(values, axis=0)
    count = frames * cols * rows
    wide[...] = jnp.zeros_like(wide)
    width = 3 * lat
    spots = (0, width, lanes)
    for b in range(3):
        for a in range(3):
            k = 9 * a + 3 * b
            wide[b, spots[a] : spots[a] + width] = k_ref[k : k + 3].reshape(width, channels)
    row = lax.broadcasted_iota(jnp.int32, (count, 1), 0) % rows
    z = [nt_dot(grad, wide[b]) for b in range(3)]
    up = jnp.where(row < rows - 1, pltpu.roll(z[0], count - 1, 0), 0.0)
    down = jnp.where(row > 0, pltpu.roll(z[2], 1, 0), 0.0)
    total = z[1] + up + down
    lane = lax.broadcasted_iota(jnp.int32, (1, lanes), 1)
    both, third = total[:, :lanes], total[:, lanes:]
    parts = (
        jnp.where(lane < width, both, 0.0),
        jnp.where(lane < width, 0.0, both),
        third,
    )
    placed = {}
    for a in range(3):
        part = parts[a].reshape(frames, cols, rows, lanes)
        base = width if a == 1 else 0
        for f in range(frames):
            out = None
            for w in range(cols):
                shift = (lat * w - base) % lanes
                one = pltpu.roll(part[f, w], shift, 1) if shift else part[f, w]
                out = one if out is None else out + one
            at = f + a - 2
            placed[at] = placed[at] + out if at in placed else out
    for f in range(frames):
        own_ref[f] = placed[f]
        prev_ref[f] = placed[f - 2]


def latent_section(grad, q, stored, stats, sums, kernel, cells):
    frames, _, rows, channels = grad.shape
    lanes = 128
    out = jax.ShapeDtypeStruct((frames, rows, lanes), jnp.float32)
    return pl.pallas_call(
        functools.partial(latent_kernel_body, cells),
        out_shape=(out, out),
        in_specs=vmem(6),
        out_specs=tuple(vmem(2)),
        scratch_shapes=[pltpu.VMEM((3, 2 * lanes, channels), jnp.bfloat16)],
        compiler_params=pltpu.CompilerParams(vmem_limit_bytes=16 * MIB),
        name="latent",
    )(grad, q, stored, stats, sums, kernel)


def assemble_kernel(lat, cols, got_ref, e_ref, perm_ref, out_ref):
    parts = {}
    for p in range(2):
        rows = jnp.concatenate([got_ref[:, p, :], got_ref[:, 2 + p, :]], axis=0)
        spots = lax.dot_general(
            jnp.concatenate(thirds(rows), axis=0),
            e_ref[...],
            (((0,), (0,)), ((), ())),
            preferred_element_type=jnp.float32,
        )
        for col in range(cols + 2):
            q = (col + 1) % 2
            piece = spots[lat * col : lat * (col + 1), 128 * col : 128 * (col + 1)]
            parts[p, q] = parts[p, q] + piece if (p, q) in parts else piece
    stacked = jnp.concatenate([parts[p, q] for p in range(2) for q in range(2)], axis=0)
    final = jnp.dot(
        perm_ref[...],
        jnp.concatenate(thirds(stacked), axis=0),
        preferred_element_type=jnp.float32,
    )
    out_ref[...] = final[:, : out_ref.shape[1]]


def assemble(got, lat, cols):
    peers, quad, _ = got.shape
    width = peers * cols // 2
    tokens = quad // 2 * width
    place = np.zeros((quad // 2, peers, (cols + 2) * 128), np.float32)
    for hh in range(quad // 2):
        for s in range(peers):
            for col in range(cols + 2):
                x = s * cols + col - 1
                if 0 <= x < peers * cols:
                    place[hh, s, 128 * col + hh * width + x // 2] = 1.0
    place = np.tile(place.reshape(-1, place.shape[-1]), (3, 1))
    perm = np.zeros((4 * lat, 4 * lat), np.float32)
    for pq in range(4):
        for one in range(lat):
            perm[one * 4 + pq, pq * lat + one] = 1.0
    perm = np.tile(perm, (1, 3))
    return pl.pallas_call(
        functools.partial(assemble_kernel, lat, cols),
        out_shape=jax.ShapeDtypeStruct((4 * lat, tokens), jnp.float32),
        in_specs=vmem(3),
        out_specs=pl.BlockSpec(memory_space=pltpu.VMEM),
        compiler_params=pltpu.CompilerParams(vmem_limit_bytes=16 * MIB),
        name="assemble",
    )(got, jnp.asarray(place, jnp.bfloat16), jnp.asarray(perm, jnp.bfloat16))


def routes():
    tms, tiles = lax.axis_size("tm"), lax.axis_size(TILE)
    back = ring(tms)
    hops = []
    for k in range(1, tiles, 2):
        hops += [(k, (k + 1) % tiles), ((k + 1) % tiles, k)]
    diagonal = [(t * tiles + s, u * tiles + d) for t, u in back for s, d in hops]
    return back, hops, diagonal


SWAP = [(0, 1), (1, 0)]


def frames_on(value):
    return lax.ppermute(value, "tm", routes()[0])


def columns_on(send_a, send_b):
    _, hops, diagonal = routes()
    rb = lax.ppermute(send_b, TILE, hops)
    rbn = lax.ppermute(send_b, TM_TILE, diagonal)
    ra = lax.ppermute(send_a, "tile_2", SWAP)
    return ra, rb, rbn


def ring(count):
    return [(t, (t - 1) % count) for t in range(count)]


def everyone(rows):
    return lax.all_to_all(rows, TILE, 0, 0)


def shards(
    first_input,
    second_input,
    output_grad,
    first_gain,
    first_shift,
    first_kernel,
    second_gain,
    second_shift,
    second_kernel,
    latent_kernel,
):
    frames, rows, cols, channels = first_input.shape
    peers = lax.axis_size(TILE)
    cells = rows * cols * peers * (channels // GROUPS)
    core = lax.axis_index("tile_2")
    even = core == 0
    tile, when = lax.axis_index(TILE), lax.axis_index("tm")
    later = when < lax.axis_size("tm") - 1
    side = jnp.where(even, tile > 0, tile < peers - 1)
    ones = jnp.stack([even, side, later]).astype(jnp.bfloat16)
    par = jnp.broadcast_to(ones[:, None], (3, channels))
    par, later, output_grad, second_input, first_input = lax.optimization_barrier(
        (par, later, output_grad, second_input, first_input)
    )
    plain = lambda x: with_layout_constraint(x, Layout(major_to_minor=(0, 1, 2, 3)))
    turn = lambda x: plain(jnp.transpose(x, (0, 2, 1, 3)))

    grad = turn(output_grad)
    vectors = (second_gain, second_shift, first_gain, first_shift)
    mine, affine = moments(second_input, first_input, vectors, peers)
    mom = everyone(mine)
    nxt = turn(plain(frames_on(plain(output_grad))))
    ra, rb, rbn = columns_on(*edge_section(par, grad, 2, INPUTS_COVER))
    part, corner = gather_section(par, grad, nxt, ra, rb, rbn)
    ran = lax.ppermute(corner, "tile_2", SWAP)
    second, first = turn(second_input), turn(first_input)
    upstream = conv_section(par, part, ran, second_kernel)
    q, sums, stats = norm_section(upstream, second, mom, affine, cells, peers)
    grad, send_a, send_b = dx_section(par, grad, q, second, stats, everyone(sums), cells)
    nxt = frames_on(grad)
    ra, rb, rbn = columns_on(send_a, send_b)
    (corner,) = edge_section(par, nxt, 1, None)
    ran = lax.ppermute(corner, "tile_2", SWAP)
    q, sums = conv_norm_section(
        par, grad, (nxt, ra, rb, ran, rbn), first_kernel, first, stats, affine, peers
    )
    own, prev = latent_section(grad, q, first, stats, everyone(sums), latent_kernel, cells)
    tms = lax.axis_size("tm")
    own = own + jnp.where(later, lax.ppermute(prev, "tm", ring(tms)), 0.0)
    got = everyone(own.reshape(peers, frames * rows // peers, own.shape[-1]))
    return assemble(got, latent_kernel.shape[1], cols)


def solution(mesh):
    torus = Mesh(
        mesh.devices.reshape(mesh.shape["tm"], 4, 2, 2), ("tm", "tile_0", "tile_1", "tile_2")
    )
    block = P("tm", None, TILE, None)
    placed = (block, block, block) + (P(),) * 7
    return jax.shard_map(
        shards, mesh=torus, in_specs=placed, out_specs=P(None, TM_TILE), check_vma=False
    )
```
